256 devices in a mesh: dap: 128 (over z_lo, x, y, core), rep: 2 (over z_hi).
Axes of the slice: x: 4, y: 4, z: 8 (z_hi: 2, z_lo: 4; z = z_hi * 4 + z_lo), core: 2. Of those that a mesh axis runs over, the one named last changes fastest.
Arguments:
- related_chain_embedding: bfloat16 [256, 384, 256], P('dap'), may hold values from -6 to 6
- couple_representation: bfloat16 [384, 384, 128], P('dap'), may hold values from -6 to 6
- homolog_present: int32 [256], replicated, may hold values 0 or 1
- amino_present: int32 [384], replicated, may hold values 0 or 1
- horizontal_query_factors: bfloat16 [4, 256, 256], P(None, None, 'rep'), may hold values from -3 to 3
- across_chain_closing_transform: bfloat16 [256, 256], P('rep'), may hold values from -0.375 to 0.375
- couple_offset_factor: bfloat16 [128, 8], P(None, 'rep'), may hold values from -1.5859375 to 1.5859375
- vertical_query_factors: bfloat16 [4, 256, 256], P(None, None, 'rep'), may hold values from -3 to 3
- down_position_closing_transform: bfloat16 [256, 256], P('rep'), may hold values from -0.375 to 0.375
- trilateral_left_right_factors: bfloat16 [4, 128, 128], P(None, None, 'rep'), may hold values from -0.5 to 0.5
- trilateral_final_factor: bfloat16 [128, 128], P('rep'), may hold values from -0.5 to 0.5
- trilateral_sigmoid_factor: bfloat16 [128, 128], P(None, 'rep'), may hold values from -0.5 to 0.5
Outputs:
- alignment_output: bfloat16 [256, 384, 256], P(None, 'dap', 'rep')
- pair_output: bfloat16 [384, 384, 128], P('dap', None, 'rep')
The draws below stay inside these ranges and needn't reach their ends.
Inputs may be any that keep to these rules, and one draw needn't show every extreme that they name: `homolog_present`: 1 marks a sequence that keys may attend to. `amino_present`: 1 marks a residue that keys and the triangle products use.
All inputs are finite; a program needn't handle non-finite values.
Results may differ from the reference program's by a relative error of at most 0.012.
The reference program's roundings to bfloat16 on the way count: a program that leaves them out, or rounds other values in their place, can miss the bound.
Values may be sent and summed in bfloat16 or wider, within the bound.
A program may use at most 128 MiB of HBM per device.

```python
import math
import jax
import jax.numpy as jnp
from jax import lax

EMBED_LANES = 256
PAIR_DIM = 128
FOCUS_GROUPS = 8
GROUP_BREADTH = 32
TRI_DIM = 128
PROTEIN_SITES = 384
RELATIVE_CHAINS = 256


def projection_draw(key, constant):
    folded = jax.random.fold_in(key, constant)
    normal_seed = jax.random.fold_in(folded, 0)
    stochastic_drawing = jax.random.normal(normal_seed, (4, EMBED_LANES, FOCUS_GROUPS * GROUP_BREADTH), jnp.float32) / math.sqrt(EMBED_LANES)
    return jnp.clip(stochastic_drawing, -3.0, 3.0)


def draw_horizontal_query_factors(key, part):
    return projection_draw(key, 101).astype(jnp.bfloat16)


def draw_vertical_query_factors(key, part):
    return projection_draw(key, 202).astype(jnp.bfloat16)


def plant(drawn, rng, smallest, high):
    place = [jax.random.randint(jax.random.fold_in(rng, axis), (), 0, length) for axis, length in enumerate(drawn.shape)]
    longest = drawn.shape.index(max(drawn.shape))
    beside = place[:longest] + [(place[longest] + 1) % drawn.shape[longest]] + place[longest + 1:]
    return drawn.at[tuple(place)].set(smallest).at[tuple(beside)].set(high)


def block_levels(stream_key, shape, pieces, smallest, largest):
    level = 1.0
    for axis_at, shards_of in pieces:
        heights = jax.random.uniform(jax.random.fold_in(jax.random.fold_in(stream_key, 6), axis_at), (shards_of,), jnp.float32, smallest / len(pieces), largest / len(pieces))
        level = level * jnp.repeat(jnp.exp(heights), shape[axis_at] // shards_of).reshape((-1,) + (1,) * (len(shape) - 1 - axis_at))
    return level


def centred(stream_key, shape, deviation, most, cuts=(), kind=jnp.bfloat16):
    loudness = block_levels(stream_key, shape, cuts, -0.22, 0.18) if cuts else 1.0
    values = jax.random.normal(stream_key, shape, jnp.float32) * deviation * loudness
    return jnp.minimum(jnp.maximum(values, -most), most).astype(kind)


def setup_inputs(seed: int = 0) -> dict:
    arg_keys = jax.random.split(jax.random.key(seed), 13)
    related_chain_embedding = centred(arg_keys[0], (RELATIVE_CHAINS, PROTEIN_SITES, EMBED_LANES), 1.0, 6.0, ((0, 128),))
    couple_representation = centred(arg_keys[1], (PROTEIN_SITES, PROTEIN_SITES, PAIR_DIM), 1.0, 6.0, ((0, 128),))
    homolog_present = plant((jax.random.randint(arg_keys[2], (RELATIVE_CHAINS,), 0, 4) < 3).astype(jnp.int32), jax.random.fold_in(arg_keys[2], 1), 0, 1)
    amino_present = plant((jax.random.randint(arg_keys[3], (PROTEIN_SITES,), 0, 4) < 3).astype(jnp.int32), jax.random.fold_in(arg_keys[3], 1), 0, 1)
    horizontal_query_factors = draw_horizontal_query_factors(jax.random.fold_in(arg_keys[12], 71), 0)
    across_chain_closing_transform = centred(arg_keys[5], (FOCUS_GROUPS * GROUP_BREADTH, EMBED_LANES), (FOCUS_GROUPS * GROUP_BREADTH) ** -0.5, 0.375, ((0, 2),))
    couple_offset_factor = centred(arg_keys[6], (PAIR_DIM, FOCUS_GROUPS), (3.0 / PAIR_DIM ** 0.5), 1.5859375, ((1, 2),))
    vertical_query_factors = draw_vertical_query_factors(jax.random.fold_in(arg_keys[12], 71), 0)
    down_position_closing_transform = centred(arg_keys[8], (FOCUS_GROUPS * GROUP_BREADTH, EMBED_LANES), (FOCUS_GROUPS * GROUP_BREADTH) ** -0.5, 0.375, ((0, 2),))
    trilateral_left_right_factors = centred(arg_keys[9], (4, PAIR_DIM, TRI_DIM), PAIR_DIM ** -0.5, 0.5, ((2, 2),))
    trilateral_final_factor = centred(arg_keys[10], (TRI_DIM, PAIR_DIM), TRI_DIM ** -0.5, 0.5, ((0, 2),))
    trilateral_sigmoid_factor = centred(arg_keys[11], (PAIR_DIM, PAIR_DIM), PAIR_DIM ** -0.5, 0.5, ((1, 2),))
    return {"related_chain_embedding": related_chain_embedding, "couple_representation": couple_representation, "homolog_present": homolog_present, "amino_present": amino_present, "horizontal_query_factors": horizontal_query_factors, "across_chain_closing_transform": across_chain_closing_transform, "couple_offset_factor": couple_offset_factor, "vertical_query_factors": vertical_query_factors, "down_position_closing_transform": down_position_closing_transform, "trilateral_left_right_factors": trilateral_left_right_factors, "trilateral_final_factor": trilateral_final_factor, "trilateral_sigmoid_factor": trilateral_sigmoid_factor}


EPS = 1e-05
NEG = 1000000000.0

def standardize_features(values):
    values = values.astype(jnp.float32)
    center = lax.optimization_barrier(jnp.mean(values, axis=-1, keepdims=True))
    spread = lax.optimization_barrier(jnp.mean(jnp.square(values - center), axis=-1, keepdims=True))
    return (values - center) * lax.rsqrt(spread + EPS)

def project_four(standardized_features, weights):
    array_extent = standardized_features.shape[:-1] + (FOCUS_GROUPS, GROUP_BREADTH)
    return tuple((jnp.dot(standardized_features, weights[number], preferred_element_type=jnp.float32).astype(jnp.bfloat16).reshape(array_extent) for number in range(4)))

def attend(query, keys, values, gate, bias):
    scores = jnp.einsum('qhd,khd->hqk', query.astype(jnp.float32), keys.astype(jnp.float32)) / jnp.sqrt(jnp.float32(GROUP_BREADTH)) + bias
    weights = jax.nn.softmax(scores, axis=-1).astype(jnp.bfloat16)
    mixed = jnp.einsum('hqk,khd->qhd', weights.astype(jnp.float32), values.astype(jnp.float32))
    return (mixed * jax.nn.sigmoid(gate.astype(jnp.float32))).astype(jnp.bfloat16)

def reference(related_chain_embedding, couple_representation, homolog_present, amino_present, horizontal_query_factors, across_chain_closing_transform, couple_offset_factor, vertical_query_factors, down_position_closing_transform, trilateral_left_right_factors, trilateral_final_factor, trilateral_sigmoid_factor):
    standardized_features = standardize_features(related_chain_embedding).astype(jnp.bfloat16)
    row_parts = project_four(standardized_features, horizontal_query_factors)
    pair_ln = standardize_features(couple_representation).astype(jnp.bfloat16)
    pair_bias = jnp.einsum('ijc,ch->hij', pair_ln.astype(jnp.float32), couple_offset_factor.astype(jnp.float32)).astype(jnp.bfloat16)
    res_float = amino_present.astype(jnp.float32)
    row_bias = pair_bias.astype(jnp.float32) + NEG * (res_float - 1.0)[None, None, :]

    def one_row(parts):
        return attend(parts[0], parts[1], parts[2], parts[3], row_bias)
    horizontal_mixed_result = lax.map(one_row, row_parts)
    horizontal_reshaped = horizontal_mixed_result.reshape(RELATIVE_CHAINS, PROTEIN_SITES, FOCUS_GROUPS * GROUP_BREADTH)
    homolog_stack_lone = (related_chain_embedding.astype(jnp.float32) + jnp.dot(horizontal_reshaped, across_chain_closing_transform, preferred_element_type=jnp.float32)).astype(jnp.bfloat16)
    column_normalized = standardize_features(homolog_stack_lone).astype(jnp.bfloat16)
    col_parts = tuple((jnp.swapaxes(part, 0, 1) for part in project_four(column_normalized, vertical_query_factors)))
    col_bias = (NEG * (homolog_present.astype(jnp.float32) - 1.0))[None, None, :]

    def one_column(parts):
        return attend(parts[0], parts[1], parts[2], parts[3], col_bias)
    col_mixed = lax.map(one_column, col_parts)
    produced_tensor = down_position_closing_transform.astype(jnp.float32).reshape(FOCUS_GROUPS, GROUP_BREADTH, EMBED_LANES)
    column_delta = jnp.einsum('rshd,hdz->srz', col_mixed.astype(jnp.float32), produced_tensor)
    alignment_output = (homolog_stack_lone.astype(jnp.float32) + column_delta).astype(jnp.bfloat16)
    pair_mask = res_float[:, None] * res_float[None, :]
    pair_float = pair_ln.astype(jnp.float32)

    def gated_side(gate_weight, value_weight):
        gate = jnp.einsum('ikd,dc->cik', pair_float, gate_weight.astype(jnp.float32))
        value = jnp.einsum('ikd,dc->cik', pair_float, value_weight.astype(jnp.float32))
        return (jax.nn.sigmoid(gate) * value * pair_mask[None]).astype(jnp.bfloat16)
    left = gated_side(trilateral_left_right_factors[0], trilateral_left_right_factors[1])
    right = gated_side(trilateral_left_right_factors[2], trilateral_left_right_factors[3])
    product = jnp.einsum('cik,cjk->cij', left.astype(jnp.float32), right.astype(jnp.float32))
    mean = lax.optimization_barrier(jnp.mean(product, axis=0))
    square = lax.optimization_barrier(jnp.mean(product * product, axis=0))
    scaled = ((product - mean) * lax.rsqrt(square - mean * mean + EPS)).astype(jnp.bfloat16)
    tri_update = jnp.einsum('cij,cz->ijz', scaled.astype(jnp.float32), trilateral_final_factor.astype(jnp.float32))
    gate_out = jax.nn.sigmoid(jnp.dot(pair_ln, trilateral_sigmoid_factor, preferred_element_type=jnp.float32))
    pair_output = (couple_representation.astype(jnp.float32) + gate_out * tri_update).astype(jnp.bfloat16)
    return (alignment_output, pair_output)
```

```python
import jax
import jax.numpy as jnp
from jax import lax
from jax.sharding import Mesh
from jax.sharding import PartitionSpec as P

GROUP_BREADTH = 32
CHIPS = ("dap_0", "dap_1", "dap_2")
CORE = "dap_3"
DAP = CHIPS + (CORE,)

EPS = 1e-05
NEG = 1000000000.0


def sent_to_all(value, axis):
    copies = jnp.broadcast_to(value, (lax.axis_size(axis), *value.shape))
    return lax.all_to_all(copies, axis, split_axis=0, concat_axis=0, tiled=True)


def standardize_features(values):
    values = values.astype(jnp.float32)
    center = jnp.mean(values, axis=-1, keepdims=True)
    spread = jnp.mean(jnp.square(values - center), axis=-1, keepdims=True)
    return (values - center) * lax.rsqrt(spread + EPS)


def from_other_rep(arrays):
    sizes = [a.size for a in arrays]
    packed = jnp.concatenate([a.reshape(-1) for a in arrays])
    deep = lax.axis_size("dap_0")
    pairs = []
    for z in range(deep):
        for r in range(2):
            pairs.append((z * 2 + r, (deep - 1 - z) * 2 + (1 - r)))
    got = lax.ppermute(packed, ("dap_0", "rep"), pairs)
    outs, at = [], 0
    for a, n in zip(arrays, sizes):
        outs.append(got[at : at + n].reshape(a.shape))
        at += n
    return outs


def attend(query, keys, values, gate, bias):
    heads = query.shape[-1] // GROUP_BREADTH

    def split(x):
        return x.reshape(x.shape[0], heads, GROUP_BREADTH)

    scores = (
        jnp.einsum("qhd,khd->hqk", split(query), split(keys), preferred_element_type=jnp.float32)
        / jnp.sqrt(jnp.float32(GROUP_BREADTH))
        + bias
    )
    weights = jax.nn.softmax(scores, axis=-1).astype(jnp.bfloat16)
    mixed = jnp.einsum("hqk,khd->qhd", weights, split(values), preferred_element_type=jnp.float32)
    gated = mixed * jax.nn.sigmoid(split(gate).astype(jnp.float32))
    return gated.astype(jnp.bfloat16).reshape(query.shape)


def per_device(
    msa,
    pair,
    homolog_present,
    amino_present,
    row_w,
    row_out,
    offset_w,
    col_w,
    col_out,
    side_w,
    final_w,
    sigmoid_w,
):
    rep = lax.axis_index("rep")
    rows_here, sites = pair.shape[0], pair.shape[1]
    seqs_here, embed = msa.shape[0], msa.shape[2]
    chips = lax.axis_size(CHIPS)
    devices = lax.axis_size(DAP)
    row_start = lax.axis_index(DAP) * rows_here
    res_float = amino_present.astype(jnp.float32)
    mask_rows = lax.dynamic_slice_in_dim(res_float, row_start, rows_here, 0)

    offset_o, side_o, final_o = from_other_rep([offset_w, side_w, final_w])
    row_w_o, row_out_o = from_other_rep([row_w, row_out])
    col_w_o, col_out_o = from_other_rep([col_w, col_out])
    offset_all = jnp.concatenate([offset_w, offset_o], 1)
    side_all = jnp.concatenate([side_w, side_o], 2)
    row_all = jnp.concatenate([row_w, row_w_o], 2)
    row_out_all = jnp.concatenate([row_out, row_out_o], 0)
    col_all = jnp.concatenate([col_w, col_w_o], 2)
    col_out_all = jnp.concatenate([col_out, col_out_o], 0)
    final_all = jnp.concatenate([final_w, final_o], 0)

    pair_ln = standardize_features(pair).astype(jnp.bfloat16)
    local_bias = jnp.einsum(
        "ijc,ch->hij", pair_ln, offset_all, preferred_element_type=jnp.float32
    ).astype(jnp.bfloat16)
    heads = local_bias.shape[0]
    near = lax.all_to_all(local_bias.reshape(2, heads // 2, rows_here, sites), CORE, 0, 0, tiled=True)
    mine = lax.dynamic_index_in_dim(near, rep, 0, keepdims=False)
    far = sent_to_all(mine, CHIPS)
    both = sent_to_all(far, CORE)
    pair_bias = both.transpose(0, 2, 1, 3, 4).reshape(heads, chips * rows_here, sites)
    row_bias = pair_bias.astype(jnp.float32) + NEG * (res_float - 1.0)[None, None, :]

    pair_mask = mask_rows[:, None] * res_float[None, :]

    def gated_side(gate_weight, value_weight):
        gate = jnp.einsum("ikd,dc->cik", pair_ln, gate_weight, preferred_element_type=jnp.float32)
        value = jnp.einsum("ikd,dc->cik", pair_ln, value_weight, preferred_element_type=jnp.float32)
        return (jax.nn.sigmoid(gate) * value * pair_mask[None]).astype(jnp.bfloat16)

    sides = jnp.stack([gated_side(side_all[0], side_all[1]), gated_side(side_all[2], side_all[3])], 1)
    sides = lax.all_to_all(sides, DAP, 0, 0, tiled=True)
    sides = sides.transpose(1, 0, 2, 3).reshape(2, devices * rows_here, sites)
    product = jnp.einsum("ik,jk->ij", sides[0], sides[1], preferred_element_type=jnp.float32)
    product = product.astype(jnp.bfloat16).reshape(devices, rows_here, sites)
    product = lax.all_to_all(product, DAP, 0, 0, tiled=True).astype(jnp.float32)

    normed = standardize_features(msa).astype(jnp.bfloat16)

    def of_rep(x):
        blocks = x.reshape(seqs_here, chips, 2, rows_here, embed)
        return lax.dynamic_index_in_dim(blocks, rep, 2, keepdims=False).reshape(
            seqs_here, chips * rows_here, embed
        )

    def project(x, weight):
        return jnp.dot(x, weight, preferred_element_type=jnp.float32).astype(jnp.bfloat16)

    normed_q = of_rep(normed)
    row_parts = (
        project(normed_q, row_all[0]),
        project(normed, row_all[1]),
        project(normed, row_all[2]),
        project(normed_q, row_all[3]),
    )
    row_mixed = lax.map(lambda parts: attend(*parts, row_bias), row_parts)
    msa_one = (
        of_rep(msa).astype(jnp.float32)
        + jnp.dot(row_mixed, row_out_all, preferred_element_type=jnp.float32)
    ).astype(jnp.bfloat16)

    blocks = msa_one.reshape(seqs_here, chips, rows_here, embed).transpose(1, 0, 2, 3)
    blocks = jnp.broadcast_to(blocks[:, None], (chips, 2, *blocks.shape[1:]))
    blocks = blocks.reshape(chips * 2, *blocks.shape[2:])
    blocks = lax.all_to_all(blocks, CHIPS + ("rep",), 0, 0, tiled=True)
    blocks = blocks.reshape(chips, 2, *blocks.shape[1:]).swapaxes(0, 1)
    blocks = lax.all_to_all(blocks, CORE, 0, 0, tiled=True)
    column = blocks.transpose(1, 0, 2, 3, 4).reshape(-1, rows_here, embed)

    column_normed = standardize_features(column).astype(jnp.bfloat16).swapaxes(0, 1)
    col_parts = tuple(project(column_normed, col_all[n]) for n in range(4))
    col_bias = (NEG * (homolog_present.astype(jnp.float32) - 1.0))[None, None, :]
    col_mixed = lax.map(lambda parts: attend(*parts, col_bias), col_parts)
    width = embed // 2
    col_half = lax.dynamic_slice_in_dim(col_out_all, rep * width, width, 1)
    column_delta = jnp.einsum("rsd,dz->srz", col_mixed, col_half, preferred_element_type=jnp.float32)
    retained = lax.dynamic_slice_in_dim(column, rep * width, width, 2)
    alignment_output = (retained.astype(jnp.float32) + column_delta).astype(jnp.bfloat16)

    mean = jnp.mean(product, axis=0)
    square = jnp.mean(product * product, axis=0)
    scaled = ((product - mean) * lax.rsqrt(square - mean * mean + EPS)).astype(jnp.bfloat16)
    half = pair.shape[2] // 2
    final_half = lax.dynamic_slice_in_dim(final_all, rep * half, half, 1)
    tri_update = jnp.einsum("cij,cz->ijz", scaled, final_half, preferred_element_type=jnp.float32)
    pair_half = lax.dynamic_slice_in_dim(pair, rep * half, half, 2)
    gate_out = jax.nn.sigmoid(jnp.dot(pair_ln, sigmoid_w, preferred_element_type=jnp.float32))
    pair_output = (pair_half.astype(jnp.float32) + gate_out * tri_update).astype(jnp.bfloat16)
    return (alignment_output, pair_output)


def solution(mesh):
    finer = Mesh(
        mesh.devices.reshape(4, 4, 4, 2, mesh.shape["rep"]),
        (*DAP, "rep"),
    )
    return jax.shard_map(
        per_device,
        mesh=finer,
        in_specs=(
            P(DAP, None, None),
            P(DAP, None, None),
            P(),
            P(),
            P(None, None, "rep"),
            P("rep", None),
            P(None, "rep"),
            P(None, None, "rep"),
            P("rep", None),
            P(None, None, "rep"),
            P("rep", None),
            P(None, "rep"),
        ),
        out_specs=(P(None, DAP, "rep"), P(DAP, None, "rep")),
        check_vma=False,
    )
```

```python
import functools

import jax
import jax.numpy as jnp
from jax import lax
from jax.experimental import pallas as pl
from jax.experimental.pallas import tpu as pltpu
from jax.sharding import Mesh
from jax.sharding import PartitionSpec as P

GROUP_BREADTH = 32
CHIPS = ("dap_0", "dap_1", "dap_2")
CORE = "dap_3"
DAP = CHIPS + (CORE,)
MESH = pl.DeviceIdType.MESH
VMEM = pl.BlockSpec(memory_space=pltpu.VMEM)

EPS = 1e-05
NEG = 1000000000.0


def standardize_features(values):
    values = values.astype(jnp.float32)
    center = jnp.mean(values, axis=-1, keepdims=True)
    spread = jnp.mean(jnp.square(values - center), axis=-1, keepdims=True)
    return (values - center) * lax.rsqrt(spread + EPS)


def place():
    z, x, y = (lax.axis_index(a) for a in CHIPS)
    return z, x, y, lax.axis_index(CORE), lax.axis_index("rep")


def send(src, dst, sent, came, device):
    pltpu.make_async_remote_copy(
        src_ref=src, dst_ref=dst, send_sem=sent, recv_sem=came, device_id=device, device_id_type=MESH
    ).start()


def wait_bytes(ref, sem):
    pltpu.make_async_copy(ref, ref, sem).wait()


def first_exchange(
    bias,
    sides,
    row_w,
    col_w,
    row_o,
    col_o,
    final,
    bias_all,
    sides_all,
    row_wx,
    col_wx,
    row_ox,
    col_ox,
    final_x,
    s_sent,
    s_came,
    line_sent,
    line_came,
    plane_sent,
    plane_came,
    core_sent,
    core_came,
):
    z, x, y, c, r = place()
    deep, wide, high = 4, 4, 4
    plane = wide * high
    xy = x * high + y
    chip = z * plane + xy
    chunk = row_w.shape[0] // (2 * plane)
    mine = pl.ds(pl.multiple_of((c * plane + xy) * chunk, chunk), chunk)
    half = pl.ds(pl.multiple_of(c * plane * chunk, plane * chunk), plane * chunk)
    mirror = (deep - 1 - z, x, y, c, 1 - r)
    partner = (z, x, y, 1 - c, r)

    for dz in range(deep):
        zt = lax.rem(z + dz, deep)
        if dz == 0:

            @pl.when(c != r)
            def _():
                send(bias, bias_all.at[r, xy, z], line_sent.at[0], line_came.at[0], (zt, x, y, r, c))

            @pl.when(c == r)
            def _():
                bias_all[r, xy, z] = bias[...]

        else:
            send(bias, bias_all.at[r, xy, z], line_sent.at[0], line_came.at[0], (zt, x, y, r, c))
    send(row_w.at[mine], row_wx.at[mine], line_sent.at[1], line_came.at[1], mirror)
    send(col_w.at[mine], col_wx.at[mine], line_sent.at[2], line_came.at[2], mirror)
    o_half = pl.ds(pl.multiple_of(c * (row_o.shape[0] // 2), row_o.shape[0] // 2), row_o.shape[0] // 2)
    send(row_o.at[o_half], row_ox.at[o_half], line_sent.at[3], line_came.at[3], mirror)
    send(col_o.at[o_half], col_ox.at[o_half], line_sent.at[4], line_came.at[4], mirror)
    send(final, final_x, line_sent.at[5], line_came.at[5], mirror)

    me = chip * 2 + c
    chips = deep * plane
    sides_all[me] = sides[chip]
    send(sides.at[chip], sides_all.at[me], s_sent, s_came, partner)

    def to_owner(i, carry):
        to = lax.rem(chip + i, chips)
        zt, xt, yt = to // plane, lax.rem(to // high, wide), lax.rem(to, high)
        send(sides.at[to], sides_all.at[me], s_sent, s_came, (zt, xt, yt, 0, r))
        send(sides.at[to], sides_all.at[me], s_sent, s_came, (zt, xt, yt, 1, r))
        return carry

    lax.fori_loop(1, chips // 2, to_owner, 0)

    @pl.when(c == r)
    def _():
        wait_bytes(bias_all.at[0, 0, pl.ds(0, deep - 1)], line_came.at[0])

    @pl.when(c != r)
    def _():
        wait_bytes(bias_all.at[0, 0], line_came.at[0])

    wait_bytes(row_wx.at[mine], line_came.at[1])
    wait_bytes(col_wx.at[mine], line_came.at[2])

    def over_plane(i, carry):
        to = lax.rem(xy + i, plane)
        device = (z, to // high, lax.rem(to, high), c, r)
        send(bias_all.at[c, xy], bias_all.at[c, xy], plane_sent.at[0], plane_came.at[0], device)
        send(row_wx.at[mine], row_wx.at[mine], plane_sent.at[1], plane_came.at[1], device)
        send(col_wx.at[mine], col_wx.at[mine], plane_sent.at[2], plane_came.at[2], device)
        return carry

    lax.fori_loop(1, plane, over_plane, 0)
    lax.fori_loop(chips // 2, chips, to_owner, 0)

    rest = pl.ds(0, (plane - 1) * chunk)
    wait_bytes(row_ox.at[o_half], line_came.at[3])
    send(row_ox.at[o_half], row_ox.at[o_half], core_sent.at[3], core_came.at[3], partner)
    wait_bytes(col_ox.at[o_half], line_came.at[4])
    send(col_ox.at[o_half], col_ox.at[o_half], core_sent.at[4], core_came.at[4], partner)
    wait_bytes(bias_all.at[0, pl.ds(0, plane - 1)], plane_came.at[0])
    send(bias_all.at[c], bias_all.at[c], core_sent.at[0], core_came.at[0], partner)
    wait_bytes(row_wx.at[rest], plane_came.at[1])
    send(row_wx.at[half], row_wx.at[half], core_sent.at[1], core_came.at[1], partner)
    wait_bytes(col_wx.at[rest], plane_came.at[2])
    send(col_wx.at[half], col_wx.at[half], core_sent.at[2], core_came.at[2], partner)

    wait_bytes(final_x, line_came.at[5])
    wait_bytes(bias_all.at[0], core_came.at[0])
    wait_bytes(row_wx.at[half], core_came.at[1])
    wait_bytes(col_wx.at[half], core_came.at[2])
    wait_bytes(row_ox.at[o_half], core_came.at[3])
    wait_bytes(col_ox.at[o_half], core_came.at[4])
    wait_bytes(sides_all.at[pl.ds(0, 2 * chips - 1)], s_came)

    @pl.when(c == r)
    def _():
        wait_bytes(bias_all.at[0, 0, pl.ds(0, deep - 1)], line_sent.at[0])

    @pl.when(c != r)
    def _():
        wait_bytes(bias_all.at[0, 0], line_sent.at[0])

    wait_bytes(row_wx.at[mine], line_sent.at[1])
    wait_bytes(col_wx.at[mine], line_sent.at[2])
    wait_bytes(row_ox.at[o_half], line_sent.at[3])
    wait_bytes(col_ox.at[o_half], line_sent.at[4])
    wait_bytes(final_x, line_sent.at[5])
    wait_bytes(bias_all.at[0, pl.ds(0, plane - 1)], plane_sent.at[0])
    wait_bytes(row_wx.at[rest], plane_sent.at[1])
    wait_bytes(col_wx.at[rest], plane_sent.at[2])
    wait_bytes(bias_all.at[0], core_sent.at[0])
    wait_bytes(row_wx.at[half], core_sent.at[1])
    wait_bytes(col_wx.at[half], core_sent.at[2])
    wait_bytes(row_ox.at[o_half], core_sent.at[3])
    wait_bytes(col_ox.at[o_half], core_sent.at[4])
    wait_bytes(sides_all.at[pl.ds(0, 2 * chips - 1)], s_sent)


def second_exchange(seqs, rows, column, product, m_sent, m_came, p_sent, p_came):
    z, x, y, c, r = place()
    wide, high = 4, 4
    plane = wide * high
    chips = seqs.shape[0]
    chip = z * plane + x * high + y
    me = chip * 2 + c
    channel = r * chips + chip

    @pl.when(c == r)
    def _():
        column[me] = seqs[chip]

    @pl.when(c != r)
    def _():
        send(seqs.at[chip], column.at[me], m_sent, m_came, (z, x, y, r, r))

    send(seqs.at[chip], column.at[me], m_sent, m_came, (z, x, y, r, 1 - r))
    product[channel] = rows[chip]
    send(rows.at[chip], product.at[channel], p_sent, p_came, (z, x, y, c, 1 - r))

    def to_owner(i, carry):
        to = lax.rem(chip + i, chips)
        zt, xt, yt = to // plane, lax.rem(to // high, wide), lax.rem(to, high)
        for rt in range(2):
            send(seqs.at[to], column.at[me], m_sent, m_came, (zt, xt, yt, r, rt))
        return carry

    def to_rows(i, carry):
        to = lax.rem(chip + i, chips)
        zt, xt, yt = to // plane, lax.rem(to // high, wide), lax.rem(to, high)
        for rt in range(2):
            send(rows.at[to], product.at[channel], p_sent, p_came, (zt, xt, yt, c, rt))
        return carry

    lax.fori_loop(1, chips, to_owner, 0)
    lax.fori_loop(1, chips, to_rows, 0)

    for sem in (m_came, m_sent):


        @pl.when(c == r)
        def _():
            wait_bytes(column.at[pl.ds(0, 2 * chips - 1)], sem)

        @pl.when(c != r)
        def _():
            wait_bytes(column, sem)

    for sem in (p_came, p_sent):
        wait_bytes(product.at[pl.ds(0, 2 * chips - 1)], sem)


def exchange(kernel, outs, semaphores, *operands):
    return pl.pallas_call(
        kernel,
        out_shape=[jax.ShapeDtypeStruct(s, jnp.bfloat16) for s in outs],
        in_specs=[VMEM] * len(operands),
        out_specs=[VMEM] * len(outs),
        scratch_shapes=[
            pltpu.SemaphoreType.DMA if n == 0 else pltpu.SemaphoreType.DMA((n,)) for n in semaphores
        ],
        compiler_params=pltpu.CompilerParams(has_side_effects=True, vmem_limit_bytes=40 << 20),
    )(*operands)


def dot_last(a, b):
    return lax.dot_general(a, b, (((1,), (1,)), ((), ())), preferred_element_type=jnp.float32)


def dot(a, b):
    return jnp.dot(a, b, preferred_element_type=jnp.float32)


def project(x, own, other):
    return jnp.concatenate([dot(x, own), dot(x, other)], 1).astype(jnp.bfloat16)


def attend_rows(q, k, v, g, bias, mixed, block, heads):
    embed = q.shape[1]
    queries = q.shape[0]
    lane = lax.broadcasted_iota(jnp.int32, (heads, embed), 1) // GROUP_BREADTH
    head = lax.broadcasted_iota(jnp.int32, (heads, embed), 0)
    own = (lane == head).astype(jnp.float32)[None]
    scale = 1.0 / jnp.sqrt(jnp.float32(GROUP_BREADTH))

    for n in range(queries // block):
        part = slice(n * block, (n + 1) * block)
        wide = q[part].astype(jnp.float32)[:, None, :] * own
        wide = wide.reshape(block * heads, embed).astype(jnp.bfloat16)
        scores = dot_last(wide, k) * scale + bias(n)
        scores = jnp.exp(scores - jnp.max(scores, axis=1, keepdims=True))
        weights = (scores * (1.0 / jnp.sum(scores, axis=1, keepdims=True))).astype(jnp.bfloat16)
        out = dot(weights, v).reshape(block, heads, embed) * own
        out = jnp.sum(out, axis=1)
        gate = 1.0 / (1.0 + jnp.exp(-g[part].astype(jnp.float32)))
        mixed[part, :] = (out * gate).astype(jnp.bfloat16)


def row_kernel(
    msa, msa_q, bias_all, hidden, w, wx, wo, wox, out, bias_rows, mixed, *, heads, block
):
    r = lax.axis_index("rep")
    planes, deep = bias_all.shape[1], bias_all.shape[2]
    rows = bias_rows.shape[0] // (planes * deep)
    sites = bias_rows.shape[2]
    away = hidden[...]

    def place_bias(p, carry):
        at, level = lax.rem(p, planes), p // planes
        both = jnp.concatenate(
            [
                bias_all[r, at, level].astype(jnp.float32),
                bias_all[1 - r, at, level].astype(jnp.float32),
            ],
            0,
        )
        for t in range(rows):
            bias_rows[p * rows + t] = both[:, t * sites : (t + 1) * sites] + away
        return carry

    lax.fori_loop(0, planes * deep, place_bias, 0)

    def one(s, carry):
        x = standardize_features(msa[s]).astype(jnp.bfloat16)
        xq = standardize_features(msa_q[s]).astype(jnp.bfloat16)
        q = project(xq, w[0], wx[0])
        k = project(x, w[1], wx[1])
        v = project(x, w[2], wx[2])
        g = project(xq, w[3], wx[3])

        def bias(n):
            return bias_rows[n * block : (n + 1) * block].reshape(block * heads, sites)

        attend_rows(q, k, v, g, bias, mixed, block, heads)
        half = wo.shape[0]
        delta = dot(mixed[:, :half], wo[...]) + dot(mixed[:, half:], wox[...])
        out[s] = (msa_q[s].astype(jnp.float32) + delta).astype(jnp.bfloat16)
        return carry

    lax.fori_loop(0, msa.shape[0], one, 0)


def col_kernel(column, hidden, w, wx, wo, wox, out, mixed, *, heads, block):
    r = lax.axis_index("rep")
    embed = w.shape[1]
    width = embed // 2
    at = pl.ds(pl.multiple_of(r * width, width), width)
    away = hidden[...]
    for t in range(column.shape[1] // embed):
        x = standardize_features(column[:, t * embed : (t + 1) * embed]).astype(jnp.bfloat16)
        q, k, v, g = [project(x, w[n], wx[n]) for n in range(4)]
        attend_rows(q, k, v, g, lambda n: away, mixed, block, heads)
        half = wo.shape[0]
        delta = dot(mixed[:, :half], wo[:, at]) + dot(mixed[:, half:], wox[:, at])
        keep = column[:, pl.ds(pl.multiple_of(t * embed + r * width, width), width)]
        out[:, t * width : (t + 1) * width] = (keep.astype(jnp.float32) + delta).astype(jnp.bfloat16)


def local_call(kernel, out, scratch, flops, *operands):
    return pl.pallas_call(
        kernel,
        out_shape=jax.ShapeDtypeStruct(out, jnp.bfloat16),
        in_specs=[VMEM] * len(operands),
        out_specs=VMEM,
        scratch_shapes=[pltpu.VMEM(*s) for s in scratch],
        compiler_params=pltpu.CompilerParams(vmem_limit_bytes=40 << 20),
        cost_estimate=pl.CostEstimate(flops=flops, bytes_accessed=4 << 20, transcendentals=0),
    )(*operands)


def per_device(
    msa,
    pair,
    homolog_present,
    amino_present,
    row_w,
    row_out,
    offset_w,
    col_w,
    col_out,
    side_w,
    final_w,
    sigmoid_w,
):
    rep = lax.axis_index("rep")
    core = lax.axis_index(CORE)
    rows_here, sites, channels = pair.shape
    seqs_here, embed = msa.shape[0], msa.shape[2]
    chips = lax.axis_size(CHIPS)
    devices = lax.axis_size(DAP)
    heads_here = offset_w.shape[1]
    heads = 2 * heads_here
    row_start = lax.axis_index(DAP) * rows_here
    res_float = amino_present.astype(jnp.float32)
    mask_rows = lax.dynamic_slice_in_dim(res_float, row_start, rows_here, 0)
    flat = rows_here * sites

    pair_ln = standardize_features(pair).astype(jnp.bfloat16).reshape(flat, channels)
    bias = jnp.einsum("nc,ch->hn", pair_ln, offset_w, preferred_element_type=jnp.float32).astype(
        jnp.bfloat16
    )
    pair_mask = (mask_rows[:, None] * res_float[None, :]).reshape(1, flat)

    def gated_side(gate_weight, value_weight):
        gate = jnp.einsum("nd,dc->cn", pair_ln, gate_weight, preferred_element_type=jnp.float32)
        value = jnp.einsum("nd,dc->cn", pair_ln, value_weight, preferred_element_type=jnp.float32)
        return (jax.nn.sigmoid(gate) * value * pair_mask).astype(jnp.bfloat16)

    sides = jnp.stack([gated_side(side_w[0], side_w[1]), gated_side(side_w[2], side_w[3])], 1)

    weight_rows = row_w.shape[0] * row_w.shape[1]
    flat_w = (weight_rows, row_w.shape[2])
    bias_all, sides_all, row_wx, col_wx, row_ox, col_ox, final_x = exchange(
        first_exchange,
        [
            (2, 16, chips // 16, heads_here, flat),
            (devices, 2, flat),
            flat_w,
            flat_w,
            row_out.shape,
            col_out.shape,
            final_w.shape,
        ],
        [0, 0, 6, 6, 3, 3, 5, 5],
        bias,
        sides,
        row_w.reshape(flat_w),
        col_w.reshape(flat_w),
        row_out,
        col_out,
        final_w,
    )

    lefts = lax.dynamic_index_in_dim(sides_all[:, 0].reshape(chips, 2, flat), core, 1, keepdims=False)
    product = jnp.einsum(
        "ik,jk->ij",
        lefts.reshape(chips * rows_here, sites),
        sides_all[:, 1].reshape(devices * rows_here, sites),
        preferred_element_type=jnp.float32,
    )
    product = product.astype(jnp.bfloat16).reshape(chips, rows_here, sites)

    blocks = msa.reshape(seqs_here, chips, 2, rows_here, embed)
    msa_q = lax.dynamic_index_in_dim(blocks, rep, 2, keepdims=False)
    queries = chips * rows_here
    msa_q = msa_q.reshape(seqs_here, queries, embed)
    hidden = (NEG * (res_float - 1.0))[None, :]
    msa_one = local_call(
        functools.partial(row_kernel, heads=heads, block=24),
        (seqs_here, queries, embed),
        [((queries, heads, sites), jnp.float32), ((queries, embed), jnp.bfloat16)],
        3 << 30,
        msa,
        msa_q,
        bias_all,
        hidden,
        row_w,
        row_wx.reshape(row_w.shape),
        row_out,
        row_ox,
    )

    seq_blocks = msa_one.reshape(seqs_here, chips, rows_here * embed).swapaxes(0, 1)
    column, product = exchange(
        second_exchange,
        [(devices, seqs_here, rows_here * embed), (devices, rows_here, sites)],
        [0, 0, 0, 0],
        seq_blocks,
        product,
    )

    column = column.reshape(devices * seqs_here, rows_here * embed)
    away = (NEG * (homolog_present.astype(jnp.float32) - 1.0))[None, :]
    width = embed // 2
    alignment_output = local_call(
        functools.partial(col_kernel, heads=heads, block=32),
        (devices * seqs_here, rows_here * width),
        [((devices * seqs_here, embed), jnp.bfloat16)],
        3 << 30,
        column,
        away,
        col_w,
        col_wx.reshape(col_w.shape),
        col_out,
        col_ox,
    ).reshape(devices * seqs_here, rows_here, width)

    product = product.astype(jnp.float32)
    mean = jnp.mean(product, axis=0)
    square = jnp.mean(product * product, axis=0)
    scaled = ((product - mean) * lax.rsqrt(square - mean * mean + EPS)).astype(jnp.bfloat16)
    half = channels // 2
    first = jnp.where(rep == 0, final_w, final_x)
    second = jnp.where(rep == 0, final_x, final_w)
    final_all = jnp.concatenate([first, second], 0)
    final_half = lax.dynamic_slice_in_dim(final_all, rep * half, half, 1)
    tri_update = jnp.einsum("cij,cz->ijz", scaled, final_half, preferred_element_type=jnp.float32)
    pair_half = lax.dynamic_slice_in_dim(pair, rep * half, half, 2)
    gate_out = jax.nn.sigmoid(dot(pair_ln, sigmoid_w)).reshape(rows_here, sites, half)
    pair_output = (pair_half.astype(jnp.float32) + gate_out * tri_update).astype(jnp.bfloat16)
    return (alignment_output, pair_output)


def solution(mesh):
    finer = Mesh(
        mesh.devices.reshape(4, 4, 4, 2, mesh.shape["rep"]),
        (*DAP, "rep"),
    )
    return jax.shard_map(
        per_device,
        mesh=finer,
        in_specs=(
            P(DAP, None, None),
            P(DAP, None, None),
            P(),
            P(),
            P(None, None, "rep"),
            P("rep", None),
            P(None, "rep"),
            P(None, None, "rep"),
            P("rep", None),
            P(None, None, "rep"),
            P("rep", None),
            P(None, "rep"),
        ),
        out_specs=(P(None, DAP, "rep"), P(DAP, None, "rep")),
        check_vma=False,
    )
```

```python
import functools

import jax
import jax.numpy as jnp
from jax import lax
from jax.experimental import pallas as pl
from jax.experimental.pallas import tpu as pltpu
from jax.sharding import Mesh
from jax.sharding import PartitionSpec as P

GROUP_BREADTH = 32
CHIPS = ("dap_0", "dap_1", "dap_2")
CORE = "dap_3"
DAP = CHIPS + (CORE,)
MESH = pl.DeviceIdType.MESH
VMEM = pl.BlockSpec(memory_space=pltpu.VMEM)

EPS = 1e-05
NEG = 1000000000.0


def standardize_features(values):
    values = values.astype(jnp.float32)
    center = jnp.mean(values, axis=-1, keepdims=True)
    spread = jnp.mean(jnp.square(values - center), axis=-1, keepdims=True)
    return (values - center) * lax.rsqrt(spread + EPS)


def place():
    z, x, y = (lax.axis_index(a) for a in CHIPS)
    return z, x, y, lax.axis_index(CORE), lax.axis_index("rep")


def send(src, dst, sent, came, device):
    pltpu.make_async_remote_copy(
        src_ref=src, dst_ref=dst, send_sem=sent, recv_sem=came, device_id=device, device_id_type=MESH
    ).start()


def wait_bytes(ref, sem):
    pltpu.make_async_copy(ref, ref, sem).wait()


def greet(device):
    pl.semaphore_signal(pltpu.get_barrier_semaphore(), inc=1, device_id=device, device_id_type=MESH)


def chip_at(to):
    plane, high = 16, 4
    return to // plane, lax.rem(to // high, high), lax.rem(to, high)


def first_exchange(
    bias,
    sides,
    row_w,
    col_w,
    row_o,
    col_o,
    final,
    bias_all,
    sides_all,
    row_wx,
    col_wx,
    row_ox,
    col_ox,
    final_x,
    s_sent,
    s_came,
    line_sent,
    line_came,
    bias_sent,
    bias_came,
    row_sent,
    row_came,
    col_sent,
    col_came,
    core_sent,
    core_came,
):
    z, x, y, c, r = place()
    deep, high = 4, 4
    plane = high * high
    chips = deep * plane
    xy = x * high + y
    chip = z * plane + xy
    chunk = row_w.shape[0] // (2 * plane)
    mirror = (deep - 1 - z, x, y, c, 1 - r)
    partner = (z, x, y, 1 - c, r)

    def rows_of(at):
        return pl.ds(pl.multiple_of((c * plane + at) * chunk, chunk), chunk)

    mine = rows_of(xy)

    def greet_group(i, carry):
        greet((*chip_at(lax.rem(chip + i, chips)), c, r))
        return carry

    lax.fori_loop(1, chips, greet_group, 0)
    greet(mirror)
    greet(partner)
    for zt in range(deep):

        @pl.when(c != r)
        def _():
            greet((zt, x, y, r, c))

    sides_all[c, chip] = sides[chip]

    @pl.when(c == r)
    def _():
        bias_all[r, xy, z] = bias[...]
        pl.semaphore_wait(pltpu.get_barrier_semaphore(), chips + 1)

    @pl.when(c != r)
    def _():
        pl.semaphore_wait(pltpu.get_barrier_semaphore(), chips + 1 + deep)

    for dz in range(deep):
        zt = lax.rem(z + dz, deep)
        if dz == 0:

            @pl.when(c != r)
            def _():
                send(bias, bias_all.at[r, xy, z], line_sent.at[0], line_came.at[0], (zt, x, y, r, c))

        else:
            send(bias, bias_all.at[r, xy, z], line_sent.at[0], line_came.at[0], (zt, x, y, r, c))
    send(row_w.at[mine], row_wx.at[mine], line_sent.at[1], line_came.at[1], mirror)
    send(col_w.at[mine], col_wx.at[mine], line_sent.at[2], line_came.at[2], mirror)
    o_half = pl.ds(pl.multiple_of(c * (row_o.shape[0] // 2), row_o.shape[0] // 2), row_o.shape[0] // 2)
    send(row_o.at[o_half], row_ox.at[o_half], line_sent.at[3], line_came.at[3], mirror)
    send(col_o.at[o_half], col_ox.at[o_half], line_sent.at[4], line_came.at[4], mirror)
    send(final, final_x, line_sent.at[5], line_came.at[5], mirror)

    def to_owner(i, carry):
        to = lax.rem(chip + i, chips)
        send(sides.at[to], sides_all.at[c, chip], s_sent, s_came.at[z], (*chip_at(to), c, r))
        return carry

    lax.fori_loop(1, plane, to_owner, 0)

    @pl.when(c == r)
    def _():
        wait_bytes(bias_all.at[0, 0, pl.ds(0, deep - 1)], line_came.at[0])

    @pl.when(c != r)
    def _():
        wait_bytes(bias_all.at[0, 0], line_came.at[0])

    def plane_device(i):
        to = lax.rem(xy + i, plane)
        return (z, to // high, lax.rem(to, high), c, r)

    def bias_plane(i, carry):
        send(bias_all.at[c, xy], bias_all.at[c, xy], bias_sent, bias_came.at[xy], plane_device(i))
        return carry

    lax.fori_loop(1, plane, bias_plane, 0)
    wait_bytes(row_wx.at[mine], line_came.at[1])
    wait_bytes(col_wx.at[mine], line_came.at[2])

    def weight_plane(i, carry):
        device = plane_device(i)
        send(row_wx.at[mine], row_wx.at[mine], row_sent, row_came.at[xy], device)
        send(col_wx.at[mine], col_wx.at[mine], col_sent, col_came.at[xy], device)
        return carry

    lax.fori_loop(1, plane, weight_plane, 0)
    lax.fori_loop(plane, chips, to_owner, 0)

    send(bias_all.at[c, xy], bias_all.at[c, xy], core_sent.at[0], core_came.at[0], partner)
    send(row_wx.at[mine], row_wx.at[mine], core_sent.at[1], core_came.at[1], partner)
    send(col_wx.at[mine], col_wx.at[mine], core_sent.at[2], core_came.at[2], partner)
    wait_bytes(row_ox.at[o_half], line_came.at[3])
    send(row_ox.at[o_half], row_ox.at[o_half], core_sent.at[3], core_came.at[3], partner)
    wait_bytes(col_ox.at[o_half], line_came.at[4])
    send(col_ox.at[o_half], col_ox.at[o_half], core_sent.at[4], core_came.at[4], partner)

    def bias_core(i, carry):
        at = lax.rem(xy + i, plane)
        wait_bytes(bias_all.at[c, at], bias_came.at[at])
        send(bias_all.at[c, at], bias_all.at[c, at], core_sent.at[0], core_came.at[0], partner)
        return carry

    lax.fori_loop(1, plane, bias_core, 0)

    def weight_core(i, carry):
        at = lax.rem(xy + i, plane)
        rows = rows_of(at)
        wait_bytes(row_wx.at[rows], row_came.at[at])
        send(row_wx.at[rows], row_wx.at[rows], core_sent.at[1], core_came.at[1], partner)
        wait_bytes(col_wx.at[rows], col_came.at[at])
        send(col_wx.at[rows], col_wx.at[rows], core_sent.at[2], core_came.at[2], partner)
        return carry

    lax.fori_loop(1, plane, weight_core, 0)

    def pass_sides(level):
        for n in range(4):
            part = pl.ds(pl.multiple_of(level * plane + n * high, high), high)
            send(sides_all.at[c, part], sides_all.at[c, part], core_sent.at[5], core_came.at[5], partner)

    wait_bytes(sides_all.at[0, pl.ds(0, plane - 1)], s_came.at[z])
    pass_sides(z)
    for dz in range(1, deep):
        level = lax.rem(z + dz, deep)
        wait_bytes(sides_all.at[0, pl.ds(0, plane)], s_came.at[level])
        pass_sides(level)

    half = pl.ds(0, plane * chunk)
    rest = pl.ds(0, (plane - 1) * chunk)
    wait_bytes(final_x, line_came.at[5])
    for sems in (core_came, core_sent):
        wait_bytes(bias_all.at[0], sems.at[0])
        wait_bytes(row_wx.at[half], sems.at[1])
        wait_bytes(col_wx.at[half], sems.at[2])
        wait_bytes(row_ox.at[o_half], sems.at[3])
        wait_bytes(col_ox.at[o_half], sems.at[4])
        wait_bytes(sides_all.at[0], sems.at[5])

    @pl.when(c == r)
    def _():
        wait_bytes(bias_all.at[0, 0, pl.ds(0, deep - 1)], line_sent.at[0])

    @pl.when(c != r)
    def _():
        wait_bytes(bias_all.at[0, 0], line_sent.at[0])

    wait_bytes(row_wx.at[mine], line_sent.at[1])
    wait_bytes(col_wx.at[mine], line_sent.at[2])
    wait_bytes(row_ox.at[o_half], line_sent.at[3])
    wait_bytes(col_ox.at[o_half], line_sent.at[4])
    wait_bytes(final_x, line_sent.at[5])
    wait_bytes(bias_all.at[0, pl.ds(0, plane - 1)], bias_sent)
    wait_bytes(row_wx.at[rest], row_sent)
    wait_bytes(col_wx.at[rest], col_sent)
    wait_bytes(sides_all.at[0, pl.ds(0, chips - 1)], s_sent)


def second_exchange(seqs, rows, column, product, m_sent, m_came, p_sent, p_came):
    z, x, y, c, r = place()
    chips = seqs.shape[0]
    chip = z * 16 + x * 4 + y
    me = chip * 2 + c
    channel = r * chips + chip
    here = (z, x, y)
    barrier = pltpu.get_barrier_semaphore()

    def greet_chip(i, carry):
        there = chip_at(lax.rem(chip + i, chips))
        for ct in range(2):
            for rt in range(2):
                greet((*there, ct, rt))
        return carry

    greet((*here, 1 - c, r))
    greet((*here, c, 1 - r))
    greet((*here, 1 - c, 1 - r))
    lax.fori_loop(1, chips, greet_chip, 0)
    product[channel] = rows[chip]

    @pl.when(c == r)
    def _():
        column[me] = seqs[chip]

    pl.semaphore_wait(barrier, 4 * chips - 1)

    @pl.when(c != r)
    def _():
        send(seqs.at[chip], column.at[me], m_sent, m_came, (*here, r, r))

    send(seqs.at[chip], column.at[me], m_sent, m_came, (*here, r, 1 - r))

    def to_owner(i, carry):
        to = lax.rem(chip + i, chips)
        for rt in range(2):
            send(seqs.at[to], column.at[me], m_sent, m_came, (*chip_at(to), r, rt))
        return carry

    def to_rows(i, carry):
        to = lax.rem(chip + i, chips)
        for rt in range(2):
            send(rows.at[to], product.at[channel], p_sent, p_came, (*chip_at(to), c, rt))
        return carry

    lax.fori_loop(1, chips, to_owner, 0)
    send(rows.at[chip], product.at[channel], p_sent, p_came, (*here, c, 1 - r))
    lax.fori_loop(1, chips, to_rows, 0)

    for sem in (m_came, m_sent):

        @pl.when(c == r)
        def _():
            wait_bytes(column.at[pl.ds(0, 2 * chips - 1)], sem)

        @pl.when(c != r)
        def _():
            wait_bytes(column, sem)

    for sem in (p_came, p_sent):
        wait_bytes(product.at[pl.ds(0, 2 * chips - 1)], sem)


def exchange(kernel, number, outs, semaphores, *operands):
    return pl.pallas_call(
        kernel,
        out_shape=[jax.ShapeDtypeStruct(s, jnp.bfloat16) for s in outs],
        in_specs=[VMEM] * len(operands),
        out_specs=[VMEM] * len(outs),
        scratch_shapes=[
            pltpu.SemaphoreType.DMA if n == 0 else pltpu.SemaphoreType.DMA((n,)) for n in semaphores
        ],
        compiler_params=pltpu.CompilerParams(
            collective_id=number, has_side_effects=True, vmem_limit_bytes=40 << 20
        ),
    )(*operands)


def dot_last(a, b):
    return lax.dot_general(a, b, (((1,), (1,)), ((), ())), preferred_element_type=jnp.float32)


def dot(a, b):
    return jnp.dot(a, b, preferred_element_type=jnp.float32)


def project(x, own, other):
    return jnp.concatenate([dot(x, own), dot(x, other)], 1).astype(jnp.bfloat16)


def attend_rows(q, k, v, g, bias, mixed, block, heads):
    embed = q.shape[1]
    queries = q.shape[0]
    lane = lax.broadcasted_iota(jnp.int32, (heads, embed), 1) // GROUP_BREADTH
    head = lax.broadcasted_iota(jnp.int32, (heads, embed), 0)
    own = (lane == head).astype(jnp.float32)[None]
    scale = 1.0 / jnp.sqrt(jnp.float32(GROUP_BREADTH))

    for n in range(queries // block):
        part = slice(n * block, (n + 1) * block)
        wide = q[part].astype(jnp.float32)[:, None, :] * own
        wide = wide.reshape(block * heads, embed).astype(jnp.bfloat16)
        scores = dot_last(wide, k) * scale + bias(n)
        scores = jnp.exp(scores - jnp.max(scores, axis=1, keepdims=True))
        weights = (scores * (1.0 / jnp.sum(scores, axis=1, keepdims=True))).astype(jnp.bfloat16)
        out = dot(weights, v).reshape(block, heads, embed) * own
        out = jnp.sum(out, axis=1)
        gate = 1.0 / (1.0 + jnp.exp(-g[part].astype(jnp.float32)))
        mixed[part, :] = (out * gate).astype(jnp.bfloat16)


def row_kernel(
    msa, msa_q, bias_all, hidden, w, wx, wo, wox, out, bias_rows, mixed, *, heads, block
):
    r = lax.axis_index("rep")
    planes, deep = bias_all.shape[1], bias_all.shape[2]
    rows = bias_rows.shape[0] // (planes * deep)
    sites = bias_rows.shape[2]
    away = hidden[...]

    def place_bias(p, carry):
        at, level = lax.rem(p, planes), p // planes
        both = jnp.concatenate(
            [
                bias_all[r, at, level].astype(jnp.float32),
                bias_all[1 - r, at, level].astype(jnp.float32),
            ],
            0,
        )
        for t in range(rows):
            bias_rows[p * rows + t] = both[:, t * sites : (t + 1) * sites] + away
        return carry

    lax.fori_loop(0, planes * deep, place_bias, 0)

    def one(s, carry):
        x = standardize_features(msa[s]).astype(jnp.bfloat16)
        xq = standardize_features(msa_q[s]).astype(jnp.bfloat16)
        q = project(xq, w[0], wx[0])
        k = project(x, w[1], wx[1])
        v = project(x, w[2], wx[2])
        g = project(xq, w[3], wx[3])

        def bias(n):
            return bias_rows[n * block : (n + 1) * block].reshape(block * heads, sites)

        attend_rows(q, k, v, g, bias, mixed, block, heads)
        half = wo.shape[0]
        delta = dot(mixed[:, :half], wo[...]) + dot(mixed[:, half:], wox[...])
        out[s] = (msa_q[s].astype(jnp.float32) + delta).astype(jnp.bfloat16)
        return carry

    lax.fori_loop(0, msa.shape[0], one, 0)


def col_kernel(column, hidden, w, wx, wo, wox, out, mixed, *, heads, block):
    r = lax.axis_index("rep")
    embed = w.shape[1]
    width = embed // 2
    at = pl.ds(pl.multiple_of(r * width, width), width)
    away = hidden[...]
    for t in range(column.shape[1] // embed):
        x = standardize_features(column[:, t * embed : (t + 1) * embed]).astype(jnp.bfloat16)
        q, k, v, g = [project(x, w[n], wx[n]) for n in range(4)]
        attend_rows(q, k, v, g, lambda n: away, mixed, block, heads)
        half = wo.shape[0]
        delta = dot(mixed[:, :half], wo[:, at]) + dot(mixed[:, half:], wox[:, at])
        keep = column[:, pl.ds(pl.multiple_of(t * embed + r * width, width), width)]
        out[:, t * width : (t + 1) * width] = (keep.astype(jnp.float32) + delta).astype(jnp.bfloat16)


def local_call(kernel, out, scratch, flops, *operands):
    return pl.pallas_call(
        kernel,
        out_shape=jax.ShapeDtypeStruct(out, jnp.bfloat16),
        in_specs=[VMEM] * len(operands),
        out_specs=VMEM,
        scratch_shapes=[pltpu.VMEM(*s) for s in scratch],
        compiler_params=pltpu.CompilerParams(vmem_limit_bytes=40 << 20),
        cost_estimate=pl.CostEstimate(flops=flops, bytes_accessed=4 << 20, transcendentals=0),
    )(*operands)


def per_device(
    msa,
    pair,
    homolog_present,
    amino_present,
    row_w,
    row_out,
    offset_w,
    col_w,
    col_out,
    side_w,
    final_w,
    sigmoid_w,
):
    rep = lax.axis_index("rep")
    core = lax.axis_index(CORE)
    rows_here, sites, channels = pair.shape
    seqs_here, embed = msa.shape[0], msa.shape[2]
    chips = lax.axis_size(CHIPS)
    devices = lax.axis_size(DAP)
    heads_here = offset_w.shape[1]
    heads = 2 * heads_here
    row_start = lax.axis_index(DAP) * rows_here
    res_float = amino_present.astype(jnp.float32)
    mask_rows = lax.dynamic_slice_in_dim(res_float, row_start, rows_here, 0)
    flat = rows_here * sites

    pair_ln = standardize_features(pair).astype(jnp.bfloat16).reshape(flat, channels)
    bias = jnp.einsum("nc,ch->hn", pair_ln, offset_w, preferred_element_type=jnp.float32).astype(
        jnp.bfloat16
    )
    pair_mask = (mask_rows[:, None] * res_float[None, :]).reshape(1, flat)

    def gated_side(gate_weight, value_weight):
        gate = jnp.einsum("nd,dc->cn", pair_ln, gate_weight, preferred_element_type=jnp.float32)
        value = jnp.einsum("nd,dc->cn", pair_ln, value_weight, preferred_element_type=jnp.float32)
        return (jax.nn.sigmoid(gate) * value * pair_mask).astype(jnp.bfloat16)

    sides = jnp.stack([gated_side(side_w[0], side_w[1]), gated_side(side_w[2], side_w[3])], 1)

    weight_rows = row_w.shape[0] * row_w.shape[1]
    flat_w = (weight_rows, row_w.shape[2])
    bias_all, sides_all, row_wx, col_wx, row_ox, col_ox, final_x = exchange(
        first_exchange,
        0,
        [
            (2, 16, chips // 16, heads_here, flat),
            (2, chips, 2, flat),
            flat_w,
            flat_w,
            row_out.shape,
            col_out.shape,
            final_w.shape,
        ],
        [0, 4, 6, 6, 0, 16, 0, 16, 0, 16, 6, 6],
        bias,
        sides,
        row_w.reshape(flat_w),
        col_w.reshape(flat_w),
        row_out,
        col_out,
        final_w,
    )

    lefts = lax.dynamic_index_in_dim(sides_all, core, 0, keepdims=False)[:, 0]
    rights = sides_all[:, :, 1].swapaxes(0, 1)
    product = jnp.einsum(
        "ik,jk->ij",
        lefts.reshape(chips * rows_here, sites),
        rights.reshape(devices * rows_here, sites),
        preferred_element_type=jnp.float32,
    )
    product = product.astype(jnp.bfloat16).reshape(chips, rows_here, sites)

    blocks = msa.reshape(seqs_here, chips, 2, rows_here, embed)
    msa_q = lax.dynamic_index_in_dim(blocks, rep, 2, keepdims=False)
    queries = chips * rows_here
    msa_q = msa_q.reshape(seqs_here, queries, embed)
    hidden = (NEG * (res_float - 1.0))[None, :]
    msa_one = local_call(
        functools.partial(row_kernel, heads=heads, block=24),
        (seqs_here, queries, embed),
        [((queries, heads, sites), jnp.float32), ((queries, embed), jnp.bfloat16)],
        3 << 30,
        msa,
        msa_q,
        bias_all,
        hidden,
        row_w,
        row_wx.reshape(row_w.shape),
        row_out,
        row_ox,
    )

    seq_blocks = msa_one.reshape(seqs_here, chips, rows_here * embed).swapaxes(0, 1)
    column, product = exchange(
        second_exchange,
        1,
        [(devices, seqs_here, rows_here * embed), (devices, rows_here, sites)],
        [0, 0, 0, 0],
        seq_blocks,
        product,
    )

    column = column.reshape(devices * seqs_here, rows_here * embed)
    away = (NEG * (homolog_present.astype(jnp.float32) - 1.0))[None, :]
    width = embed // 2
    alignment_output = local_call(
        functools.partial(col_kernel, heads=heads, block=32),
        (devices * seqs_here, rows_here * width),
        [((devices * seqs_here, embed), jnp.bfloat16)],
        3 << 30,
        column,
        away,
        col_w,
        col_wx.reshape(col_w.shape),
        col_out,
        col_ox,
    ).reshape(devices * seqs_here, rows_here, width)

    product = product.astype(jnp.float32)
    mean = jnp.mean(product, axis=0)
    square = jnp.mean(product * product, axis=0)
    scaled = ((product - mean) * lax.rsqrt(square - mean * mean + EPS)).astype(jnp.bfloat16)
    half = channels // 2
    first = jnp.where(rep == 0, final_w, final_x)
    second = jnp.where(rep == 0, final_x, final_w)
    final_all = jnp.concatenate([first, second], 0)
    final_half = lax.dynamic_slice_in_dim(final_all, rep * half, half, 1)
    tri_update = jnp.einsum("cij,cz->ijz", scaled, final_half, preferred_element_type=jnp.float32)
    pair_half = lax.dynamic_slice_in_dim(pair, rep * half, half, 2)
    gate_out = jax.nn.sigmoid(dot(pair_ln, sigmoid_w)).reshape(rows_here, sites, half)
    pair_output = (pair_half.astype(jnp.float32) + gate_out * tri_update).astype(jnp.bfloat16)
    return (alignment_output, pair_output)


def solution(mesh):
    finer = Mesh(
        mesh.devices.reshape(4, 4, 4, 2, mesh.shape["rep"]),
        (*DAP, "rep"),
    )
    return jax.shard_map(
        per_device,
        mesh=finer,
        in_specs=(
            P(DAP, None, None),
            P(DAP, None, None),
            P(),
            P(),
            P(None, None, "rep"),
            P("rep", None),
            P(None, "rep"),
            P(None, None, "rep"),
            P("rep", None),
            P(None, None, "rep"),
            P("rep", None),
            P(None, "rep"),
        ),
        out_specs=(P(None, DAP, "rep"), P(DAP, None, "rep")),
        check_vma=False,
    )
```

```python
import functools

import jax
import jax.numpy as jnp
from jax import lax
from jax.experimental import pallas as pl
from jax.experimental.pallas import tpu as pltpu
from jax.sharding import Mesh
from jax.sharding import PartitionSpec as P

GROUP_BREADTH = 32
CHIPS = ("dap_0", "dap_1", "dap_2")
CORE = "dap_3"
DAP = CHIPS + (CORE,)
MESH = pl.DeviceIdType.MESH
VMEM = pl.BlockSpec(memory_space=pltpu.VMEM)

EPS = 1e-05
NEG = 1000000000.0


def standardize_features(values):
    values = values.astype(jnp.float32)
    center = jnp.mean(values, axis=-1, keepdims=True)
    spread = jnp.mean(jnp.square(values - center), axis=-1, keepdims=True)
    return (values - center) * lax.rsqrt(spread + EPS)


def place():
    z, x, y = (lax.axis_index(a) for a in CHIPS)
    return z, x, y, lax.axis_index(CORE), lax.axis_index("rep")


def send(src, dst, sent, came, device):
    pltpu.make_async_remote_copy(
        src_ref=src, dst_ref=dst, send_sem=sent, recv_sem=came, device_id=device, device_id_type=MESH
    ).start()


def wait_bytes(ref, sem):
    pltpu.make_async_copy(ref, ref, sem).wait()


def greet(device):
    pl.semaphore_signal(pltpu.get_barrier_semaphore(), inc=1, device_id=device, device_id_type=MESH)


def chip_at(to):
    plane, high = 16, 4
    return to // plane, lax.rem(to // high, high), lax.rem(to, high)


def first_exchange(
    bias,
    sides,
    row_w,
    col_w,
    row_o,
    col_o,
    final,
    bias_all,
    sides_all,
    row_wx,
    col_wx,
    row_ox,
    col_ox,
    final_x,
    s_sent,
    s_came,
    line_sent,
    line_came,
    bias_sent,
    bias_came,
    row_sent,
    row_came,
    col_sent,
    col_came,
    core_sent,
    core_came,
):
    z, x, y, c, r = place()
    deep, high = 4, 4
    plane = high * high
    chips = deep * plane
    xy = x * high + y
    chip = z * plane + xy
    chunk = row_w.shape[0] // (2 * plane)
    mirror = (deep - 1 - z, x, y, c, 1 - r)
    partner = (z, x, y, 1 - c, r)

    def rows_of(at):
        return pl.ds(pl.multiple_of((c * plane + at) * chunk, chunk), chunk)

    mine = rows_of(xy)

    def greet_group(i, carry):
        greet((*chip_at(lax.rem(chip + i, chips)), c, r))
        return carry

    lax.fori_loop(1, chips, greet_group, 0)
    greet(mirror)
    greet(partner)
    for zt in range(deep):

        @pl.when(c != r)
        def _():
            greet((zt, x, y, r, c))

    sides_all[c, chip] = sides[chip]

    @pl.when(c == r)
    def _():
        bias_all[r, xy, z] = bias[...]
        pl.semaphore_wait(pltpu.get_barrier_semaphore(), chips + 1)

    @pl.when(c != r)
    def _():
        pl.semaphore_wait(pltpu.get_barrier_semaphore(), chips + 1 + deep)

    for dz in range(deep):
        zt = lax.rem(z + dz, deep)
        if dz == 0:

            @pl.when(c != r)
            def _():
                send(bias, bias_all.at[r, xy, z], line_sent.at[0], line_came.at[0], (zt, x, y, r, c))

        else:
            send(bias, bias_all.at[r, xy, z], line_sent.at[0], line_came.at[0], (zt, x, y, r, c))
    send(row_w.at[mine], row_wx.at[mine], line_sent.at[1], line_came.at[1], mirror)
    send(col_w.at[mine], col_wx.at[mine], line_sent.at[2], line_came.at[2], mirror)
    o_half = pl.ds(pl.multiple_of(c * (row_o.shape[0] // 2), row_o.shape[0] // 2), row_o.shape[0] // 2)
    send(row_o.at[o_half], row_ox.at[o_half], line_sent.at[3], line_came.at[3], mirror)
    send(col_o.at[o_half], col_ox.at[o_half], line_sent.at[4], line_came.at[4], mirror)
    send(final, final_x, line_sent.at[5], line_came.at[5], mirror)

    def to_owner(i, carry):
        to = lax.rem(chip + i, chips)
        send(sides.at[to], sides_all.at[c, chip], s_sent, s_came.at[z], (*chip_at(to), c, r))
        return carry

    lax.fori_loop(1, plane, to_owner, 0)

    @pl.when(c == r)
    def _():
        wait_bytes(bias_all.at[0, 0, pl.ds(0, deep - 1)], line_came.at[0])

    @pl.when(c != r)
    def _():
        wait_bytes(bias_all.at[0, 0], line_came.at[0])

    def plane_device(i):
        to = lax.rem(xy + i, plane)
        return (z, to // high, lax.rem(to, high), c, r)

    def bias_plane(i, carry):
        send(bias_all.at[c, xy], bias_all.at[c, xy], bias_sent, bias_came.at[xy], plane_device(i))
        return carry

    lax.fori_loop(1, plane, bias_plane, 0)
    wait_bytes(row_wx.at[mine], line_came.at[1])
    wait_bytes(col_wx.at[mine], line_came.at[2])

    def weight_plane(i, carry):
        device = plane_device(i)
        send(row_wx.at[mine], row_wx.at[mine], row_sent, row_came.at[xy], device)
        send(col_wx.at[mine], col_wx.at[mine], col_sent, col_came.at[xy], device)
        return carry

    lax.fori_loop(1, plane, weight_plane, 0)
    lax.fori_loop(plane, chips, to_owner, 0)

    send(bias_all.at[c, xy], bias_all.at[c, xy], core_sent.at[0], core_came.at[0], partner)
    send(row_wx.at[mine], row_wx.at[mine], core_sent.at[1], core_came.at[1], partner)
    send(col_wx.at[mine], col_wx.at[mine], core_sent.at[2], core_came.at[2], partner)
    wait_bytes(row_ox.at[o_half], line_came.at[3])
    send(row_ox.at[o_half], row_ox.at[o_half], core_sent.at[3], core_came.at[3], partner)
    wait_bytes(col_ox.at[o_half], line_came.at[4])
    send(col_ox.at[o_half], col_ox.at[o_half], core_sent.at[4], core_came.at[4], partner)

    def bias_core(i, carry):
        at = lax.rem(xy + i, plane)
        wait_bytes(bias_all.at[c, at], bias_came.at[at])
        send(bias_all.at[c, at], bias_all.at[c, at], core_sent.at[0], core_came.at[0], partner)
        return carry

    lax.fori_loop(1, plane, bias_core, 0)

    def weight_core(i, carry):
        at = lax.rem(xy + i, plane)
        rows = rows_of(at)
        wait_bytes(row_wx.at[rows], row_came.at[at])
        send(row_wx.at[rows], row_wx.at[rows], core_sent.at[1], core_came.at[1], partner)
        wait_bytes(col_wx.at[rows], col_came.at[at])
        send(col_wx.at[rows], col_wx.at[rows], core_sent.at[2], core_came.at[2], partner)
        return carry

    lax.fori_loop(1, plane, weight_core, 0)

    def pass_sides(level):
        for n in range(4):
            part = pl.ds(pl.multiple_of(level * plane + n * high, high), high)
            send(sides_all.at[c, part], sides_all.at[c, part], core_sent.at[5], core_came.at[5], partner)

    wait_bytes(sides_all.at[0, pl.ds(0, plane - 1)], s_came.at[z])
    pass_sides(z)
    for dz in range(1, deep):
        level = lax.rem(z + dz, deep)
        wait_bytes(sides_all.at[0, pl.ds(0, plane)], s_came.at[level])
        pass_sides(level)

    half = pl.ds(0, plane * chunk)
    rest = pl.ds(0, (plane - 1) * chunk)
    wait_bytes(final_x, line_came.at[5])
    for sems in (core_came, core_sent):
        wait_bytes(bias_all.at[0], sems.at[0])
        wait_bytes(row_wx.at[half], sems.at[1])
        wait_bytes(col_wx.at[half], sems.at[2])
        wait_bytes(row_ox.at[o_half], sems.at[3])
        wait_bytes(col_ox.at[o_half], sems.at[4])
        wait_bytes(sides_all.at[0], sems.at[5])

    @pl.when(c == r)
    def _():
        wait_bytes(bias_all.at[0, 0, pl.ds(0, deep - 1)], line_sent.at[0])

    @pl.when(c != r)
    def _():
        wait_bytes(bias_all.at[0, 0], line_sent.at[0])

    wait_bytes(row_wx.at[mine], line_sent.at[1])
    wait_bytes(col_wx.at[mine], line_sent.at[2])
    wait_bytes(row_ox.at[o_half], line_sent.at[3])
    wait_bytes(col_ox.at[o_half], line_sent.at[4])
    wait_bytes(final_x, line_sent.at[5])
    wait_bytes(bias_all.at[0, pl.ds(0, plane - 1)], bias_sent)
    wait_bytes(row_wx.at[rest], row_sent)
    wait_bytes(col_wx.at[rest], col_sent)
    wait_bytes(sides_all.at[0, pl.ds(0, chips - 1)], s_sent)


def second_exchange(seqs, column, m_sent, m_came):
    z, x, y, c, r = place()
    chips = seqs.shape[0]
    chip = z * 16 + x * 4 + y
    me = chip * 2 + c
    here = (z, x, y)

    def greet_chip(i, carry):
        there = chip_at(lax.rem(chip + i, chips))
        greet((*there, r, 1 - r))

        @pl.when(c == r)
        def _():
            greet((*there, r, r))
            greet((*there, 1 - r, r))

        @pl.when(c != r)
        def _():
            greet((*there, r, r))
            greet((*there, 1 - r, 1 - r))

        return carry

    lax.fori_loop(1, chips, greet_chip, 0)
    greet((*here, r, 1 - r))

    @pl.when(c == r)
    def _():
        greet((*here, 1 - r, r))
        column[me] = seqs[chip]
        pl.semaphore_wait(pltpu.get_barrier_semaphore(), 3 * chips - 1)

    @pl.when(c != r)
    def _():
        greet((*here, r, r))
        greet((*here, 1 - r, 1 - r))
        pl.semaphore_wait(pltpu.get_barrier_semaphore(), 3 * chips)

    @pl.when(c != r)
    def _():
        send(seqs.at[chip], column.at[me], m_sent, m_came, (*here, r, r))

    def to_owner(i, carry):
        to = lax.rem(chip + i, chips)
        send(seqs.at[to], column.at[me], m_sent, m_came, (*chip_at(to), r, 1 - r))
        send(seqs.at[to], column.at[me], m_sent, m_came, (*chip_at(to), r, r))
        return carry

    lax.fori_loop(1, chips, to_owner, 0)
    send(seqs.at[chip], column.at[me], m_sent, m_came, (*here, r, 1 - r))

    for sem in (m_came, m_sent):

        @pl.when(c == r)
        def _():
            wait_bytes(column.at[pl.ds(0, 2 * chips - 1)], sem)

        @pl.when(c != r)
        def _():
            wait_bytes(column, sem)


def exchange(kernel, number, outs, semaphores, *operands):
    return pl.pallas_call(
        kernel,
        out_shape=[jax.ShapeDtypeStruct(s, jnp.bfloat16) for s in outs],
        in_specs=[VMEM] * len(operands),
        out_specs=[VMEM] * len(outs),
        scratch_shapes=[
            pltpu.SemaphoreType.DMA if n == 0 else pltpu.SemaphoreType.DMA((n,)) for n in semaphores
        ],
        compiler_params=pltpu.CompilerParams(
            collective_id=number, has_side_effects=True, vmem_limit_bytes=40 << 20
        ),
    )(*operands)


def dot_last(a, b):
    return lax.dot_general(a, b, (((1,), (1,)), ((), ())), preferred_element_type=jnp.float32)


def dot(a, b):
    return jnp.dot(a, b, preferred_element_type=jnp.float32)


def project(x, own, other):
    return jnp.concatenate([dot(x, own), dot(x, other)], 1).astype(jnp.bfloat16)


def attend_rows(q, k, v, g, bias, mixed, block, heads):
    embed = q.shape[1]
    queries = q.shape[0]
    lane = lax.broadcasted_iota(jnp.int32, (heads, embed), 1) // GROUP_BREADTH
    head = lax.broadcasted_iota(jnp.int32, (heads, embed), 0)
    own = (lane == head).astype(jnp.float32)[None]
    scale = 1.0 / jnp.sqrt(jnp.float32(GROUP_BREADTH))

    for n in range(queries // block):
        part = slice(n * block, (n + 1) * block)
        wide = q[part].astype(jnp.float32)[:, None, :] * own
        wide = wide.reshape(block * heads, embed).astype(jnp.bfloat16)
        scores = dot_last(wide, k) * scale + bias(n)
        scores = jnp.exp(scores - jnp.max(scores, axis=1, keepdims=True))
        weights = (scores * (1.0 / jnp.sum(scores, axis=1, keepdims=True))).astype(jnp.bfloat16)
        out = dot(weights, v).reshape(block, heads, embed) * own
        out = jnp.sum(out, axis=1)
        gate = 1.0 / (1.0 + jnp.exp(-g[part].astype(jnp.float32)))
        mixed[part, :] = (out * gate).astype(jnp.bfloat16)


def row_kernel(
    rows,
    msa,
    pick,
    bias_all,
    hidden,
    w,
    wx,
    wo,
    wox,
    out,
    product,
    bias_rows,
    mixed,
    p_sent,
    p_came,
    *,
    heads,
    block,
):
    z, x, y, c, r = place()
    chips = rows.shape[0]
    chip = z * 16 + x * 4 + y
    channel = r * chips + chip

    def greet_rows(i, carry):
        there = chip_at(lax.rem(chip + i, chips))
        greet((*there, c, 1 - r))
        greet((*there, c, r))
        return carry

    lax.fori_loop(1, chips, greet_rows, 0)
    greet((z, x, y, c, 1 - r))
    product[channel] = rows[chip]

    planes = bias_all.shape[1]
    rows_each = bias_rows.shape[0] // chips
    sites = bias_rows.shape[2]
    away = hidden[...]

    def place_bias(p, carry):
        at, level = lax.rem(p, planes), p // planes
        both = jnp.concatenate(
            [
                bias_all[r, at, level].astype(jnp.float32),
                bias_all[1 - r, at, level].astype(jnp.float32),
            ],
            0,
        )
        for t in range(rows_each):
            bias_rows[p * rows_each + t] = both[:, t * sites : (t + 1) * sites] + away
        return carry

    lax.fori_loop(0, chips, place_bias, 0)

    pl.semaphore_wait(pltpu.get_barrier_semaphore(), 2 * chips - 1)

    def to_rows(i, carry):
        to = lax.rem(chip + i, chips)
        send(rows.at[to], product.at[channel], p_sent, p_came, (*chip_at(to), c, 1 - r))
        send(rows.at[to], product.at[channel], p_sent, p_came, (*chip_at(to), c, r))
        return carry

    lax.fori_loop(1, chips, to_rows, 0)
    send(rows.at[chip], product.at[channel], p_sent, p_came, (z, x, y, c, 1 - r))

    def one(s, carry):
        x = standardize_features(msa[s]).astype(jnp.bfloat16)
        xq = dot(pick[...], x).astype(jnp.bfloat16)
        q = project(xq, w[0], wx[0])
        k = project(x, w[1], wx[1])
        v = project(x, w[2], wx[2])
        g = project(xq, w[3], wx[3])

        def bias(n):
            return bias_rows[n * block : (n + 1) * block].reshape(block * heads, sites)

        attend_rows(q, k, v, g, bias, mixed, block, heads)
        half = wo.shape[0]
        delta = dot(mixed[:, :half], wo[...]) + dot(mixed[:, half:], wox[...])
        out[s] = (dot(pick[...], msa[s]) + delta).astype(jnp.bfloat16)
        return carry

    lax.fori_loop(0, msa.shape[0], one, 0)
    for sem in (p_came, p_sent):
        wait_bytes(product.at[pl.ds(0, 2 * chips - 1)], sem)


def col_kernel(column, hidden, w, wx, wo, wox, out, mixed, *, heads, block):
    r = lax.axis_index("rep")
    embed = w.shape[1]
    width = embed // 2
    at = pl.ds(pl.multiple_of(r * width, width), width)
    away = hidden[...]
    for t in range(column.shape[1] // embed):
        x = standardize_features(column[:, t * embed : (t + 1) * embed]).astype(jnp.bfloat16)
        q, k, v, g = [project(x, w[n], wx[n]) for n in range(4)]
        attend_rows(q, k, v, g, lambda n: away, mixed, block, heads)
        half = wo.shape[0]
        delta = dot(mixed[:, :half], wo[:, at]) + dot(mixed[:, half:], wox[:, at])
        keep = column[:, pl.ds(pl.multiple_of(t * embed + r * width, width), width)]
        out[:, t * width : (t + 1) * width] = (keep.astype(jnp.float32) + delta).astype(jnp.bfloat16)


def local_call(kernel, out, scratch, flops, *operands):
    return pl.pallas_call(
        kernel,
        out_shape=jax.ShapeDtypeStruct(out, jnp.bfloat16),
        in_specs=[VMEM] * len(operands),
        out_specs=VMEM,
        scratch_shapes=[pltpu.VMEM(*s) for s in scratch],
        compiler_params=pltpu.CompilerParams(vmem_limit_bytes=40 << 20),
        cost_estimate=pl.CostEstimate(flops=flops, bytes_accessed=4 << 20, transcendentals=0),
    )(*operands)


def per_device(
    msa,
    pair,
    homolog_present,
    amino_present,
    row_w,
    row_out,
    offset_w,
    col_w,
    col_out,
    side_w,
    final_w,
    sigmoid_w,
):
    rep = lax.axis_index("rep")
    core = lax.axis_index(CORE)
    rows_here, sites, channels = pair.shape
    seqs_here, embed = msa.shape[0], msa.shape[2]
    chips = lax.axis_size(CHIPS)
    devices = lax.axis_size(DAP)
    heads_here = offset_w.shape[1]
    heads = 2 * heads_here
    row_start = lax.axis_index(DAP) * rows_here
    res_float = amino_present.astype(jnp.float32)
    mask_rows = lax.dynamic_slice_in_dim(res_float, row_start, rows_here, 0)
    flat = rows_here * sites

    pair_ln = standardize_features(pair).astype(jnp.bfloat16).reshape(flat, channels)
    bias = jnp.einsum("nc,ch->hn", pair_ln, offset_w, preferred_element_type=jnp.float32).astype(
        jnp.bfloat16
    )
    pair_mask = (mask_rows[:, None] * res_float[None, :]).reshape(1, flat)

    def gated_side(gate_weight, value_weight):
        gate = jnp.einsum("nd,dc->cn", pair_ln, gate_weight, preferred_element_type=jnp.float32)
        value = jnp.einsum("nd,dc->cn", pair_ln, value_weight, preferred_element_type=jnp.float32)
        return (jax.nn.sigmoid(gate) * value * pair_mask).astype(jnp.bfloat16)

    sides = jnp.stack([gated_side(side_w[0], side_w[1]), gated_side(side_w[2], side_w[3])], 1)

    weight_rows = row_w.shape[0] * row_w.shape[1]
    flat_w = (weight_rows, row_w.shape[2])
    bias_all, sides_all, row_wx, col_wx, row_ox, col_ox, final_x = exchange(
        first_exchange,
        0,
        [
            (2, 16, chips // 16, heads_here, flat),
            (2, chips, 2, flat),
            flat_w,
            flat_w,
            row_out.shape,
            col_out.shape,
            final_w.shape,
        ],
        [0, 4, 6, 6, 0, 16, 0, 16, 0, 16, 6, 6],
        bias,
        sides,
        row_w.reshape(flat_w),
        col_w.reshape(flat_w),
        row_out,
        col_out,
        final_w,
    )

    lefts = lax.dynamic_index_in_dim(sides_all, core, 0, keepdims=False)[:, 0]
    rights = sides_all[:, :, 1].swapaxes(0, 1)
    product = jnp.einsum(
        "ik,jk->ij",
        lefts.reshape(chips * rows_here, sites),
        rights.reshape(devices * rows_here, sites),
        preferred_element_type=jnp.float32,
    )
    product = product.astype(jnp.bfloat16).reshape(chips, rows_here, sites)

    queries = chips * rows_here
    query = lax.broadcasted_iota(jnp.int32, (queries, sites), 0)
    site = lax.broadcasted_iota(jnp.int32, (queries, sites), 1)
    picked = 2 * rows_here * (query // rows_here) + rows_here * rep + query % rows_here
    pick = (site == picked).astype(jnp.bfloat16)
    hidden = (NEG * (res_float - 1.0))[None, :]
    operands = (
        product,
        msa,
        pick,
        bias_all,
        hidden,
        row_w,
        row_wx.reshape(row_w.shape),
        row_out,
        row_ox,
    )
    msa_one, product = pl.pallas_call(
        functools.partial(row_kernel, heads=heads, block=24),
        out_shape=[
            jax.ShapeDtypeStruct((seqs_here, queries, embed), jnp.bfloat16),
            jax.ShapeDtypeStruct((devices, rows_here, sites), jnp.bfloat16),
        ],
        in_specs=[VMEM] * len(operands),
        out_specs=[VMEM] * 2,
        scratch_shapes=[
            pltpu.VMEM((queries, heads, sites), jnp.float32),
            pltpu.VMEM((queries, embed), jnp.bfloat16),
            pltpu.SemaphoreType.DMA,
            pltpu.SemaphoreType.DMA,
        ],
        compiler_params=pltpu.CompilerParams(
            collective_id=2, has_side_effects=True, vmem_limit_bytes=40 << 20
        ),
    )(*operands)

    seq_blocks = msa_one.reshape(seqs_here, chips, rows_here * embed).swapaxes(0, 1)
    (column,) = exchange(
        second_exchange,
        1,
        [(devices, seqs_here, rows_here * embed)],
        [0, 0],
        seq_blocks,
    )

    column = column.reshape(devices * seqs_here, rows_here * embed)
    away = (NEG * (homolog_present.astype(jnp.float32) - 1.0))[None, :]
    width = embed // 2
    alignment_output = local_call(
        functools.partial(col_kernel, heads=heads, block=32),
        (devices * seqs_here, rows_here * width),
        [((devices * seqs_here, embed), jnp.bfloat16)],
        3 << 30,
        column,
        away,
        col_w,
        col_wx.reshape(col_w.shape),
        col_out,
        col_ox,
    ).reshape(devices * seqs_here, rows_here, width)

    product = product.astype(jnp.float32)
    mean = jnp.mean(product, axis=0)
    square = jnp.mean(product * product, axis=0)
    scaled = ((product - mean) * lax.rsqrt(square - mean * mean + EPS)).astype(jnp.bfloat16)
    half = channels // 2
    first = jnp.where(rep == 0, final_w, final_x)
    second = jnp.where(rep == 0, final_x, final_w)
    final_all = jnp.concatenate([first, second], 0)
    final_half = lax.dynamic_slice_in_dim(final_all, rep * half, half, 1)
    tri_update = jnp.einsum("cij,cz->ijz", scaled, final_half, preferred_element_type=jnp.float32)
    pair_half = lax.dynamic_slice_in_dim(pair, rep * half, half, 2)
    gate_out = jax.nn.sigmoid(dot(pair_ln, sigmoid_w)).reshape(rows_here, sites, half)
    pair_output = (pair_half.astype(jnp.float32) + gate_out * tri_update).astype(jnp.bfloat16)
    return (alignment_output, pair_output)


def solution(mesh):
    finer = Mesh(
        mesh.devices.reshape(4, 4, 4, 2, mesh.shape["rep"]),
        (*DAP, "rep"),
    )
    return jax.shard_map(
        per_device,
        mesh=finer,
        in_specs=(
            P(DAP, None, None),
            P(DAP, None, None),
            P(),
            P(),
            P(None, None, "rep"),
            P("rep", None),
            P(None, "rep"),
            P(None, None, "rep"),
            P("rep", None),
            P(None, None, "rep"),
            P("rep", None),
            P(None, "rep"),
        ),
        out_specs=(P(None, DAP, "rep"), P(DAP, None, "rep")),
        check_vma=False,
    )
```

```python
import functools

import jax
import jax.numpy as jnp
from jax import lax
from jax.experimental import pallas as pl
from jax.experimental.pallas import tpu as pltpu
from jax.sharding import Mesh
from jax.sharding import PartitionSpec as P

GROUP_BREADTH = 32
CHIPS = ("dap_0", "dap_1", "dap_2")
CORE = "dap_3"
DAP = CHIPS + (CORE,)
MESH = pl.DeviceIdType.MESH
VMEM = pl.BlockSpec(memory_space=pltpu.VMEM)

EPS = 1e-05
NEG = 1000000000.0


def standardize_features(values):
    values = values.astype(jnp.float32)
    center = jnp.mean(values, axis=-1, keepdims=True)
    spread = jnp.mean(jnp.square(values - center), axis=-1, keepdims=True)
    return (values - center) * lax.rsqrt(spread + EPS)


def place():
    z, x, y = (lax.axis_index(a) for a in CHIPS)
    return z, x, y, lax.axis_index(CORE), lax.axis_index("rep")


def send(src, dst, sent, came, device):
    pltpu.make_async_remote_copy(
        src_ref=src, dst_ref=dst, send_sem=sent, recv_sem=came, device_id=device, device_id_type=MESH
    ).start()


def wait_bytes(ref, sem):
    pltpu.make_async_copy(ref, ref, sem).wait()


def greet(device):
    pl.semaphore_signal(pltpu.get_barrier_semaphore(), inc=1, device_id=device, device_id_type=MESH)


def chip_at(to):
    plane, high = 16, 4
    return to // plane, lax.rem(to // high, high), lax.rem(to, high)


def first_exchange(
    bias,
    sides,
    row_w,
    col_w,
    row_o,
    col_o,
    final,
    bias_all,
    sides_all,
    row_wx,
    col_wx,
    row_ox,
    col_ox,
    final_x,
    s_sent,
    s_came,
    line_sent,
    line_came,
    bias_sent,
    bias_came,
    row_sent,
    row_came,
    col_sent,
    col_came,
    core_sent,
    core_came,
):
    z, x, y, c, r = place()
    deep, high = 4, 4
    plane = high * high
    chips = deep * plane
    xy = x * high + y
    chip = z * plane + xy
    chunk = row_w.shape[0] // (2 * plane)
    mirror = (deep - 1 - z, x, y, c, 1 - r)
    partner = (z, x, y, 1 - c, r)

    def rows_of(at):
        return pl.ds(pl.multiple_of((c * plane + at) * chunk, chunk), chunk)

    mine = rows_of(xy)

    def greet_group(i, carry):
        greet((*chip_at(lax.rem(chip + i, chips)), c, r))
        return carry

    lax.fori_loop(1, chips, greet_group, 0)
    greet(mirror)
    greet(partner)
    for zt in range(deep):

        @pl.when(c != r)
        def _():
            greet((zt, x, y, r, c))

    sides_all[c, chip] = sides[chip]

    @pl.when(c == r)
    def _():
        bias_all[r, xy, z] = bias[...]
        pl.semaphore_wait(pltpu.get_barrier_semaphore(), chips + 1)

    @pl.when(c != r)
    def _():
        pl.semaphore_wait(pltpu.get_barrier_semaphore(), chips + 1 + deep)

    for dz in range(deep):
        zt = lax.rem(z + dz, deep)
        if dz == 0:

            @pl.when(c != r)
            def _():
                send(bias, bias_all.at[r, xy, z], line_sent.at[0], line_came.at[0], (zt, x, y, r, c))

        else:
            send(bias, bias_all.at[r, xy, z], line_sent.at[0], line_came.at[0], (zt, x, y, r, c))
    send(row_w.at[mine], row_wx.at[mine], line_sent.at[1], line_came.at[1], mirror)
    send(col_w.at[mine], col_wx.at[mine], line_sent.at[2], line_came.at[2], mirror)
    o_half = pl.ds(pl.multiple_of(c * (row_o.shape[0] // 2), row_o.shape[0] // 2), row_o.shape[0] // 2)
    send(row_o.at[o_half], row_ox.at[o_half], line_sent.at[3], line_came.at[3], mirror)
    send(col_o.at[o_half], col_ox.at[o_half], line_sent.at[4], line_came.at[4], mirror)
    send(final, final_x, line_sent.at[5], line_came.at[5], mirror)

    def to_owner(i, carry):
        to = lax.rem(chip + i, chips)
        send(sides.at[to], sides_all.at[c, chip], s_sent, s_came.at[z], (*chip_at(to), c, r))
        return carry

    lax.fori_loop(1, plane, to_owner, 0)

    @pl.when(c == r)
    def _():
        wait_bytes(bias_all.at[0, 0, pl.ds(0, deep - 1)], line_came.at[0])

    @pl.when(c != r)
    def _():
        wait_bytes(bias_all.at[0, 0], line_came.at[0])

    def plane_device(i):
        to = lax.rem(xy + i, plane)
        return (z, to // high, lax.rem(to, high), c, r)

    def bias_plane(i, carry):
        send(bias_all.at[c, xy], bias_all.at[c, xy], bias_sent, bias_came.at[xy], plane_device(i))
        return carry

    lax.fori_loop(1, plane, bias_plane, 0)
    wait_bytes(row_wx.at[mine], line_came.at[1])
    wait_bytes(col_wx.at[mine], line_came.at[2])

    def weight_plane(i, carry):
        device = plane_device(i)
        send(row_wx.at[mine], row_wx.at[mine], row_sent, row_came.at[xy], device)
        send(col_wx.at[mine], col_wx.at[mine], col_sent, col_came.at[xy], device)
        return carry

    lax.fori_loop(1, plane, weight_plane, 0)
    lax.fori_loop(plane, chips, to_owner, 0)

    send(bias_all.at[c, xy], bias_all.at[c, xy], core_sent.at[0], core_came.at[0], partner)
    send(row_wx.at[mine], row_wx.at[mine], core_sent.at[1], core_came.at[1], partner)
    send(col_wx.at[mine], col_wx.at[mine], core_sent.at[2], core_came.at[2], partner)
    wait_bytes(row_ox.at[o_half], line_came.at[3])
    send(row_ox.at[o_half], row_ox.at[o_half], core_sent.at[3], core_came.at[3], partner)
    wait_bytes(col_ox.at[o_half], line_came.at[4])
    send(col_ox.at[o_half], col_ox.at[o_half], core_sent.at[4], core_came.at[4], partner)

    def bias_core(i, carry):
        at = lax.rem(xy + i, plane)
        wait_bytes(bias_all.at[c, at], bias_came.at[at])
        send(bias_all.at[c, at], bias_all.at[c, at], core_sent.at[0], core_came.at[0], partner)
        return carry

    lax.fori_loop(1, plane, bias_core, 0)

    def weight_core(i, carry):
        at = lax.rem(xy + i, plane)
        rows = rows_of(at)
        wait_bytes(row_wx.at[rows], row_came.at[at])
        send(row_wx.at[rows], row_wx.at[rows], core_sent.at[1], core_came.at[1], partner)
        wait_bytes(col_wx.at[rows], col_came.at[at])
        send(col_wx.at[rows], col_wx.at[rows], core_sent.at[2], core_came.at[2], partner)
        return carry

    lax.fori_loop(1, plane, weight_core, 0)

    def pass_sides(level):
        for n in range(4):
            part = pl.ds(pl.multiple_of(level * plane + n * high, high), high)
            send(sides_all.at[c, part], sides_all.at[c, part], core_sent.at[5], core_came.at[5], partner)

    wait_bytes(sides_all.at[0, pl.ds(0, plane - 1)], s_came.at[z])
    pass_sides(z)
    for dz in range(1, deep):
        level = lax.rem(z + dz, deep)
        wait_bytes(sides_all.at[0, pl.ds(0, plane)], s_came.at[level])
        pass_sides(level)

    half = pl.ds(0, plane * chunk)
    rest = pl.ds(0, (plane - 1) * chunk)
    wait_bytes(final_x, line_came.at[5])
    for sems in (core_came, core_sent):
        wait_bytes(bias_all.at[0], sems.at[0])
        wait_bytes(row_wx.at[half], sems.at[1])
        wait_bytes(col_wx.at[half], sems.at[2])
        wait_bytes(row_ox.at[o_half], sems.at[3])
        wait_bytes(col_ox.at[o_half], sems.at[4])
        wait_bytes(sides_all.at[0], sems.at[5])

    @pl.when(c == r)
    def _():
        wait_bytes(bias_all.at[0, 0, pl.ds(0, deep - 1)], line_sent.at[0])

    @pl.when(c != r)
    def _():
        wait_bytes(bias_all.at[0, 0], line_sent.at[0])

    wait_bytes(row_wx.at[mine], line_sent.at[1])
    wait_bytes(col_wx.at[mine], line_sent.at[2])
    wait_bytes(row_ox.at[o_half], line_sent.at[3])
    wait_bytes(col_ox.at[o_half], line_sent.at[4])
    wait_bytes(final_x, line_sent.at[5])
    wait_bytes(bias_all.at[0, pl.ds(0, plane - 1)], bias_sent)
    wait_bytes(row_wx.at[rest], row_sent)
    wait_bytes(col_wx.at[rest], col_sent)
    wait_bytes(sides_all.at[0, pl.ds(0, chips - 1)], s_sent)


def exchange(kernel, number, outs, semaphores, *operands):
    return pl.pallas_call(
        kernel,
        out_shape=[jax.ShapeDtypeStruct(s, jnp.bfloat16) for s in outs],
        in_specs=[VMEM] * len(operands),
        out_specs=[VMEM] * len(outs),
        scratch_shapes=[
            pltpu.SemaphoreType.DMA if n == 0 else pltpu.SemaphoreType.DMA((n,)) for n in semaphores
        ],
        compiler_params=pltpu.CompilerParams(
            collective_id=number, has_side_effects=True, vmem_limit_bytes=40 << 20
        ),
    )(*operands)


def dot_last(a, b):
    return lax.dot_general(a, b, (((1,), (1,)), ((), ())), preferred_element_type=jnp.float32)


def dot(a, b):
    return jnp.dot(a, b, preferred_element_type=jnp.float32)


def project(x, own, other):
    return jnp.concatenate([dot(x, own), dot(x, other)], 1).astype(jnp.bfloat16)


def attend_rows(q, k, v, g, bias, mixed, block, heads):
    embed = q.shape[1]
    queries = q.shape[0]
    lane = lax.broadcasted_iota(jnp.int32, (heads, embed), 1) // GROUP_BREADTH
    head = lax.broadcasted_iota(jnp.int32, (heads, embed), 0)
    own = (lane == head).astype(jnp.float32)[None]
    scale = 1.0 / jnp.sqrt(jnp.float32(GROUP_BREADTH))

    for n in range(queries // block):
        part = slice(n * block, (n + 1) * block)
        wide = q[part].astype(jnp.float32)[:, None, :] * own
        wide = wide.reshape(block * heads, embed).astype(jnp.bfloat16)
        scores = dot_last(wide, k) * scale + bias(n)
        scores = jnp.exp(scores - jnp.max(scores, axis=1, keepdims=True))
        weights = (scores * (1.0 / jnp.sum(scores, axis=1, keepdims=True))).astype(jnp.bfloat16)
        out = dot(weights, v).reshape(block, heads, embed) * own
        out = jnp.sum(out, axis=1)
        gate = 1.0 / (1.0 + jnp.exp(-g[part].astype(jnp.float32)))
        mixed[part, :] = (out * gate).astype(jnp.bfloat16)


def row_kernel(
    rows,
    msa,
    pick,
    bias_all,
    hidden,
    w,
    wx,
    wo,
    wox,
    column,
    product,
    bias_rows,
    mixed,
    done,
    seqs,
    p_sent,
    p_came,
    m_sent,
    m_came,
    *,
    heads,
    block,
):
    z, x, y, c, r = place()
    chips = rows.shape[0]
    chip = z * 16 + x * 4 + y
    me = chip * 2 + c
    channel = r * chips + chip
    here = (z, x, y)
    embed = w.shape[1]

    def greet_chip(i, carry):
        there = chip_at(lax.rem(chip + i, chips))
        for ct in range(2):
            for rt in range(2):
                greet((*there, ct, rt))
        return carry

    lax.fori_loop(1, chips, greet_chip, 0)
    greet((*here, 1 - c, r))
    greet((*here, c, 1 - r))
    greet((*here, 1 - c, 1 - r))
    product[channel] = rows[chip]

    planes = bias_all.shape[1]
    rows_each = bias_rows.shape[0] // chips
    sites = bias_rows.shape[2]
    away = hidden[...]

    def place_bias(p, carry):
        at, level = lax.rem(p, planes), p // planes
        both = jnp.concatenate(
            [
                bias_all[r, at, level].astype(jnp.float32),
                bias_all[1 - r, at, level].astype(jnp.float32),
            ],
            0,
        )
        for t in range(rows_each):
            bias_rows[t * chips + p] = both[:, t * sites : (t + 1) * sites] + away
        return carry

    lax.fori_loop(0, chips, place_bias, 0)

    def to_rows(i, carry):
        to = lax.rem(chip + i, chips)
        send(rows.at[to], product.at[channel], p_sent, p_came, (*chip_at(to), c, 1 - r))
        send(rows.at[to], product.at[channel], p_sent, p_came, (*chip_at(to), c, r))
        return carry

    def one(s, carry):
        @pl.when(s == 1)
        def _():
            pl.semaphore_wait(pltpu.get_barrier_semaphore(), 4 * chips - 1)
            lax.fori_loop(1, chips, to_rows, 0)
            send(rows.at[chip], product.at[channel], p_sent, p_came, (*here, c, 1 - r))

        x = standardize_features(msa[s]).astype(jnp.bfloat16)
        xq = dot(pick[...], x).astype(jnp.bfloat16)
        q = project(xq, w[0], wx[0])
        k = project(x, w[1], wx[1])
        v = project(x, w[2], wx[2])
        g = project(xq, w[3], wx[3])

        def bias(n):
            return bias_rows[n * block : (n + 1) * block].reshape(block * heads, sites)

        attend_rows(q, k, v, g, bias, mixed, block, heads)
        half = wo.shape[0]
        delta = dot(mixed[:, :half], wo[...]) + dot(mixed[:, half:], wox[...])
        done[s] = dot(pick[...], msa[s]) + delta
        return carry

    lax.fori_loop(0, msa.shape[0], one, 0)

    for t in range(rows_each):
        part = slice(t * chips, (t + 1) * chips)
        both = jnp.concatenate([done[0, part, :][:, None, :], done[1, part, :][:, None, :]], 1)
        seqs[:, :, t * embed : (t + 1) * embed] = both.astype(jnp.bfloat16)

    @pl.when(c == r)
    def _():
        column[me] = seqs[chip]

    def to_owner(i, carry):
        to = lax.rem(chip + i, chips)
        send(seqs.at[to], column.at[me], m_sent, m_came, (*chip_at(to), r, 1 - r))
        send(seqs.at[to], column.at[me], m_sent, m_came, (*chip_at(to), r, r))
        return carry

    lax.fori_loop(1, chips, to_owner, 0)

    @pl.when(c != r)
    def _():
        send(seqs.at[chip], column.at[me], m_sent, m_came, (*here, r, r))

    send(seqs.at[chip], column.at[me], m_sent, m_came, (*here, r, 1 - r))

    for sem in (m_came, m_sent):

        @pl.when(c == r)
        def _():
            wait_bytes(column.at[pl.ds(0, 2 * chips - 1)], sem)

        @pl.when(c != r)
        def _():
            wait_bytes(column, sem)

    for sem in (p_came, p_sent):
        wait_bytes(product.at[pl.ds(0, 2 * chips - 1)], sem)


def col_kernel(column, hidden, w, wx, wo, wox, out, mixed, *, heads, block):
    r = lax.axis_index("rep")
    embed = w.shape[1]
    width = embed // 2
    at = pl.ds(pl.multiple_of(r * width, width), width)
    away = hidden[...]
    for t in range(column.shape[1] // embed):
        x = standardize_features(column[:, t * embed : (t + 1) * embed]).astype(jnp.bfloat16)
        q, k, v, g = [project(x, w[n], wx[n]) for n in range(4)]
        attend_rows(q, k, v, g, lambda n: away, mixed, block, heads)
        half = wo.shape[0]
        delta = dot(mixed[:, :half], wo[:, at]) + dot(mixed[:, half:], wox[:, at])
        keep = column[:, pl.ds(pl.multiple_of(t * embed + r * width, width), width)]
        out[:, t * width : (t + 1) * width] = (keep.astype(jnp.float32) + delta).astype(jnp.bfloat16)


def local_call(kernel, out, scratch, flops, *operands):
    return pl.pallas_call(
        kernel,
        out_shape=jax.ShapeDtypeStruct(out, jnp.bfloat16),
        in_specs=[VMEM] * len(operands),
        out_specs=VMEM,
        scratch_shapes=[pltpu.VMEM(*s) for s in scratch],
        compiler_params=pltpu.CompilerParams(vmem_limit_bytes=40 << 20),
        cost_estimate=pl.CostEstimate(flops=flops, bytes_accessed=4 << 20, transcendentals=0),
    )(*operands)


def per_device(
    msa,
    pair,
    homolog_present,
    amino_present,
    row_w,
    row_out,
    offset_w,
    col_w,
    col_out,
    side_w,
    final_w,
    sigmoid_w,
):
    rep = lax.axis_index("rep")
    core = lax.axis_index(CORE)
    rows_here, sites, channels = pair.shape
    seqs_here, embed = msa.shape[0], msa.shape[2]
    chips = lax.axis_size(CHIPS)
    devices = lax.axis_size(DAP)
    heads_here = offset_w.shape[1]
    heads = 2 * heads_here
    row_start = lax.axis_index(DAP) * rows_here
    res_float = amino_present.astype(jnp.float32)
    mask_rows = lax.dynamic_slice_in_dim(res_float, row_start, rows_here, 0)
    flat = rows_here * sites

    pair_ln = standardize_features(pair).astype(jnp.bfloat16).reshape(flat, channels)
    bias = jnp.einsum("nc,ch->hn", pair_ln, offset_w, preferred_element_type=jnp.float32).astype(
        jnp.bfloat16
    )
    pair_mask = (mask_rows[:, None] * res_float[None, :]).reshape(1, flat)

    def gated_side(gate_weight, value_weight):
        gate = jnp.einsum("nd,dc->cn", pair_ln, gate_weight, preferred_element_type=jnp.float32)
        value = jnp.einsum("nd,dc->cn", pair_ln, value_weight, preferred_element_type=jnp.float32)
        return (jax.nn.sigmoid(gate) * value * pair_mask).astype(jnp.bfloat16)

    sides = jnp.stack([gated_side(side_w[0], side_w[1]), gated_side(side_w[2], side_w[3])], 1)

    weight_rows = row_w.shape[0] * row_w.shape[1]
    flat_w = (weight_rows, row_w.shape[2])
    bias_all, sides_all, row_wx, col_wx, row_ox, col_ox, final_x = exchange(
        first_exchange,
        0,
        [
            (2, 16, chips // 16, heads_here, flat),
            (2, chips, 2, flat),
            flat_w,
            flat_w,
            row_out.shape,
            col_out.shape,
            final_w.shape,
        ],
        [0, 4, 6, 6, 0, 16, 0, 16, 0, 16, 6, 6],
        bias,
        sides,
        row_w.reshape(flat_w),
        col_w.reshape(flat_w),
        row_out,
        col_out,
        final_w,
    )

    lefts = lax.dynamic_index_in_dim(sides_all, core, 0, keepdims=False)[:, 0]
    rights = sides_all[:, :, 1].swapaxes(0, 1)
    product = jnp.einsum(
        "ik,jk->ij",
        lefts.reshape(chips * rows_here, sites),
        rights.reshape(devices * rows_here, sites),
        preferred_element_type=jnp.float32,
    )
    product = product.astype(jnp.bfloat16).reshape(chips, rows_here, sites)

    queries = chips * rows_here
    query = lax.broadcasted_iota(jnp.int32, (queries, sites), 0)
    site = lax.broadcasted_iota(jnp.int32, (queries, sites), 1)
    picked = 2 * rows_here * (query % chips) + rows_here * rep + query // chips
    pick = (site == picked).astype(jnp.bfloat16)
    hidden = (NEG * (res_float - 1.0))[None, :]
    operands = (
        product,
        msa,
        pick,
        bias_all,
        hidden,
        row_w,
        row_wx.reshape(row_w.shape),
        row_out,
        row_ox,
    )
    column, product = pl.pallas_call(
        functools.partial(row_kernel, heads=heads, block=24),
        out_shape=[
            jax.ShapeDtypeStruct((devices, seqs_here, rows_here * embed), jnp.bfloat16),
            jax.ShapeDtypeStruct((devices, rows_here, sites), jnp.bfloat16),
        ],
        in_specs=[VMEM] * len(operands),
        out_specs=[VMEM] * 2,
        scratch_shapes=[
            pltpu.VMEM((queries, heads, sites), jnp.float32),
            pltpu.VMEM((queries, embed), jnp.bfloat16),
            pltpu.VMEM((seqs_here, queries, embed), jnp.float32),
            pltpu.VMEM((chips, seqs_here, rows_here * embed), jnp.bfloat16),
            pltpu.SemaphoreType.DMA,
            pltpu.SemaphoreType.DMA,
            pltpu.SemaphoreType.DMA,
            pltpu.SemaphoreType.DMA,
        ],
        compiler_params=pltpu.CompilerParams(
            collective_id=1, has_side_effects=True, vmem_limit_bytes=40 << 20
        ),
    )(*operands)

    column = column.reshape(devices * seqs_here, rows_here * embed)
    away = (NEG * (homolog_present.astype(jnp.float32) - 1.0))[None, :]
    width = embed // 2
    alignment_output = local_call(
        functools.partial(col_kernel, heads=heads, block=32),
        (devices * seqs_here, rows_here * width),
        [((devices * seqs_here, embed), jnp.bfloat16)],
        3 << 30,
        column,
        away,
        col_w,
        col_wx.reshape(col_w.shape),
        col_out,
        col_ox,
    ).reshape(devices * seqs_here, rows_here, width)

    product = product.astype(jnp.float32)
    mean = jnp.mean(product, axis=0)
    square = jnp.mean(product * product, axis=0)
    scaled = ((product - mean) * lax.rsqrt(square - mean * mean + EPS)).astype(jnp.bfloat16)
    half = channels // 2
    first = jnp.where(rep == 0, final_w, final_x)
    second = jnp.where(rep == 0, final_x, final_w)
    final_all = jnp.concatenate([first, second], 0)
    final_half = lax.dynamic_slice_in_dim(final_all, rep * half, half, 1)
    tri_update = jnp.einsum("cij,cz->ijz", scaled, final_half, preferred_element_type=jnp.float32)
    pair_half = lax.dynamic_slice_in_dim(pair, rep * half, half, 2)
    gate_out = jax.nn.sigmoid(dot(pair_ln, sigmoid_w)).reshape(rows_here, sites, half)
    pair_output = (pair_half.astype(jnp.float32) + gate_out * tri_update).astype(jnp.bfloat16)
    return (alignment_output, pair_output)


def solution(mesh):
    finer = Mesh(
        mesh.devices.reshape(4, 4, 4, 2, mesh.shape["rep"]),
        (*DAP, "rep"),
    )
    return jax.shard_map(
        per_device,
        mesh=finer,
        in_specs=(
            P(DAP, None, None),
            P(DAP, None, None),
            P(),
            P(),
            P(None, None, "rep"),
            P("rep", None),
            P(None, "rep"),
            P(None, None, "rep"),
            P("rep", None),
            P(None, None, "rep"),
            P("rep", None),
            P(None, "rep"),
        ),
        out_specs=(P(None, DAP, "rep"), P(DAP, None, "rep")),
        check_vma=False,
    )
```

```python
import functools

import jax
import jax.numpy as jnp
from jax import lax
from jax.experimental import pallas as pl
from jax.experimental.pallas import tpu as pltpu
from jax.sharding import Mesh
from jax.sharding import PartitionSpec as P

GROUP_BREADTH = 32
CHIPS = ("dap_0", "dap_1", "dap_2")
CORE = "dap_3"
DAP = CHIPS + (CORE,)
MESH = pl.DeviceIdType.MESH
VMEM = pl.BlockSpec(memory_space=pltpu.VMEM)

EPS = 1e-05
NEG = 1000000000.0


def standardize_features(values):
    values = values.astype(jnp.float32)
    center = jnp.mean(values, axis=-1, keepdims=True)
    spread = jnp.mean(jnp.square(values - center), axis=-1, keepdims=True)
    return (values - center) * lax.rsqrt(spread + EPS)


def place():
    z, x, y = (lax.axis_index(a) for a in CHIPS)
    return z, x, y, lax.axis_index(CORE), lax.axis_index("rep")


def send(src, dst, sent, came, device):
    pltpu.make_async_remote_copy(
        src_ref=src, dst_ref=dst, send_sem=sent, recv_sem=came, device_id=device, device_id_type=MESH
    ).start()


def wait_bytes(ref, sem):
    pltpu.make_async_copy(ref, ref, sem).wait()


def greet(device):
    pl.semaphore_signal(pltpu.get_barrier_semaphore(), inc=1, device_id=device, device_id_type=MESH)


def chip_at(to):
    plane, high = 16, 4
    return to // plane, lax.rem(to // high, high), lax.rem(to, high)


def dot_last(a, b):
    return lax.dot_general(a, b, (((1,), (1,)), ((), ())), preferred_element_type=jnp.float32)


def dot(a, b):
    return jnp.dot(a, b, preferred_element_type=jnp.float32)


def project(x, own, other):
    return jnp.concatenate([dot(x, own), dot(x, other)], 1).astype(jnp.bfloat16)


def attend_rows(q, k, v, g, bias, mixed, block, heads):
    embed = q.shape[1]
    queries = q.shape[0]
    lane = lax.broadcasted_iota(jnp.int32, (heads, embed), 1) // GROUP_BREADTH
    head = lax.broadcasted_iota(jnp.int32, (heads, embed), 0)
    own = (lane == head).astype(jnp.float32)[None]
    scale = 1.0 / jnp.sqrt(jnp.float32(GROUP_BREADTH))

    for n in range(queries // block):
        part = slice(n * block, (n + 1) * block)
        wide = q[part].astype(jnp.float32)[:, None, :] * own
        wide = wide.reshape(block * heads, embed).astype(jnp.bfloat16)
        scores = dot_last(wide, k) * scale + bias(n)
        scores = jnp.exp(scores - jnp.max(scores, axis=1, keepdims=True))
        weights = (scores * (1.0 / jnp.sum(scores, axis=1, keepdims=True))).astype(jnp.bfloat16)
        out = dot(weights, v).reshape(block, heads, embed) * own
        out = jnp.sum(out, axis=1)
        gate = 1.0 / (1.0 + jnp.exp(-g[part].astype(jnp.float32)))
        mixed[part, :] = (out * gate).astype(jnp.bfloat16)


def main_kernel(
    pair,
    pair_mask,
    offset_w,
    side_w,
    row_w,
    col_w,
    row_o,
    col_o,
    final,
    msa,
    pick,
    hidden,
    pair_ln,
    column,
    product,
    col_wx,
    col_ox,
    final_x,
    bias,
    sides,
    bias_all,
    sides_all,
    row_wx,
    row_ox,
    rows,
    bias_rows,
    mixed,
    done,
    seqs,
    s_sent,
    s_came,
    line_sent,
    line_came,
    bias_sent,
    bias_came,
    row_sent,
    row_came,
    col_sent,
    col_came,
    core_sent,
    core_came,
    p_sent,
    p_came,
    m_sent,
    m_came,
    *,
    heads,
    block,
):
    z, x, y, c, r = place()
    deep, high = 4, 4
    plane = high * high
    chips = deep * plane
    xy = x * high + y
    chip = z * plane + xy
    me = chip * 2 + c
    channel = r * chips + chip
    here = (z, x, y)
    chunk = row_w.shape[0] // (2 * plane)
    mirror = (deep - 1 - z, x, y, c, 1 - r)
    partner = (z, x, y, 1 - c, r)
    rows_each, sites = pair.shape[0], pair.shape[1]
    embed = msa.shape[2]

    def rows_of(at):
        return pl.ds(pl.multiple_of((c * plane + at) * chunk, chunk), chunk)

    mine = rows_of(xy)

    def greet_chip(i, carry):
        there = chip_at(lax.rem(chip + i, chips))
        for ct in range(2):
            for rt in range(2):
                greet((*there, ct, rt))
        return carry

    lax.fori_loop(1, chips, greet_chip, 0)
    greet((*here, 1 - c, r))
    greet((*here, c, 1 - r))
    greet((*here, 1 - c, 1 - r))

    for t in range(rows_each):
        part = slice(t * sites, (t + 1) * sites)
        normed = standardize_features(pair[t]).astype(jnp.bfloat16)
        pair_ln[t] = normed
        bias[:, part] = dot_last(offset_w[...], normed).astype(jnp.bfloat16)
        both = []
        for n in range(2):
            gate = dot_last(side_w[2 * n], normed)
            value = dot_last(side_w[2 * n + 1], normed)
            side = value / (1.0 + jnp.exp(-gate)) * pair_mask[t : t + 1, :]
            both.append(side[:, None, :])
        sides[:, :, part] = jnp.concatenate(both, 1).astype(jnp.bfloat16)
    sides_all[c, chip] = sides[chip]

    @pl.when(c == r)
    def _():
        bias_all[r, xy, z] = bias[...]

    pl.semaphore_wait(pltpu.get_barrier_semaphore(), 4 * chips - 1)

    for dz in range(deep):
        zt = lax.rem(z + dz, deep)
        if dz == 0:

            @pl.when(c != r)
            def _():
                send(bias, bias_all.at[r, xy, z], line_sent.at[0], line_came.at[0], (zt, x, y, r, c))

        else:
            send(bias, bias_all.at[r, xy, z], line_sent.at[0], line_came.at[0], (zt, x, y, r, c))
    send(row_w.at[mine], row_wx.at[mine], line_sent.at[1], line_came.at[1], mirror)
    send(col_w.at[mine], col_wx.at[mine], line_sent.at[2], line_came.at[2], mirror)
    o_half = pl.ds(pl.multiple_of(c * (row_o.shape[0] // 2), row_o.shape[0] // 2), row_o.shape[0] // 2)
    send(row_o.at[o_half], row_ox.at[o_half], line_sent.at[3], line_came.at[3], mirror)
    send(col_o.at[o_half], col_ox.at[o_half], line_sent.at[4], line_came.at[4], mirror)
    send(final, final_x, line_sent.at[5], line_came.at[5], mirror)

    def to_owner(i, carry):
        to = lax.rem(chip + i, chips)
        send(sides.at[to], sides_all.at[c, chip], s_sent, s_came.at[z], (*chip_at(to), c, r))
        return carry

    lax.fori_loop(1, plane, to_owner, 0)

    @pl.when(c == r)
    def _():
        wait_bytes(bias_all.at[0, 0, pl.ds(0, deep - 1)], line_came.at[0])

    @pl.when(c != r)
    def _():
        wait_bytes(bias_all.at[0, 0], line_came.at[0])

    def plane_device(i):
        to = lax.rem(xy + i, plane)
        return (z, to // high, lax.rem(to, high), c, r)

    def bias_plane(i, carry):
        send(bias_all.at[c, xy], bias_all.at[c, xy], bias_sent, bias_came.at[xy], plane_device(i))
        return carry

    lax.fori_loop(1, plane, bias_plane, 0)
    wait_bytes(row_wx.at[mine], line_came.at[1])
    wait_bytes(col_wx.at[mine], line_came.at[2])

    def weight_plane(i, carry):
        device = plane_device(i)
        send(row_wx.at[mine], row_wx.at[mine], row_sent, row_came.at[xy], device)
        send(col_wx.at[mine], col_wx.at[mine], col_sent, col_came.at[xy], device)
        return carry

    lax.fori_loop(1, plane, weight_plane, 0)
    lax.fori_loop(plane, chips, to_owner, 0)

    send(bias_all.at[c, xy], bias_all.at[c, xy], core_sent.at[0], core_came.at[0], partner)
    send(row_wx.at[mine], row_wx.at[mine], core_sent.at[1], core_came.at[1], partner)
    send(col_wx.at[mine], col_wx.at[mine], core_sent.at[2], core_came.at[2], partner)
    wait_bytes(row_ox.at[o_half], line_came.at[3])
    send(row_ox.at[o_half], row_ox.at[o_half], core_sent.at[3], core_came.at[3], partner)
    wait_bytes(col_ox.at[o_half], line_came.at[4])
    send(col_ox.at[o_half], col_ox.at[o_half], core_sent.at[4], core_came.at[4], partner)

    def bias_core(i, carry):
        at = lax.rem(xy + i, plane)
        wait_bytes(bias_all.at[c, at], bias_came.at[at])
        send(bias_all.at[c, at], bias_all.at[c, at], core_sent.at[0], core_came.at[0], partner)
        return carry

    lax.fori_loop(1, plane, bias_core, 0)

    def weight_core(i, carry):
        at = lax.rem(xy + i, plane)
        rows = rows_of(at)
        wait_bytes(row_wx.at[rows], row_came.at[at])
        send(row_wx.at[rows], row_wx.at[rows], core_sent.at[1], core_came.at[1], partner)
        wait_bytes(col_wx.at[rows], col_came.at[at])
        send(col_wx.at[rows], col_wx.at[rows], core_sent.at[2], core_came.at[2], partner)
        return carry

    lax.fori_loop(1, plane, weight_core, 0)

    def pass_sides(level):
        for n in range(4):
            part = pl.ds(pl.multiple_of(level * plane + n * high, high), high)
            send(sides_all.at[c, part], sides_all.at[c, part], core_sent.at[5], core_came.at[5], partner)

    wait_bytes(sides_all.at[0, pl.ds(0, plane - 1)], s_came.at[z])
    pass_sides(z)
    for dz in range(1, deep):
        level = lax.rem(z + dz, deep)
        wait_bytes(sides_all.at[0, pl.ds(0, plane)], s_came.at[level])
        pass_sides(level)

    wait_bytes(sides_all.at[0], core_came.at[5])
    site = lax.broadcasted_iota(jnp.int32, (sites, chips), 0)
    owner = lax.broadcasted_iota(jnp.int32, (sites, chips), 1)

    def side_of(core, t, n):
        part = sides_all[core, :, :, t * sites : (t + 1) * sites].astype(jnp.float32)
        return part[:, n, :].astype(jnp.bfloat16)

    rights = jnp.zeros((sites, sites), jnp.float32)
    for core in range(2):
        for t in range(rows_each):
            put = site == owner * (2 * rows_each) + (core * rows_each + t)
            rights += dot(put.astype(jnp.float32).astype(jnp.bfloat16), side_of(core, t, 1))
    rights = rights.astype(jnp.bfloat16)
    parts = [dot_last(side_of(c, t, 0), rights)[:, None, :] for t in range(rows_each)]
    rows[...] = jnp.concatenate(parts, 1).astype(jnp.bfloat16)
    product[channel] = rows[chip]

    def to_rows(i, carry):
        to = lax.rem(chip + i, chips)
        send(rows.at[to], product.at[channel], p_sent, p_came, (*chip_at(to), c, 1 - r))
        send(rows.at[to], product.at[channel], p_sent, p_came, (*chip_at(to), c, r))
        return carry

    lax.fori_loop(1, chips, to_rows, 0)
    send(rows.at[chip], product.at[channel], p_sent, p_came, (*here, c, 1 - r))

    half_rows = pl.ds(0, plane * chunk)
    wait_bytes(bias_all.at[0], core_came.at[0])
    wait_bytes(row_wx.at[half_rows], core_came.at[1])
    wait_bytes(row_ox.at[o_half], core_came.at[3])
    away = hidden[...]

    def place_bias(p, carry):
        at, level = lax.rem(p, plane), p // plane
        both = jnp.concatenate(
            [
                bias_all[r, at, level].astype(jnp.float32),
                bias_all[1 - r, at, level].astype(jnp.float32),
            ],
            0,
        )
        for t in range(rows_each):
            bias_rows[t * chips + p] = both[:, t * sites : (t + 1) * sites] + away
        return carry

    lax.fori_loop(0, chips, place_bias, 0)

    def part_of(n):
        return slice(n * embed, (n + 1) * embed)

    def one(s, carry):
        x = standardize_features(msa[s]).astype(jnp.bfloat16)
        xq = dot(pick[...], x).astype(jnp.bfloat16)
        q = project(xq, row_w[part_of(0)], row_wx[part_of(0)])
        k = project(x, row_w[part_of(1)], row_wx[part_of(1)])
        v = project(x, row_w[part_of(2)], row_wx[part_of(2)])
        g = project(xq, row_w[part_of(3)], row_wx[part_of(3)])

        def bias_of(n):
            return bias_rows[n * block : (n + 1) * block].reshape(block * heads, sites)

        attend_rows(q, k, v, g, bias_of, mixed, block, heads)
        half = row_o.shape[0]
        delta = dot(mixed[:, :half], row_o[...]) + dot(mixed[:, half:], row_ox[...])
        done[s] = dot(pick[...], msa[s]) + delta
        return carry

    lax.fori_loop(0, msa.shape[0], one, 0)
    for t in range(rows_each):
        part = slice(t * chips, (t + 1) * chips)
        both = jnp.concatenate([done[0, part, :][:, None, :], done[1, part, :][:, None, :]], 1)
        seqs[:, :, t * embed : (t + 1) * embed] = both.astype(jnp.bfloat16)

    @pl.when(c == r)
    def _():
        column[me] = seqs[chip]

    def to_owner(i, carry):
        to = lax.rem(chip + i, chips)
        send(seqs.at[to], column.at[me], m_sent, m_came, (*chip_at(to), r, 1 - r))
        send(seqs.at[to], column.at[me], m_sent, m_came, (*chip_at(to), r, r))
        return carry

    lax.fori_loop(1, chips, to_owner, 0)

    @pl.when(c != r)
    def _():
        send(seqs.at[chip], column.at[me], m_sent, m_came, (*here, r, r))

    send(seqs.at[chip], column.at[me], m_sent, m_came, (*here, r, 1 - r))

    for sem in (m_came, m_sent):

        @pl.when(c == r)
        def _():
            wait_bytes(column.at[pl.ds(0, 2 * chips - 1)], sem)

        @pl.when(c != r)
        def _():
            wait_bytes(column, sem)

    for sem in (p_came, p_sent):
        wait_bytes(product.at[pl.ds(0, 2 * chips - 1)], sem)

    half = pl.ds(0, plane * chunk)
    rest = pl.ds(0, (plane - 1) * chunk)
    wait_bytes(final_x, line_came.at[5])
    for sems in (core_came, core_sent):
        wait_bytes(col_wx.at[half], sems.at[2])
        wait_bytes(col_ox.at[o_half], sems.at[4])

    wait_bytes(bias_all.at[0], core_sent.at[0])
    wait_bytes(row_wx.at[half], core_sent.at[1])
    wait_bytes(row_ox.at[o_half], core_sent.at[3])
    wait_bytes(sides_all.at[0], core_sent.at[5])

    @pl.when(c == r)
    def _():
        wait_bytes(bias_all.at[0, 0, pl.ds(0, deep - 1)], line_sent.at[0])

    @pl.when(c != r)
    def _():
        wait_bytes(bias_all.at[0, 0], line_sent.at[0])

    wait_bytes(row_wx.at[mine], line_sent.at[1])
    wait_bytes(col_wx.at[mine], line_sent.at[2])
    wait_bytes(row_ox.at[o_half], line_sent.at[3])
    wait_bytes(col_ox.at[o_half], line_sent.at[4])
    wait_bytes(final_x, line_sent.at[5])
    wait_bytes(bias_all.at[0, pl.ds(0, plane - 1)], bias_sent)
    wait_bytes(row_wx.at[rest], row_sent)
    wait_bytes(col_wx.at[rest], col_sent)
    wait_bytes(sides_all.at[0, pl.ds(0, chips - 1)], s_sent)


def col_kernel(column, hidden, w, wx, wo, wox, out, mixed, *, heads, block):
    r = lax.axis_index("rep")
    embed = w.shape[1]
    width = embed // 2
    at = pl.ds(pl.multiple_of(r * width, width), width)
    away = hidden[...]
    for t in range(column.shape[1] // embed):
        x = standardize_features(column[:, t * embed : (t + 1) * embed]).astype(jnp.bfloat16)
        q, k, v, g = [project(x, w[n], wx[n]) for n in range(4)]
        attend_rows(q, k, v, g, lambda n: away, mixed, block, heads)
        half = wo.shape[0]
        delta = dot(mixed[:, :half], wo[:, at]) + dot(mixed[:, half:], wox[:, at])
        keep = column[:, pl.ds(pl.multiple_of(t * embed + r * width, width), width)]
        out[:, t * width : (t + 1) * width] = (keep.astype(jnp.float32) + delta).astype(jnp.bfloat16)


def local_call(kernel, out, scratch, flops, *operands):
    return pl.pallas_call(
        kernel,
        out_shape=jax.ShapeDtypeStruct(out, jnp.bfloat16),
        in_specs=[VMEM] * len(operands),
        out_specs=VMEM,
        scratch_shapes=[pltpu.VMEM(*s) for s in scratch],
        compiler_params=pltpu.CompilerParams(vmem_limit_bytes=40 << 20),
        cost_estimate=pl.CostEstimate(flops=flops, bytes_accessed=4 << 20, transcendentals=0),
    )(*operands)


def per_device(
    msa,
    pair,
    homolog_present,
    amino_present,
    row_w,
    row_out,
    offset_w,
    col_w,
    col_out,
    side_w,
    final_w,
    sigmoid_w,
):
    rep = lax.axis_index("rep")
    rows_here, sites, channels = pair.shape
    seqs_here, embed = msa.shape[0], msa.shape[2]
    chips = lax.axis_size(CHIPS)
    devices = lax.axis_size(DAP)
    heads_here = offset_w.shape[1]
    heads = 2 * heads_here
    row_start = lax.axis_index(DAP) * rows_here
    res_float = amino_present.astype(jnp.float32)
    mask_rows = lax.dynamic_slice_in_dim(res_float, row_start, rows_here, 0)
    flat = rows_here * sites
    pair_mask = mask_rows[:, None] * res_float[None, :]
    flat_w = (row_w.shape[0] * row_w.shape[1], row_w.shape[2])
    queries = chips * rows_here
    query = lax.broadcasted_iota(jnp.int32, (queries, sites), 0)
    site = lax.broadcasted_iota(jnp.int32, (queries, sites), 1)
    picked = 2 * rows_here * (query % chips) + rows_here * rep + query // chips
    pick = (site == picked).astype(jnp.bfloat16)
    hidden = (NEG * (res_float - 1.0))[None, :]
    operands = (
        pair,
        pair_mask,
        offset_w.T,
        side_w.swapaxes(1, 2),
        row_w.reshape(flat_w),
        col_w.reshape(flat_w),
        row_out,
        col_out,
        final_w,
        msa,
        pick,
        hidden,
    )
    side_channels = side_w.shape[2]
    bf = jnp.bfloat16
    outs = [
        pair.shape,
        (devices, seqs_here, rows_here * embed),
        (devices, rows_here, sites),
        flat_w,
        col_out.shape,
        final_w.shape,
    ]
    scratch = [
        ((heads_here, flat), bf),
        ((side_channels, 2, flat), bf),
        ((2, 16, chips // 16, heads_here, flat), bf),
        ((2, chips, 2, flat), bf),
        (flat_w, bf),
        (row_out.shape, bf),
        ((chips, rows_here, sites), bf),
        ((queries, heads, sites), jnp.float32),
        ((queries, embed), bf),
        ((seqs_here, queries, embed), jnp.float32),
        ((chips, seqs_here, rows_here * embed), bf),
    ]
    semaphores = [0, 4, 6, 6, 0, 16, 0, 16, 0, 16, 6, 6, 0, 0, 0, 0]
    pair_ln, column, product, col_wx, col_ox, final_x = pl.pallas_call(
        functools.partial(main_kernel, heads=heads, block=24),
        out_shape=[jax.ShapeDtypeStruct(shape, bf) for shape in outs],
        in_specs=[VMEM] * len(operands),
        out_specs=[VMEM] * len(outs),
        scratch_shapes=[pltpu.VMEM(*one) for one in scratch]
        + [pltpu.SemaphoreType.DMA if n == 0 else pltpu.SemaphoreType.DMA((n,)) for n in semaphores],
        compiler_params=pltpu.CompilerParams(
            collective_id=0, has_side_effects=True, vmem_limit_bytes=48 << 20
        ),
    )(*operands)
    pair_ln = pair_ln.reshape(flat, channels)

    column = column.reshape(devices * seqs_here, rows_here * embed)
    away = (NEG * (homolog_present.astype(jnp.float32) - 1.0))[None, :]
    width = embed // 2
    alignment_output = local_call(
        functools.partial(col_kernel, heads=heads, block=32),
        (devices * seqs_here, rows_here * width),
        [((devices * seqs_here, embed), jnp.bfloat16)],
        3 << 30,
        column,
        away,
        col_w,
        col_wx.reshape(col_w.shape),
        col_out,
        col_ox,
    ).reshape(devices * seqs_here, rows_here, width)

    product = product.astype(jnp.float32)
    mean = jnp.mean(product, axis=0)
    square = jnp.mean(product * product, axis=0)
    scaled = ((product - mean) * lax.rsqrt(square - mean * mean + EPS)).astype(jnp.bfloat16)
    half = channels // 2
    first = jnp.where(rep == 0, final_w, final_x)
    second = jnp.where(rep == 0, final_x, final_w)
    final_all = jnp.concatenate([first, second], 0)
    final_half = lax.dynamic_slice_in_dim(final_all, rep * half, half, 1)
    tri_update = jnp.einsum("cij,cz->ijz", scaled, final_half, preferred_element_type=jnp.float32)
    pair_half = lax.dynamic_slice_in_dim(pair, rep * half, half, 2)
    gate_out = jax.nn.sigmoid(dot(pair_ln, sigmoid_w)).reshape(rows_here, sites, half)
    pair_output = (pair_half.astype(jnp.float32) + gate_out * tri_update).astype(jnp.bfloat16)
    return (alignment_output, pair_output)


def solution(mesh):
    finer = Mesh(
        mesh.devices.reshape(4, 4, 4, 2, mesh.shape["rep"]),
        (*DAP, "rep"),
    )
    return jax.shard_map(
        per_device,
        mesh=finer,
        in_specs=(
            P(DAP, None, None),
            P(DAP, None, None),
            P(),
            P(),
            P(None, None, "rep"),
            P("rep", None),
            P(None, "rep"),
            P(None, None, "rep"),
            P("rep", None),
            P(None, None, "rep"),
            P("rep", None),
            P(None, "rep"),
        ),
        out_specs=(P(None, DAP, "rep"), P(DAP, None, "rep")),
        check_vma=False,
    )
```

```python
import functools

import jax
import jax.numpy as jnp
from jax import lax
from jax.experimental import pallas as pl
from jax.experimental.pallas import tpu as pltpu
from jax.sharding import Mesh
from jax.sharding import PartitionSpec as P

GROUP_BREADTH = 32
CHIPS = ("dap_0", "dap_1", "dap_2")
CORE = "dap_3"
DAP = CHIPS + (CORE,)
MESH = pl.DeviceIdType.MESH
VMEM = pl.BlockSpec(memory_space=pltpu.VMEM)

EPS = 1e-05
NEG = 1000000000.0


def standardize_features(values):
    values = values.astype(jnp.float32)
    center = jnp.mean(values, axis=-1, keepdims=True)
    spread = jnp.mean(jnp.square(values - center), axis=-1, keepdims=True)
    return (values - center) * lax.rsqrt(spread + EPS)


def place():
    z, x, y = (lax.axis_index(a) for a in CHIPS)
    return z, x, y, lax.axis_index(CORE), lax.axis_index("rep")


def send(src, dst, sent, came, device):
    pltpu.make_async_remote_copy(
        src_ref=src, dst_ref=dst, send_sem=sent, recv_sem=came, device_id=device, device_id_type=MESH
    ).start()


def wait_bytes(ref, sem):
    pltpu.make_async_copy(ref, ref, sem).wait()


def greet(device):
    pl.semaphore_signal(pltpu.get_barrier_semaphore(), inc=1, device_id=device, device_id_type=MESH)


def chip_at(to):
    plane, high = 16, 4
    return to // plane, lax.rem(to // high, high), lax.rem(to, high)


def dot_last(a, b):
    return lax.dot_general(a, b, (((1,), (1,)), ((), ())), preferred_element_type=jnp.float32)


def dot(a, b):
    return jnp.dot(a, b, preferred_element_type=jnp.float32)


def project(x, own, other):
    return jnp.concatenate([dot(x, own), dot(x, other)], 1).astype(jnp.bfloat16)


def attend_rows(q, k, v, g, bias, mixed, block, heads):
    embed = q.shape[1]
    queries = q.shape[0]
    lane = lax.broadcasted_iota(jnp.int32, (heads, embed), 1) // GROUP_BREADTH
    head = lax.broadcasted_iota(jnp.int32, (heads, embed), 0)
    own = (lane == head).astype(jnp.float32)[None]
    scale = 1.0 / jnp.sqrt(jnp.float32(GROUP_BREADTH))

    for n in range(queries // block):
        part = slice(n * block, (n + 1) * block)
        wide = q[part].astype(jnp.float32)[:, None, :] * own
        wide = wide.reshape(block * heads, embed).astype(jnp.bfloat16)
        scores = dot_last(wide, k) * scale + bias(n)
        scores = jnp.exp(scores - jnp.max(scores, axis=1, keepdims=True))
        weights = (scores * (1.0 / jnp.sum(scores, axis=1, keepdims=True))).astype(jnp.bfloat16)
        out = dot(weights, v).reshape(block, heads, embed) * own
        out = jnp.sum(out, axis=1)
        gate = 1.0 / (1.0 + jnp.exp(-g[part].astype(jnp.float32)))
        mixed[part, :] = (out * gate).astype(jnp.bfloat16)


def main_kernel(
    pair_in,
    side_in,
    msa_in,
    row_w_in,
    row_o_in,
    col_w_in,
    col_o_in,
    pair_mask,
    offset_w,
    final,
    sigmoid_w,
    pick,
    hidden,
    pair_out,
    column,
    col_wx,
    col_ox,
    pair,
    side_w,
    msa,
    row_w,
    row_o,
    pair_ln,
    product,
    final_x,
    bias,
    sides,
    bias_all,
    sides_all,
    row_wx,
    row_ox,
    rows,
    bias_rows,
    mixed,
    done,
    seqs,
    s_sent,
    s_came,
    line_sent,
    line_came,
    bias_sent,
    bias_came,
    row_sent,
    row_came,
    col_sent,
    col_came,
    core_sent,
    core_came,
    p_sent,
    p_came,
    m_sent,
    m_came,
    loaded,
    *,
    heads,
    block,
):
    loads = []
    moves = [(pair_in, pair), (side_in, side_w), (msa_in, msa), (row_w_in, row_w), (row_o_in, row_o)]
    for n, (src, dst) in enumerate(moves):
        loads.append(pltpu.make_async_copy(src, dst, loaded.at[n]))
        loads[-1].start()
    z, x, y, c, r = place()
    deep, high = 4, 4
    plane = high * high
    chips = deep * plane
    xy = x * high + y
    chip = z * plane + xy
    me = chip * 2 + c
    channel = r * chips + chip
    here = (z, x, y)
    chunk = row_w.shape[0] // (2 * plane)
    mirror = (deep - 1 - z, x, y, c, 1 - r)
    partner = (z, x, y, 1 - c, r)
    rows_each, sites = pair.shape[0], pair.shape[1]
    embed = msa.shape[2]

    def rows_of(at):
        return pl.ds(pl.multiple_of((c * plane + at) * chunk, chunk), chunk)

    mine = rows_of(xy)

    def greet_chip(i, carry):
        there = chip_at(lax.rem(chip + i, chips))
        for ct in range(2):
            for rt in range(2):
                greet((*there, ct, rt))
        return carry

    lax.fori_loop(1, chips, greet_chip, 0)
    greet((*here, 1 - c, r))
    greet((*here, c, 1 - r))
    greet((*here, 1 - c, 1 - r))

    loads[0].wait()
    loads[1].wait()
    for t in range(rows_each):
        part = slice(t * sites, (t + 1) * sites)
        normed = standardize_features(pair[t]).astype(jnp.bfloat16)
        pair_ln[t] = normed
        bias[:, part] = dot_last(offset_w[...], normed).astype(jnp.bfloat16)
        both = []
        for n in range(2):
            gate = dot_last(side_w[2 * n], normed)
            value = dot_last(side_w[2 * n + 1], normed)
            side = value / (1.0 + jnp.exp(-gate)) * pair_mask[t : t + 1, :]
            both.append(side[:, None, :])
        sides[:, :, part] = jnp.concatenate(both, 1).astype(jnp.bfloat16)
    sides_all[c, chip] = sides[chip]

    @pl.when(c == r)
    def _():
        bias_all[r, xy, z] = bias[...]

    pl.semaphore_wait(pltpu.get_barrier_semaphore(), 4 * chips - 1)

    for dz in range(deep):
        zt = lax.rem(z + dz, deep)
        if dz == 0:

            @pl.when(c != r)
            def _():
                send(bias, bias_all.at[r, xy, z], line_sent.at[0], line_came.at[0], (zt, x, y, r, c))

        else:
            send(bias, bias_all.at[r, xy, z], line_sent.at[0], line_came.at[0], (zt, x, y, r, c))
    send(row_w_in.at[mine], row_wx.at[mine], line_sent.at[1], line_came.at[1], mirror)
    send(col_w_in.at[mine], col_wx.at[mine], line_sent.at[2], line_came.at[2], mirror)
    o_half = pl.ds(pl.multiple_of(c * (row_o.shape[0] // 2), row_o.shape[0] // 2), row_o.shape[0] // 2)
    send(row_o_in.at[o_half], row_ox.at[o_half], line_sent.at[3], line_came.at[3], mirror)
    send(col_o_in.at[o_half], col_ox.at[o_half], line_sent.at[4], line_came.at[4], mirror)
    send(final, final_x, line_sent.at[5], line_came.at[5], mirror)

    def to_owner(i, carry):
        to = lax.rem(chip + i, chips)
        send(sides.at[to], sides_all.at[c, chip], s_sent, s_came.at[z], (*chip_at(to), c, r))
        return carry

    lax.fori_loop(1, plane, to_owner, 0)

    @pl.when(c == r)
    def _():
        wait_bytes(bias_all.at[0, 0, pl.ds(0, deep - 1)], line_came.at[0])

    @pl.when(c != r)
    def _():
        wait_bytes(bias_all.at[0, 0], line_came.at[0])

    def plane_device(i):
        to = lax.rem(xy + i, plane)
        return (z, to // high, lax.rem(to, high), c, r)

    def bias_plane(i, carry):
        send(bias_all.at[c, xy], bias_all.at[c, xy], bias_sent, bias_came.at[xy], plane_device(i))
        return carry

    lax.fori_loop(1, plane, bias_plane, 0)
    wait_bytes(row_wx.at[mine], line_came.at[1])
    wait_bytes(col_wx.at[mine], line_came.at[2])

    def weight_plane(i, carry):
        device = plane_device(i)
        send(row_wx.at[mine], row_wx.at[mine], row_sent, row_came.at[xy], device)
        send(col_wx.at[mine], col_wx.at[mine], col_sent, col_came.at[xy], device)
        return carry

    lax.fori_loop(1, plane, weight_plane, 0)
    lax.fori_loop(plane, chips, to_owner, 0)

    send(bias_all.at[c, xy], bias_all.at[c, xy], core_sent.at[0], core_came.at[0], partner)
    send(row_wx.at[mine], row_wx.at[mine], core_sent.at[1], core_came.at[1], partner)
    send(col_wx.at[mine], col_wx.at[mine], core_sent.at[2], core_came.at[2], partner)
    wait_bytes(row_ox.at[o_half], line_came.at[3])
    send(row_ox.at[o_half], row_ox.at[o_half], core_sent.at[3], core_came.at[3], partner)
    wait_bytes(col_ox.at[o_half], line_came.at[4])
    send(col_ox.at[o_half], col_ox.at[o_half], core_sent.at[4], core_came.at[4], partner)

    def bias_core(i, carry):
        at = lax.rem(xy + i, plane)
        wait_bytes(bias_all.at[c, at], bias_came.at[at])
        send(bias_all.at[c, at], bias_all.at[c, at], core_sent.at[0], core_came.at[0], partner)
        return carry

    lax.fori_loop(1, plane, bias_core, 0)

    def weight_core(i, carry):
        at = lax.rem(xy + i, plane)
        rows = rows_of(at)
        wait_bytes(row_wx.at[rows], row_came.at[at])
        send(row_wx.at[rows], row_wx.at[rows], core_sent.at[1], core_came.at[1], partner)
        wait_bytes(col_wx.at[rows], col_came.at[at])
        send(col_wx.at[rows], col_wx.at[rows], core_sent.at[2], core_came.at[2], partner)
        return carry

    lax.fori_loop(1, plane, weight_core, 0)

    def pass_sides(level):
        for n in range(4):
            part = pl.ds(pl.multiple_of(level * plane + n * high, high), high)
            send(sides_all.at[c, part], sides_all.at[c, part], core_sent.at[5], core_came.at[5], partner)

    wait_bytes(sides_all.at[0, pl.ds(0, plane - 1)], s_came.at[z])
    pass_sides(z)
    for dz in range(1, deep):
        level = lax.rem(z + dz, deep)
        wait_bytes(sides_all.at[0, pl.ds(0, plane)], s_came.at[level])
        pass_sides(level)

    wait_bytes(sides_all.at[0], core_came.at[5])
    site = lax.broadcasted_iota(jnp.int32, (sites, chips), 0)
    owner = lax.broadcasted_iota(jnp.int32, (sites, chips), 1)

    def side_of(core, t, n):
        part = sides_all[core, :, :, t * sites : (t + 1) * sites].astype(jnp.float32)
        return part[:, n, :].astype(jnp.bfloat16)

    rights = jnp.zeros((sites, sites), jnp.float32)
    for core in range(2):
        for t in range(rows_each):
            put = site == owner * (2 * rows_each) + (core * rows_each + t)
            rights += dot(put.astype(jnp.float32).astype(jnp.bfloat16), side_of(core, t, 1))
    rights = rights.astype(jnp.bfloat16)
    parts = [dot_last(side_of(c, t, 0), rights)[:, None, :] for t in range(rows_each)]
    rows[...] = jnp.concatenate(parts, 1).astype(jnp.bfloat16)
    product[channel] = rows[chip]

    def to_rows(i, carry):
        to = lax.rem(chip + i, chips)
        send(rows.at[to], product.at[channel], p_sent, p_came, (*chip_at(to), c, 1 - r))
        send(rows.at[to], product.at[channel], p_sent, p_came, (*chip_at(to), c, r))
        return carry

    lax.fori_loop(1, chips, to_rows, 0)
    send(rows.at[chip], product.at[channel], p_sent, p_came, (*here, c, 1 - r))

    half_rows = pl.ds(0, plane * chunk)
    wait_bytes(bias_all.at[0], core_came.at[0])
    wait_bytes(row_wx.at[half_rows], core_came.at[1])
    wait_bytes(row_ox.at[o_half], core_came.at[3])
    for load in loads[2:]:
        load.wait()
    away = hidden[...]

    def place_bias(p, carry):
        at, level = lax.rem(p, plane), p // plane
        both = jnp.concatenate(
            [
                bias_all[r, at, level].astype(jnp.float32),
                bias_all[1 - r, at, level].astype(jnp.float32),
            ],
            0,
        )
        for t in range(rows_each):
            bias_rows[t * chips + p] = both[:, t * sites : (t + 1) * sites] + away
        return carry

    lax.fori_loop(0, chips, place_bias, 0)

    def part_of(n):
        return slice(n * embed, (n + 1) * embed)

    def one(s, carry):
        x = standardize_features(msa[s]).astype(jnp.bfloat16)
        xq = dot(pick[...], x).astype(jnp.bfloat16)
        q = project(xq, row_w[part_of(0)], row_wx[part_of(0)])
        k = project(x, row_w[part_of(1)], row_wx[part_of(1)])
        v = project(x, row_w[part_of(2)], row_wx[part_of(2)])
        g = project(xq, row_w[part_of(3)], row_wx[part_of(3)])

        def bias_of(n):
            return bias_rows[n * block : (n + 1) * block].reshape(block * heads, sites)

        attend_rows(q, k, v, g, bias_of, mixed, block, heads)
        half = row_o.shape[0]
        delta = dot(mixed[:, :half], row_o[...]) + dot(mixed[:, half:], row_ox[...])
        done[s] = dot(pick[...], msa[s]) + delta
        return carry

    lax.fori_loop(0, msa.shape[0], one, 0)
    for t in range(rows_each):
        part = slice(t * chips, (t + 1) * chips)
        both = jnp.concatenate([done[0, part, :][:, None, :], done[1, part, :][:, None, :]], 1)
        seqs[:, :, t * embed : (t + 1) * embed] = both.astype(jnp.bfloat16)

    @pl.when(c == r)
    def _():
        column[me] = seqs[chip]

    def to_owner(i, carry):
        to = lax.rem(chip + i, chips)
        send(seqs.at[to], column.at[me], m_sent, m_came, (*chip_at(to), r, 1 - r))
        send(seqs.at[to], column.at[me], m_sent, m_came, (*chip_at(to), r, r))
        return carry

    lax.fori_loop(1, chips, to_owner, 0)

    @pl.when(c != r)
    def _():
        send(seqs.at[chip], column.at[me], m_sent, m_came, (*here, r, r))

    send(seqs.at[chip], column.at[me], m_sent, m_came, (*here, r, 1 - r))

    wait_bytes(product.at[pl.ds(0, 2 * chips - 1)], p_came)
    wait_bytes(final_x, line_came.at[5])
    ours, theirs = final[...].astype(jnp.float32), final_x[...].astype(jnp.float32)
    first = jnp.where(r == 0, ours, theirs)
    second = jnp.where(r == 0, theirs, ours)
    finals = jnp.concatenate([first, second], 0).astype(jnp.bfloat16)
    width = pair_out.shape[1]

    def half_of(values):
        return jnp.where(r == 0, values[:width], values[width:])

    products = product[...].astype(jnp.float32)
    for t in range(rows_each):
        value = products[:, t, :]
        mean = jnp.mean(value, axis=0, keepdims=True)
        square = jnp.mean(value * value, axis=0, keepdims=True)
        scaled = ((value - mean) * lax.rsqrt(square - mean * mean + EPS)).astype(jnp.bfloat16)
        update = lax.dot_general(
            finals, scaled, (((0,), (0,)), ((), ())), preferred_element_type=jnp.float32
        )
        gate = 1.0 / (1.0 + jnp.exp(-dot_last(sigmoid_w[...], pair_ln[t])))
        keep = half_of(pair[t].astype(jnp.float32).T)
        pair_out[t] = (keep + gate * half_of(update)).astype(jnp.bfloat16)

    for sem in (m_came, m_sent):

        @pl.when(c == r)
        def _():
            wait_bytes(column.at[pl.ds(0, 2 * chips - 1)], sem)

        @pl.when(c != r)
        def _():
            wait_bytes(column, sem)

    wait_bytes(product.at[pl.ds(0, 2 * chips - 1)], p_sent)

    half = pl.ds(0, plane * chunk)
    rest = pl.ds(0, (plane - 1) * chunk)
    for sems in (core_came, core_sent):
        wait_bytes(col_wx.at[half], sems.at[2])
        wait_bytes(col_ox.at[o_half], sems.at[4])

    wait_bytes(bias_all.at[0], core_sent.at[0])
    wait_bytes(row_wx.at[half], core_sent.at[1])
    wait_bytes(row_ox.at[o_half], core_sent.at[3])
    wait_bytes(sides_all.at[0], core_sent.at[5])

    @pl.when(c == r)
    def _():
        wait_bytes(bias_all.at[0, 0, pl.ds(0, deep - 1)], line_sent.at[0])

    @pl.when(c != r)
    def _():
        wait_bytes(bias_all.at[0, 0], line_sent.at[0])

    wait_bytes(row_wx.at[mine], line_sent.at[1])
    wait_bytes(col_wx.at[mine], line_sent.at[2])
    wait_bytes(row_ox.at[o_half], line_sent.at[3])
    wait_bytes(col_ox.at[o_half], line_sent.at[4])
    wait_bytes(final_x, line_sent.at[5])
    wait_bytes(bias_all.at[0, pl.ds(0, plane - 1)], bias_sent)
    wait_bytes(row_wx.at[rest], row_sent)
    wait_bytes(col_wx.at[rest], col_sent)
    wait_bytes(sides_all.at[0, pl.ds(0, chips - 1)], s_sent)


def col_kernel(column, hidden, w, wx, wo, wox, out, mixed, *, heads, block):
    r = lax.axis_index("rep")
    embed = w.shape[1]
    width = embed // 2
    at = pl.ds(pl.multiple_of(r * width, width), width)
    away = hidden[...]
    for t in range(column.shape[1] // embed):
        x = standardize_features(column[:, t * embed : (t + 1) * embed]).astype(jnp.bfloat16)
        q, k, v, g = [project(x, w[n], wx[n]) for n in range(4)]
        attend_rows(q, k, v, g, lambda n: away, mixed, block, heads)
        half = wo.shape[0]
        delta = dot(mixed[:, :half], wo[:, at]) + dot(mixed[:, half:], wox[:, at])
        keep = column[:, pl.ds(pl.multiple_of(t * embed + r * width, width), width)]
        out[t] = (keep.astype(jnp.float32) + delta).astype(jnp.bfloat16)


def local_call(kernel, out, scratch, flops, *operands):
    return pl.pallas_call(
        kernel,
        out_shape=jax.ShapeDtypeStruct(out, jnp.bfloat16),
        in_specs=[VMEM] * len(operands),
        out_specs=VMEM,
        scratch_shapes=[pltpu.VMEM(*s) for s in scratch],
        compiler_params=pltpu.CompilerParams(vmem_limit_bytes=40 << 20),
        cost_estimate=pl.CostEstimate(flops=flops, bytes_accessed=4 << 20, transcendentals=0),
    )(*operands)


def per_device(
    msa,
    pair,
    homolog_present,
    amino_present,
    row_w,
    row_out,
    offset_w,
    col_w,
    col_out,
    side_w,
    final_w,
    sigmoid_w,
):
    rep = lax.axis_index("rep")
    rows_here, sites, channels = pair.shape
    seqs_here, embed = msa.shape[0], msa.shape[2]
    chips = lax.axis_size(CHIPS)
    devices = lax.axis_size(DAP)
    heads_here = offset_w.shape[1]
    heads = 2 * heads_here
    row_start = lax.axis_index(DAP) * rows_here
    res_float = amino_present.astype(jnp.float32)
    mask_rows = lax.dynamic_slice_in_dim(res_float, row_start, rows_here, 0)
    flat = rows_here * sites
    pair_mask = mask_rows[:, None] * res_float[None, :]
    flat_w = (row_w.shape[0] * row_w.shape[1], row_w.shape[2])
    queries = chips * rows_here
    query = lax.broadcasted_iota(jnp.int32, (queries, sites), 0)
    site = lax.broadcasted_iota(jnp.int32, (queries, sites), 1)
    picked = 2 * rows_here * (query % chips) + rows_here * rep + query // chips
    pick = (site == picked).astype(jnp.bfloat16)
    hidden = (NEG * (res_float - 1.0))[None, :]
    operands = (
        pair,
        side_w.swapaxes(1, 2),
        msa,
        row_w.reshape(flat_w),
        row_out,
        col_w.reshape(flat_w),
        col_out,
        pair_mask,
        offset_w.T,
        final_w,
        sigmoid_w.T,
        pick,
        hidden,
    )
    side_channels = side_w.shape[2]
    half = channels // 2
    bf = jnp.bfloat16
    outs = [
        (rows_here, half, sites),
        (devices, seqs_here, rows_here * embed),
        flat_w,
        col_out.shape,
    ]
    scratch = [
        (pair.shape, bf),
        ((side_w.shape[0], side_channels, channels), bf),
        (msa.shape, bf),
        (flat_w, bf),
        (row_out.shape, bf),
        (pair.shape, bf),
        ((devices, rows_here, sites), bf),
        (final_w.shape, bf),
        ((heads_here, flat), bf),
        ((side_channels, 2, flat), bf),
        ((2, 16, chips // 16, heads_here, flat), bf),
        ((2, chips, 2, flat), bf),
        (flat_w, bf),
        (row_out.shape, bf),
        ((chips, rows_here, sites), bf),
        ((queries, heads, sites), jnp.float32),
        ((queries, embed), bf),
        ((seqs_here, queries, embed), jnp.float32),
        ((chips, seqs_here, rows_here * embed), bf),
    ]
    semaphores = [0, 4, 6, 6, 0, 16, 0, 16, 0, 16, 6, 6, 0, 0, 0, 0, 5]
    pair_output, column, col_wx, col_ox = pl.pallas_call(
        functools.partial(main_kernel, heads=heads, block=24),
        out_shape=[jax.ShapeDtypeStruct(shape, bf) for shape in outs],
        in_specs=[pl.BlockSpec(memory_space=pl.ANY)] * 7 + [VMEM] * (len(operands) - 7),
        out_specs=[VMEM] * len(outs),
        scratch_shapes=[pltpu.VMEM(*one) for one in scratch]
        + [pltpu.SemaphoreType.DMA if n == 0 else pltpu.SemaphoreType.DMA((n,)) for n in semaphores],
        compiler_params=pltpu.CompilerParams(
            collective_id=0, has_side_effects=True, vmem_limit_bytes=60 << 20
        ),
    )(*operands)
    column = column.reshape(devices * seqs_here, rows_here * embed)
    away = (NEG * (homolog_present.astype(jnp.float32) - 1.0))[None, :]
    width = embed // 2
    alignment_output = local_call(
        functools.partial(col_kernel, heads=heads, block=32),
        (rows_here, devices * seqs_here, width),
        [((devices * seqs_here, embed), jnp.bfloat16)],
        3 << 30,
        column,
        away,
        col_w,
        col_wx.reshape(col_w.shape),
        col_out,
        col_ox,
    ).swapaxes(0, 1)

    return (alignment_output, pair_output.swapaxes(1, 2))


def solution(mesh):
    finer = Mesh(
        mesh.devices.reshape(4, 4, 4, 2, mesh.shape["rep"]),
        (*DAP, "rep"),
    )
    return jax.shard_map(
        per_device,
        mesh=finer,
        in_specs=(
            P(DAP, None, None),
            P(DAP, None, None),
            P(),
            P(),
            P(None, None, "rep"),
            P("rep", None),
            P(None, "rep"),
            P(None, None, "rep"),
            P("rep", None),
            P(None, None, "rep"),
            P("rep", None),
            P(None, "rep"),
        ),
        out_specs=(P(None, DAP, "rep"), P(DAP, None, "rep")),
        check_vma=False,
    )
```

```python
import functools

import jax
import jax.numpy as jnp
from jax import lax
from jax.experimental import pallas as pl
from jax.experimental.pallas import tpu as pltpu
from jax.sharding import Mesh
from jax.sharding import PartitionSpec as P

GROUP_BREADTH = 32
CHIPS = ("dap_0", "dap_1", "dap_2")
CORE = "dap_3"
DAP = CHIPS + (CORE,)
MESH = pl.DeviceIdType.MESH
VMEM = pl.BlockSpec(memory_space=pltpu.VMEM)

EPS = 1e-05
NEG = 1000000000.0


def standardize_features(values):
    values = values.astype(jnp.float32)
    center = jnp.mean(values, axis=-1, keepdims=True)
    spread = jnp.mean(jnp.square(values - center), axis=-1, keepdims=True)
    return (values - center) * lax.rsqrt(spread + EPS)


def place():
    z, x, y = (lax.axis_index(a) for a in CHIPS)
    return z, x, y, lax.axis_index(CORE), lax.axis_index("rep")


def send(src, dst, sent, came, device):
    pltpu.make_async_remote_copy(
        src_ref=src, dst_ref=dst, send_sem=sent, recv_sem=came, device_id=device, device_id_type=MESH
    ).start()


def wait_bytes(ref, sem):
    pltpu.make_async_copy(ref, ref, sem).wait()


def greet(device):
    pl.semaphore_signal(pltpu.get_barrier_semaphore(), inc=1, device_id=device, device_id_type=MESH)


def chip_at(to):
    plane, high = 16, 4
    return to // plane, lax.rem(to // high, high), lax.rem(to, high)


def dot_last(a, b):
    return lax.dot_general(a, b, (((1,), (1,)), ((), ())), preferred_element_type=jnp.float32)


def dot(a, b):
    return jnp.dot(a, b, preferred_element_type=jnp.float32)


def project(x, own, other):
    return jnp.concatenate([dot(x, own), dot(x, other)], 1).astype(jnp.bfloat16)


def attend_rows(q, k, v, g, bias, mixed, block, heads):
    embed = q.shape[1]
    queries = q.shape[0]
    lane = lax.broadcasted_iota(jnp.int32, (heads, embed), 1) // GROUP_BREADTH
    head = lax.broadcasted_iota(jnp.int32, (heads, embed), 0)
    own = (lane == head).astype(jnp.float32)[None]
    scale = 1.0 / jnp.sqrt(jnp.float32(GROUP_BREADTH))

    for n in range(queries // block):
        part = slice(n * block, (n + 1) * block)
        wide = q[part].astype(jnp.float32)[:, None, :] * own
        wide = wide.reshape(block * heads, embed).astype(jnp.bfloat16)
        scores = dot_last(wide, k) * scale + bias(n)
        scores = jnp.exp(scores - jnp.max(scores, axis=1, keepdims=True))
        weights = (scores * (1.0 / jnp.sum(scores, axis=1, keepdims=True))).astype(jnp.bfloat16)
        out = dot(weights, v).reshape(block, heads, embed) * own
        out = jnp.sum(out, axis=1)
        gate = 1.0 / (1.0 + jnp.exp(-g[part].astype(jnp.float32)))
        mixed[part, :] = (out * gate).astype(jnp.bfloat16)


def over_chips(step, chips):
    def three(j, carry):
        for n in range(3):
            step(3 * j + n + 1, 0)
        return carry

    lax.fori_loop(0, (chips - 1) // 3, three, 0)


def main_kernel(
    pair_in,
    side_in,
    msa_in,
    row_w_in,
    row_o_in,
    col_w_in,
    col_o_in,
    amino,
    offset_w,
    final,
    sigmoid_w,
    pair_out,
    column,
    col_wx,
    col_ox,
    pair,
    side_w,
    msa,
    row_w,
    row_o,
    pair_ln,
    product,
    final_x,
    bias,
    sides,
    bias_all,
    sides_all,
    row_wx,
    row_ox,
    rows,
    bias_rows,
    mixed,
    done,
    seqs,
    s_sent,
    s_came,
    line_sent,
    line_came,
    bias_sent,
    bias_came,
    row_sent,
    row_came,
    col_sent,
    col_came,
    core_sent,
    core_came,
    p_sent,
    p_came,
    m_sent,
    m_came,
    loaded,
    pick,
    *,
    heads,
    block,
):
    loads = []
    moves = [(pair_in, pair), (side_in, side_w), (msa_in, msa), (row_w_in, row_w), (row_o_in, row_o)]
    for n, (src, dst) in enumerate(moves):
        loads.append(pltpu.make_async_copy(src, dst, loaded.at[n]))
        loads[-1].start()
    z, x, y, c, r = place()
    deep, high = 4, 4
    plane = high * high
    chips = deep * plane
    xy = x * high + y
    chip = z * plane + xy
    me = chip * 2 + c
    channel = r * chips + chip
    here = (z, x, y)
    chunk = row_w.shape[0] // (2 * plane)
    mirror = (deep - 1 - z, x, y, c, 1 - r)
    partner = (z, x, y, 1 - c, r)
    rows_each, sites = pair.shape[0], pair.shape[1]
    embed = msa.shape[2]

    def rows_of(at):
        return pl.ds(pl.multiple_of((c * plane + at) * chunk, chunk), chunk)

    mine = rows_of(xy)

    def greet_chip(i, carry):
        there = chip_at(lax.rem(chip + i, chips))
        for ct in range(2):
            for rt in range(2):
                greet((*there, ct, rt))
        return carry

    over_chips(greet_chip, chips)
    greet((*here, 1 - c, r))
    greet((*here, c, 1 - r))
    greet((*here, 1 - c, 1 - r))

    present = amino[...].astype(jnp.float32).reshape(1, sites)
    at_site = lax.broadcasted_iota(jnp.int32, (1, sites), 1)
    query = lax.broadcasted_iota(jnp.int32, pick.shape, 0)
    picked = 2 * rows_each * (query & (chips - 1)) + rows_each * r + query // chips
    pick[...] = jnp.where(
        lax.broadcasted_iota(jnp.int32, pick.shape, 1) == picked, 1.0, 0.0
    ).astype(jnp.bfloat16)

    loads[0].wait()
    loads[1].wait()
    for t in range(rows_each):
        part = slice(t * sites, (t + 1) * sites)
        normed = standardize_features(pair[t]).astype(jnp.bfloat16)
        pair_ln[t] = normed
        bias[:, part] = dot_last(offset_w[...], normed).astype(jnp.bfloat16)
        here_too = jnp.where(at_site == me * rows_each + t, present, 0.0)
        mask = present * jnp.sum(here_too, axis=1, keepdims=True)
        both = []
        for n in range(2):
            gate = dot_last(side_w[2 * n], normed)
            value = dot_last(side_w[2 * n + 1], normed)
            side = value / (1.0 + jnp.exp(-gate)) * mask
            both.append(side[:, None, :])
        sides[:, :, part] = jnp.concatenate(both, 1).astype(jnp.bfloat16)
    sides_all[c, chip] = sides[chip]

    @pl.when(c == r)
    def _():
        bias_all[r, xy, z] = bias[...]

    pl.semaphore_wait(pltpu.get_barrier_semaphore(), 4 * chips - 1)

    for dz in range(deep):
        zt = lax.rem(z + dz, deep)
        if dz == 0:

            @pl.when(c != r)
            def _():
                send(bias, bias_all.at[r, xy, z], line_sent.at[0], line_came.at[0], (zt, x, y, r, c))

        else:
            send(bias, bias_all.at[r, xy, z], line_sent.at[0], line_came.at[0], (zt, x, y, r, c))
    send(row_w_in.at[mine], row_wx.at[mine], line_sent.at[1], line_came.at[1], mirror)
    send(col_w_in.at[mine], col_wx.at[mine], line_sent.at[2], line_came.at[2], mirror)
    o_half = pl.ds(pl.multiple_of(c * (row_o.shape[0] // 2), row_o.shape[0] // 2), row_o.shape[0] // 2)
    send(row_o_in.at[o_half], row_ox.at[o_half], line_sent.at[3], line_came.at[3], mirror)
    send(col_o_in.at[o_half], col_ox.at[o_half], line_sent.at[4], line_came.at[4], mirror)
    send(final, final_x, line_sent.at[5], line_came.at[5], mirror)

    def to_owner(i, carry):
        to = lax.rem(chip + i, chips)
        send(sides.at[to], sides_all.at[c, chip], s_sent, s_came.at[z], (*chip_at(to), c, r))
        return carry

    lax.fori_loop(1, plane, to_owner, 0)

    @pl.when(c == r)
    def _():
        wait_bytes(bias_all.at[0, 0, pl.ds(0, deep - 1)], line_came.at[0])

    @pl.when(c != r)
    def _():
        wait_bytes(bias_all.at[0, 0], line_came.at[0])

    def plane_device(i):
        to = lax.rem(xy + i, plane)
        return (z, to // high, lax.rem(to, high), c, r)

    def bias_plane(i, carry):
        send(bias_all.at[c, xy], bias_all.at[c, xy], bias_sent, bias_came.at[xy], plane_device(i))
        return carry

    lax.fori_loop(1, plane, bias_plane, 0)
    wait_bytes(row_wx.at[mine], line_came.at[1])
    wait_bytes(col_wx.at[mine], line_came.at[2])

    def weight_plane(i, carry):
        device = plane_device(i)
        send(row_wx.at[mine], row_wx.at[mine], row_sent, row_came.at[xy], device)
        send(col_wx.at[mine], col_wx.at[mine], col_sent, col_came.at[xy], device)
        return carry

    lax.fori_loop(1, plane, weight_plane, 0)
    lax.fori_loop(plane, chips, to_owner, 0)

    send(bias_all.at[c, xy], bias_all.at[c, xy], core_sent.at[0], core_came.at[0], partner)
    send(row_wx.at[mine], row_wx.at[mine], core_sent.at[1], core_came.at[1], partner)
    send(col_wx.at[mine], col_wx.at[mine], core_sent.at[2], core_came.at[2], partner)
    wait_bytes(row_ox.at[o_half], line_came.at[3])
    send(row_ox.at[o_half], row_ox.at[o_half], core_sent.at[3], core_came.at[3], partner)
    wait_bytes(col_ox.at[o_half], line_came.at[4])
    send(col_ox.at[o_half], col_ox.at[o_half], core_sent.at[4], core_came.at[4], partner)

    def bias_core(i, carry):
        at = lax.rem(xy + i, plane)
        wait_bytes(bias_all.at[c, at], bias_came.at[at])
        send(bias_all.at[c, at], bias_all.at[c, at], core_sent.at[0], core_came.at[0], partner)
        return carry

    lax.fori_loop(1, plane, bias_core, 0)

    def weight_core(i, carry):
        at = lax.rem(xy + i, plane)
        rows = rows_of(at)
        wait_bytes(row_wx.at[rows], row_came.at[at])
        send(row_wx.at[rows], row_wx.at[rows], core_sent.at[1], core_came.at[1], partner)
        wait_bytes(col_wx.at[rows], col_came.at[at])
        send(col_wx.at[rows], col_wx.at[rows], core_sent.at[2], core_came.at[2], partner)
        return carry

    lax.fori_loop(1, plane, weight_core, 0)

    def pass_sides(level):
        for n in range(4):
            part = pl.ds(pl.multiple_of(level * plane + n * high, high), high)
            send(sides_all.at[c, part], sides_all.at[c, part], core_sent.at[5], core_came.at[5], partner)

    wait_bytes(sides_all.at[0, pl.ds(0, plane - 1)], s_came.at[z])
    pass_sides(z)
    for dz in range(1, deep):
        level = lax.rem(z + dz, deep)
        wait_bytes(sides_all.at[0, pl.ds(0, plane)], s_came.at[level])
        pass_sides(level)

    half_rows = pl.ds(0, plane * chunk)
    wait_bytes(bias_all.at[0], core_came.at[0])
    wait_bytes(row_wx.at[half_rows], core_came.at[1])
    wait_bytes(row_ox.at[o_half], core_came.at[3])
    for load in loads[2:]:
        load.wait()
    away = NEG * (present - 1.0)

    def place_bias(p, carry):
        at, level = lax.rem(p, plane), p // plane
        both = jnp.concatenate(
            [
                bias_all[r, at, level].astype(jnp.float32),
                bias_all[1 - r, at, level].astype(jnp.float32),
            ],
            0,
        )
        for t in range(rows_each):
            bias_rows[t * chips + p] = both[:, t * sites : (t + 1) * sites] + away
        return carry

    lax.fori_loop(0, chips, place_bias, 0)

    wait_bytes(sides_all.at[0], core_came.at[5])
    site = lax.broadcasted_iota(jnp.int32, (sites, chips), 0)
    owner = lax.broadcasted_iota(jnp.int32, (sites, chips), 1)

    def side_of(core, t, n):
        part = sides_all[core, :, :, t * sites : (t + 1) * sites].astype(jnp.float32)
        return part[:, n, :].astype(jnp.bfloat16)

    rights = jnp.zeros((sites, sites), jnp.float32)
    for core in range(2):
        for t in range(rows_each):
            put = site == owner * (2 * rows_each) + (core * rows_each + t)
            rights += dot(put.astype(jnp.float32).astype(jnp.bfloat16), side_of(core, t, 1))
    rights = rights.astype(jnp.bfloat16)
    parts = [dot_last(side_of(c, t, 0), rights)[:, None, :] for t in range(rows_each)]
    rows[...] = jnp.concatenate(parts, 1).astype(jnp.bfloat16)
    product[channel] = rows[chip]

    def to_rows(i, carry):
        to = lax.rem(chip + i, chips)
        send(rows.at[to], product.at[channel], p_sent, p_came, (*chip_at(to), c, 1 - r))
        send(rows.at[to], product.at[channel], p_sent, p_came, (*chip_at(to), c, r))
        return carry

    over_chips(to_rows, chips)
    send(rows.at[chip], product.at[channel], p_sent, p_came, (*here, c, 1 - r))

    def part_of(n):
        return slice(n * embed, (n + 1) * embed)

    def one(s, carry):
        x = standardize_features(msa[s]).astype(jnp.bfloat16)
        xq = dot(pick[...], x).astype(jnp.bfloat16)
        q = project(xq, row_w[part_of(0)], row_wx[part_of(0)])
        k = project(x, row_w[part_of(1)], row_wx[part_of(1)])
        v = project(x, row_w[part_of(2)], row_wx[part_of(2)])
        g = project(xq, row_w[part_of(3)], row_wx[part_of(3)])

        def bias_of(n):
            return bias_rows[n * block : (n + 1) * block].reshape(block * heads, sites)

        attend_rows(q, k, v, g, bias_of, mixed, block, heads)
        half = row_o.shape[0]
        delta = dot(mixed[:, :half], row_o[...]) + dot(mixed[:, half:], row_ox[...])
        done[s] = dot(pick[...], msa[s]) + delta
        return carry

    lax.fori_loop(0, msa.shape[0], one, 0)
    for t in range(rows_each):
        part = slice(t * chips, (t + 1) * chips)
        both = jnp.concatenate([done[0, part, :][:, None, :], done[1, part, :][:, None, :]], 1)
        seqs[:, :, t * embed : (t + 1) * embed] = both.astype(jnp.bfloat16)

    @pl.when(c == r)
    def _():
        column[me] = seqs[chip]

    def to_owner(i, carry):
        to = lax.rem(chip + i, chips)
        send(seqs.at[to], column.at[me], m_sent, m_came, (*chip_at(to), r, 1 - r))
        send(seqs.at[to], column.at[me], m_sent, m_came, (*chip_at(to), r, r))
        return carry

    over_chips(to_owner, chips)

    @pl.when(c != r)
    def _():
        send(seqs.at[chip], column.at[me], m_sent, m_came, (*here, r, r))

    send(seqs.at[chip], column.at[me], m_sent, m_came, (*here, r, 1 - r))

    wait_bytes(product.at[pl.ds(0, 2 * chips - 1)], p_came)
    wait_bytes(final_x, line_came.at[5])
    ours, theirs = final[...].astype(jnp.float32), final_x[...].astype(jnp.float32)
    first = jnp.where(r == 0, ours, theirs)
    second = jnp.where(r == 0, theirs, ours)
    finals = jnp.concatenate([first, second], 0).astype(jnp.bfloat16)
    width = pair_out.shape[1]

    def half_of(values):
        return jnp.where(r == 0, values[:width], values[width:])

    products = product[...].astype(jnp.float32)
    for t in range(rows_each):
        value = products[:, t, :]
        mean = jnp.mean(value, axis=0, keepdims=True)
        square = jnp.mean(value * value, axis=0, keepdims=True)
        scaled = ((value - mean) * lax.rsqrt(square - mean * mean + EPS)).astype(jnp.bfloat16)
        update = lax.dot_general(
            finals, scaled, (((0,), (0,)), ((), ())), preferred_element_type=jnp.float32
        )
        gate = 1.0 / (1.0 + jnp.exp(-dot_last(sigmoid_w[...], pair_ln[t])))
        keep = half_of(pair[t].astype(jnp.float32).T)
        pair_out[t] = (keep + gate * half_of(update)).astype(jnp.bfloat16)

    for sem in (m_came, m_sent):

        @pl.when(c == r)
        def _():
            wait_bytes(column.at[pl.ds(0, 2 * chips - 1)], sem)

        @pl.when(c != r)
        def _():
            wait_bytes(column, sem)

    wait_bytes(product.at[pl.ds(0, 2 * chips - 1)], p_sent)

    half = pl.ds(0, plane * chunk)
    rest = pl.ds(0, (plane - 1) * chunk)
    for sems in (core_came, core_sent):
        wait_bytes(col_wx.at[half], sems.at[2])
        wait_bytes(col_ox.at[o_half], sems.at[4])

    wait_bytes(bias_all.at[0], core_sent.at[0])
    wait_bytes(row_wx.at[half], core_sent.at[1])
    wait_bytes(row_ox.at[o_half], core_sent.at[3])
    wait_bytes(sides_all.at[0], core_sent.at[5])

    @pl.when(c == r)
    def _():
        wait_bytes(bias_all.at[0, 0, pl.ds(0, deep - 1)], line_sent.at[0])

    @pl.when(c != r)
    def _():
        wait_bytes(bias_all.at[0, 0], line_sent.at[0])

    wait_bytes(row_wx.at[mine], line_sent.at[1])
    wait_bytes(col_wx.at[mine], line_sent.at[2])
    wait_bytes(row_ox.at[o_half], line_sent.at[3])
    wait_bytes(col_ox.at[o_half], line_sent.at[4])
    wait_bytes(final_x, line_sent.at[5])
    wait_bytes(bias_all.at[0, pl.ds(0, plane - 1)], bias_sent)
    wait_bytes(row_wx.at[rest], row_sent)
    wait_bytes(col_wx.at[rest], col_sent)
    wait_bytes(sides_all.at[0, pl.ds(0, chips - 1)], s_sent)


def col_kernel(column, hidden, w, wx, wo, wox, out, mixed, *, heads, block):
    r = lax.axis_index("rep")
    embed = w.shape[1]
    width = embed // 2
    at = pl.ds(pl.multiple_of(r * width, width), width)
    away = NEG * (hidden[...].astype(jnp.float32).reshape(1, column.shape[0]) - 1.0)
    for t in range(column.shape[1] // embed):
        x = standardize_features(column[:, t * embed : (t + 1) * embed]).astype(jnp.bfloat16)
        q, k, v, g = [project(x, w[n], wx[n]) for n in range(4)]
        attend_rows(q, k, v, g, lambda n: away, mixed, block, heads)
        half = wo.shape[0]
        delta = dot(mixed[:, :half], wo[:, at]) + dot(mixed[:, half:], wox[:, at])
        keep = column[:, pl.ds(pl.multiple_of(t * embed + r * width, width), width)]
        out[t] = (keep.astype(jnp.float32) + delta).astype(jnp.bfloat16)


def local_call(kernel, out, scratch, flops, *operands):
    return pl.pallas_call(
        kernel,
        out_shape=jax.ShapeDtypeStruct(out, jnp.bfloat16),
        in_specs=[VMEM] * len(operands),
        out_specs=VMEM,
        scratch_shapes=[pltpu.VMEM(*s) for s in scratch],
        compiler_params=pltpu.CompilerParams(vmem_limit_bytes=40 << 20),
        cost_estimate=pl.CostEstimate(flops=flops, bytes_accessed=4 << 20, transcendentals=0),
    )(*operands)


def per_device(
    msa,
    pair,
    homolog_present,
    amino_present,
    row_w,
    row_out,
    offset_w,
    col_w,
    col_out,
    side_w,
    final_w,
    sigmoid_w,
):
    rows_here, sites, channels = pair.shape
    seqs_here, embed = msa.shape[0], msa.shape[2]
    chips = lax.axis_size(CHIPS)
    devices = lax.axis_size(DAP)
    heads_here = offset_w.shape[1]
    heads = 2 * heads_here
    flat = rows_here * sites
    flat_w = (row_w.shape[0] * row_w.shape[1], row_w.shape[2])
    queries = chips * rows_here
    operands = (
        pair,
        side_w.swapaxes(1, 2),
        msa,
        row_w.reshape(flat_w),
        row_out,
        col_w.reshape(flat_w),
        col_out,
        amino_present,
        offset_w.T,
        final_w,
        sigmoid_w.T,
    )
    side_channels = side_w.shape[2]
    half = channels // 2
    bf = jnp.bfloat16
    outs = [
        (rows_here, half, sites),
        (devices, seqs_here, rows_here * embed),
        flat_w,
        col_out.shape,
    ]
    scratch = [
        (pair.shape, bf),
        ((side_w.shape[0], side_channels, channels), bf),
        (msa.shape, bf),
        (flat_w, bf),
        (row_out.shape, bf),
        (pair.shape, bf),
        ((devices, rows_here, sites), bf),
        (final_w.shape, bf),
        ((heads_here, flat), bf),
        ((side_channels, 2, flat), bf),
        ((2, 16, chips // 16, heads_here, flat), bf),
        ((2, chips, 2, flat), bf),
        (flat_w, bf),
        (row_out.shape, bf),
        ((chips, rows_here, sites), bf),
        ((queries, heads, sites), jnp.float32),
        ((queries, embed), bf),
        ((seqs_here, queries, embed), jnp.float32),
        ((chips, seqs_here, rows_here * embed), bf),
    ]
    semaphores = [0, 4, 6, 6, 0, 16, 0, 16, 0, 16, 6, 6, 0, 0, 0, 0, 5]
    pair_output, column, col_wx, col_ox = pl.pallas_call(
        functools.partial(main_kernel, heads=heads, block=24),
        out_shape=[jax.ShapeDtypeStruct(shape, bf) for shape in outs],
        in_specs=[pl.BlockSpec(memory_space=pl.ANY)] * 7 + [VMEM] * (len(operands) - 7),
        out_specs=[VMEM] * len(outs),
        scratch_shapes=[pltpu.VMEM(*one) for one in scratch]
        + [pltpu.SemaphoreType.DMA if n == 0 else pltpu.SemaphoreType.DMA((n,)) for n in semaphores]
        + [pltpu.VMEM((queries, sites), bf)],
        compiler_params=pltpu.CompilerParams(
            collective_id=0, has_side_effects=True, vmem_limit_bytes=60 << 20
        ),
    )(*operands)
    column = column.reshape(devices * seqs_here, rows_here * embed)
    width = embed // 2
    alignment_output = local_call(
        functools.partial(col_kernel, heads=heads, block=32),
        (rows_here, devices * seqs_here, width),
        [((devices * seqs_here, embed), jnp.bfloat16)],
        3 << 30,
        column,
        homolog_present,
        col_w,
        col_wx.reshape(col_w.shape),
        col_out,
        col_ox,
    ).swapaxes(0, 1)

    return (alignment_output, pair_output.swapaxes(1, 2))


def solution(mesh):
    finer = Mesh(
        mesh.devices.reshape(4, 4, 4, 2, mesh.shape["rep"]),
        (*DAP, "rep"),
    )
    return jax.shard_map(
        per_device,
        mesh=finer,
        in_specs=(
            P(DAP, None, None),
            P(DAP, None, None),
            P(),
            P(),
            P(None, None, "rep"),
            P("rep", None),
            P(None, "rep"),
            P(None, None, "rep"),
            P("rep", None),
            P(None, None, "rep"),
            P("rep", None),
            P(None, "rep"),
        ),
        out_specs=(P(None, DAP, "rep"), P(DAP, None, "rep")),
        check_vma=False,
    )
```

```python
import functools

import jax
import jax.numpy as jnp
from jax import lax
from jax.experimental import pallas as pl
from jax.experimental.pallas import tpu as pltpu
from jax.sharding import Mesh
from jax.sharding import PartitionSpec as P

GROUP_BREADTH = 32
CHIPS = ("dap_0", "dap_1", "dap_2")
CORE = "dap_3"
DAP = CHIPS + (CORE,)
MESH = pl.DeviceIdType.MESH
VMEM = pl.BlockSpec(memory_space=pltpu.VMEM)

EPS = 1e-05
NEG = 1000000000.0


def standardize_features(values):
    values = values.astype(jnp.float32)
    center = jnp.mean(values, axis=-1, keepdims=True)
    spread = jnp.mean(jnp.square(values - center), axis=-1, keepdims=True)
    return (values - center) * lax.rsqrt(spread + EPS)


def place():
    z, x, y = (lax.axis_index(a) for a in CHIPS)
    return z, x, y, lax.axis_index(CORE), lax.axis_index("rep")


def send(src, dst, sent, came, device):
    pltpu.make_async_remote_copy(
        src_ref=src, dst_ref=dst, send_sem=sent, recv_sem=came, device_id=device, device_id_type=MESH
    ).start()


def wait_bytes(ref, sem):
    pltpu.make_async_copy(ref, ref, sem).wait()


def greet(device):
    pl.semaphore_signal(pltpu.get_barrier_semaphore(), inc=1, device_id=device, device_id_type=MESH)


def chip_at(to):
    plane, high = 16, 4
    return to // plane, lax.rem(to // high, high), lax.rem(to, high)


def dot_last(a, b):
    return lax.dot_general(a, b, (((1,), (1,)), ((), ())), preferred_element_type=jnp.float32)


def dot(a, b):
    return jnp.dot(a, b, preferred_element_type=jnp.float32)


def project(x, own, other):
    return jnp.concatenate([dot(x, own), dot(x, other)], 1).astype(jnp.bfloat16)


def attend_rows(q, k, v, g, bias, mixed, block, heads):
    embed = q.shape[1]
    queries = q.shape[0]
    lane = lax.broadcasted_iota(jnp.int32, (heads, embed), 1) // GROUP_BREADTH
    head = lax.broadcasted_iota(jnp.int32, (heads, embed), 0)
    own = (lane == head).astype(jnp.float32)[None]
    scale = 1.0 / jnp.sqrt(jnp.float32(GROUP_BREADTH))

    for n in range(queries // block):
        part = slice(n * block, (n + 1) * block)
        wide = q[part].astype(jnp.float32)[:, None, :] * own
        wide = wide.reshape(block * heads, embed).astype(jnp.bfloat16)
        scores = dot_last(wide, k) * scale + bias(n)
        scores = jnp.exp(scores - jnp.max(scores, axis=1, keepdims=True))
        weights = (scores * (1.0 / jnp.sum(scores, axis=1, keepdims=True))).astype(jnp.bfloat16)
        out = dot(weights, v).reshape(block, heads, embed) * own
        out = jnp.sum(out, axis=1)
        gate = 1.0 / (1.0 + jnp.exp(-g[part].astype(jnp.float32)))
        mixed[part, :] = (out * gate).astype(jnp.bfloat16)


def over_chips(step, chips):
    def three(j, carry):
        for n in range(3):
            step(3 * j + n + 1, 0)
        return carry

    lax.fori_loop(0, (chips - 1) // 3, three, 0)


def main_kernel(
    pair_in,
    side_in,
    msa_in,
    row_w_in,
    row_o_in,
    col_w_in,
    col_o_in,
    amino,
    offset_w,
    final,
    sigmoid_w,
    pair_out,
    column,
    col_wx,
    col_ox,
    pair,
    side_w,
    msa,
    row_w,
    row_o,
    pair_ln,
    product,
    final_x,
    bias,
    sides,
    bias_all,
    sides_all,
    row_wx,
    row_ox,
    rows,
    bias_rows,
    mixed,
    done,
    seqs,
    s_sent,
    s_came,
    line_sent,
    line_came,
    bias_sent,
    bias_came,
    row_sent,
    row_came,
    col_sent,
    col_came,
    core_sent,
    core_came,
    p_sent,
    p_came,
    m_sent,
    m_came,
    loaded,
    pick,
    *,
    heads,
    block,
):
    loads = []
    moves = [(pair_in, pair), (side_in, side_w), (msa_in, msa), (row_w_in, row_w), (row_o_in, row_o)]
    for n, (src, dst) in enumerate(moves):
        loads.append(pltpu.make_async_copy(src, dst, loaded.at[n]))
        loads[-1].start()
    z, x, y, c, r = place()
    deep, high = 4, 4
    plane = high * high
    chips = deep * plane
    xy = x * high + y
    chip = z * plane + xy
    me = chip * 2 + c
    channel = r * chips + chip
    here = (z, x, y)
    chunk = row_w.shape[0] // (2 * plane)
    mirror = (deep - 1 - z, x, y, c, 1 - r)
    partner = (z, x, y, 1 - c, r)
    rows_each, sites = pair.shape[0], pair.shape[1]
    embed = msa.shape[2]

    def rows_of(at):
        return pl.ds(pl.multiple_of((c * plane + at) * chunk, chunk), chunk)

    mine = rows_of(xy)

    def greet_chip(i, carry):
        there = chip_at(lax.rem(chip + i, chips))
        for ct in range(2):
            for rt in range(2):
                greet((*there, ct, rt))
        return carry

    over_chips(greet_chip, chips)
    greet((*here, 1 - c, r))
    greet((*here, c, 1 - r))
    greet((*here, 1 - c, 1 - r))

    present = amino[...].astype(jnp.float32).reshape(1, sites)
    at_site = lax.broadcasted_iota(jnp.int32, (1, sites), 1)
    query = lax.broadcasted_iota(jnp.int32, pick.shape, 0)
    picked = 2 * rows_each * (query & (chips - 1)) + rows_each * r + query // chips
    pick[...] = jnp.where(
        lax.broadcasted_iota(jnp.int32, pick.shape, 1) == picked, 1.0, 0.0
    ).astype(jnp.bfloat16)

    loads[0].wait()
    loads[1].wait()
    for t in range(rows_each):
        part = slice(t * sites, (t + 1) * sites)
        normed = standardize_features(pair[t]).astype(jnp.bfloat16)
        pair_ln[t] = normed
        bias[:, part] = dot_last(offset_w[...], normed).astype(jnp.bfloat16)
        here_too = jnp.where(at_site == me * rows_each + t, present, 0.0)
        mask = present * jnp.sum(here_too, axis=1, keepdims=True)
        both = []
        for n in range(2):
            gate = dot_last(side_w[2 * n], normed)
            value = dot_last(side_w[2 * n + 1], normed)
            side = value / (1.0 + jnp.exp(-gate)) * mask
            both.append(side[:, None, :])
        sides[:, :, part] = jnp.concatenate(both, 1).astype(jnp.bfloat16)
    sides_all[c, chip] = sides[chip]

    @pl.when(c == r)
    def _():
        bias_all[r, xy, z] = bias[...]

    pl.semaphore_wait(pltpu.get_barrier_semaphore(), 4 * chips - 1)

    for dz in range(deep):
        zt = lax.rem(z + dz, deep)
        if dz == 0:

            @pl.when(c != r)
            def _():
                send(bias, bias_all.at[r, xy, z], line_sent.at[0], line_came.at[0], (zt, x, y, r, c))

        else:
            send(bias, bias_all.at[r, xy, z], line_sent.at[0], line_came.at[0], (zt, x, y, r, c))
    send(row_w_in.at[mine], row_wx.at[mine], line_sent.at[1], line_came.at[1], mirror)
    send(col_w_in.at[mine], col_wx.at[mine], line_sent.at[2], line_came.at[2], mirror)
    o_half = pl.ds(pl.multiple_of(c * (row_o.shape[0] // 2), row_o.shape[0] // 2), row_o.shape[0] // 2)
    send(row_o_in.at[o_half], row_ox.at[o_half], line_sent.at[3], line_came.at[3], mirror)
    send(col_o_in.at[o_half], col_ox.at[o_half], line_sent.at[4], line_came.at[4], mirror)
    send(final, final_x, line_sent.at[5], line_came.at[5], mirror)

    def to_owner(i, carry):
        to = lax.rem(chip + i, chips)
        send(sides.at[to], sides_all.at[c, chip], s_sent, s_came.at[z], (*chip_at(to), c, r))
        return carry

    lax.fori_loop(1, plane, to_owner, 0)

    @pl.when(c == r)
    def _():
        wait_bytes(bias_all.at[0, 0, pl.ds(0, deep - 1)], line_came.at[0])

    @pl.when(c != r)
    def _():
        wait_bytes(bias_all.at[0, 0], line_came.at[0])

    def plane_device(i):
        to = lax.rem(xy + i, plane)
        return (z, to // high, lax.rem(to, high), c, r)

    def bias_plane(i, carry):
        send(bias_all.at[c, xy], bias_all.at[c, xy], bias_sent, bias_came.at[xy], plane_device(i))
        return carry

    lax.fori_loop(1, plane, bias_plane, 0)
    wait_bytes(row_wx.at[mine], line_came.at[1])
    wait_bytes(col_wx.at[mine], line_came.at[2])

    def weight_plane(i, carry):
        device = plane_device(i)
        send(row_wx.at[mine], row_wx.at[mine], row_sent, row_came.at[xy], device)
        send(col_wx.at[mine], col_wx.at[mine], col_sent, col_came.at[xy], device)
        return carry

    lax.fori_loop(1, plane, weight_plane, 0)
    lax.fori_loop(plane, chips, to_owner, 0)

    send(bias_all.at[c, xy], bias_all.at[c, xy], core_sent.at[0], core_came.at[0], partner)
    send(row_wx.at[mine], row_wx.at[mine], core_sent.at[1], core_came.at[1], partner)
    send(col_wx.at[mine], col_wx.at[mine], core_sent.at[2], core_came.at[2], partner)
    wait_bytes(row_ox.at[o_half], line_came.at[3])
    send(row_ox.at[o_half], row_ox.at[o_half], core_sent.at[3], core_came.at[3], partner)
    wait_bytes(col_ox.at[o_half], line_came.at[4])
    send(col_ox.at[o_half], col_ox.at[o_half], core_sent.at[4], core_came.at[4], partner)

    def bias_core(i, carry):
        at = lax.rem(xy + i, plane)
        wait_bytes(bias_all.at[c, at], bias_came.at[at])
        send(bias_all.at[c, at], bias_all.at[c, at], core_sent.at[0], core_came.at[0], partner)
        return carry

    lax.fori_loop(1, plane, bias_core, 0)

    def weight_core(i, carry):
        at = lax.rem(xy + i, plane)
        rows = rows_of(at)
        wait_bytes(row_wx.at[rows], row_came.at[at])
        send(row_wx.at[rows], row_wx.at[rows], core_sent.at[1], core_came.at[1], partner)
        wait_bytes(col_wx.at[rows], col_came.at[at])
        send(col_wx.at[rows], col_wx.at[rows], core_sent.at[2], core_came.at[2], partner)
        return carry

    lax.fori_loop(1, plane, weight_core, 0)

    def pass_sides(level):
        for n in range(4):
            part = pl.ds(pl.multiple_of(level * plane + n * high, high), high)
            send(sides_all.at[c, part], sides_all.at[c, part], core_sent.at[5], core_came.at[5], partner)

    wait_bytes(sides_all.at[0, pl.ds(0, plane - 1)], s_came.at[z])
    pass_sides(z)
    for dz in range(1, deep):
        level = lax.rem(z + dz, deep)
        wait_bytes(sides_all.at[0, pl.ds(0, plane)], s_came.at[level])
        pass_sides(level)

    half_rows = pl.ds(0, plane * chunk)
    wait_bytes(bias_all.at[0], core_came.at[0])
    wait_bytes(row_wx.at[half_rows], core_came.at[1])
    wait_bytes(row_ox.at[o_half], core_came.at[3])
    for load in loads[2:]:
        load.wait()
    away = NEG * (present - 1.0)

    def place_bias(p, carry):
        at, level = lax.rem(p, plane), p // plane
        both = jnp.concatenate(
            [
                bias_all[r, at, level].astype(jnp.float32),
                bias_all[1 - r, at, level].astype(jnp.float32),
            ],
            0,
        )
        for t in range(rows_each):
            bias_rows[t * chips + p] = both[:, t * sites : (t + 1) * sites] + away
        return carry

    lax.fori_loop(0, chips, place_bias, 0)

    wait_bytes(sides_all.at[0], core_came.at[5])
    site = lax.broadcasted_iota(jnp.int32, (sites, chips), 0)
    owner = lax.broadcasted_iota(jnp.int32, (sites, chips), 1)

    def side_of(core, t, n):
        part = sides_all[core, :, :, t * sites : (t + 1) * sites].astype(jnp.float32)
        return part[:, n, :].astype(jnp.bfloat16)

    rights = jnp.zeros((sites, sites), jnp.float32)
    for core in range(2):
        for t in range(rows_each):
            put = site == owner * (2 * rows_each) + (core * rows_each + t)
            rights += dot(put.astype(jnp.float32).astype(jnp.bfloat16), side_of(core, t, 1))
    rights = rights.astype(jnp.bfloat16)
    parts = [dot_last(side_of(c, t, 0), rights)[:, None, :] for t in range(rows_each)]
    rows[...] = jnp.concatenate(parts, 1).astype(jnp.bfloat16)
    product[channel] = rows[chip]

    def to_rows(i, carry):
        to = lax.rem(chip + i, chips)
        send(rows.at[to], product.at[channel], p_sent, p_came, (*chip_at(to), c, 1 - r))
        send(rows.at[to], product.at[channel], p_sent, p_came, (*chip_at(to), c, r))
        return carry

    over_chips(to_rows, chips)
    send(rows.at[chip], product.at[channel], p_sent, p_came, (*here, c, 1 - r))

    def part_of(n):
        return slice(n * embed, (n + 1) * embed)

    def one(s, carry):
        x = standardize_features(msa[s]).astype(jnp.bfloat16)
        xq = dot(pick[...], x).astype(jnp.bfloat16)
        q = project(xq, row_w[part_of(0)], row_wx[part_of(0)])
        k = project(x, row_w[part_of(1)], row_wx[part_of(1)])
        v = project(x, row_w[part_of(2)], row_wx[part_of(2)])
        g = project(xq, row_w[part_of(3)], row_wx[part_of(3)])

        def bias_of(n):
            return bias_rows[n * block : (n + 1) * block].reshape(block * heads, sites)

        attend_rows(q, k, v, g, bias_of, mixed, block, heads)
        half = row_o.shape[0]
        delta = dot(mixed[:, :half], row_o[...]) + dot(mixed[:, half:], row_ox[...])
        done[s] = dot(pick[...], msa[s]) + delta
        return carry

    lax.fori_loop(0, msa.shape[0], one, 0)
    for t in range(rows_each):
        part = slice(t * chips, (t + 1) * chips)
        both = jnp.concatenate([done[0, part, :][:, None, :], done[1, part, :][:, None, :]], 1)
        seqs[:, :, t * embed : (t + 1) * embed] = both.astype(jnp.bfloat16)

    @pl.when(c == r)
    def _():
        column[me] = seqs[chip]

    def to_owner(i, carry):
        to = lax.rem(chip + i, chips)
        send(seqs.at[to], column.at[me], m_sent, m_came, (*chip_at(to), r, 1 - r))
        send(seqs.at[to], column.at[me], m_sent, m_came, (*chip_at(to), r, r))
        return carry

    over_chips(to_owner, chips)

    @pl.when(c != r)
    def _():
        send(seqs.at[chip], column.at[me], m_sent, m_came, (*here, r, r))

    send(seqs.at[chip], column.at[me], m_sent, m_came, (*here, r, 1 - r))

    wait_bytes(product.at[pl.ds(0, 2 * chips - 1)], p_came)
    wait_bytes(final_x, line_came.at[5])
    ours, theirs = final[...].astype(jnp.float32), final_x[...].astype(jnp.float32)
    first = jnp.where(r == 0, ours, theirs)
    second = jnp.where(r == 0, theirs, ours)
    finals = jnp.concatenate([first, second], 0).astype(jnp.bfloat16)
    width = pair_out.shape[1]

    def half_of(values):
        return jnp.where(r == 0, values[:width], values[width:])

    products = product[...].astype(jnp.float32)
    for t in range(rows_each):
        value = products[:, t, :]
        mean = jnp.mean(value, axis=0, keepdims=True)
        square = jnp.mean(value * value, axis=0, keepdims=True)
        scaled = ((value - mean) * lax.rsqrt(square - mean * mean + EPS)).astype(jnp.bfloat16)
        update = lax.dot_general(
            finals, scaled, (((0,), (0,)), ((), ())), preferred_element_type=jnp.float32
        )
        gate = 1.0 / (1.0 + jnp.exp(-dot_last(sigmoid_w[...], pair_ln[t])))
        keep = half_of(pair[t].astype(jnp.float32).T)
        pair_out[t] = (keep + gate * half_of(update)).astype(jnp.bfloat16)

    for sem in (m_came, m_sent):

        @pl.when(c == r)
        def _():
            wait_bytes(column.at[pl.ds(0, 2 * chips - 1)], sem)

        @pl.when(c != r)
        def _():
            wait_bytes(column, sem)

    wait_bytes(product.at[pl.ds(0, 2 * chips - 1)], p_sent)

    half = pl.ds(0, plane * chunk)
    rest = pl.ds(0, (plane - 1) * chunk)
    for sems in (core_came, core_sent):
        wait_bytes(col_wx.at[half], sems.at[2])
        wait_bytes(col_ox.at[o_half], sems.at[4])

    wait_bytes(bias_all.at[0], core_sent.at[0])
    wait_bytes(row_wx.at[half], core_sent.at[1])
    wait_bytes(row_ox.at[o_half], core_sent.at[3])
    wait_bytes(sides_all.at[0], core_sent.at[5])

    @pl.when(c == r)
    def _():
        wait_bytes(bias_all.at[0, 0, pl.ds(0, deep - 1)], line_sent.at[0])

    @pl.when(c != r)
    def _():
        wait_bytes(bias_all.at[0, 0], line_sent.at[0])

    wait_bytes(row_wx.at[mine], line_sent.at[1])
    wait_bytes(col_wx.at[mine], line_sent.at[2])
    wait_bytes(row_ox.at[o_half], line_sent.at[3])
    wait_bytes(col_ox.at[o_half], line_sent.at[4])
    wait_bytes(final_x, line_sent.at[5])
    wait_bytes(bias_all.at[0, pl.ds(0, plane - 1)], bias_sent)
    wait_bytes(row_wx.at[rest], row_sent)
    wait_bytes(col_wx.at[rest], col_sent)
    wait_bytes(sides_all.at[0, pl.ds(0, chips - 1)], s_sent)


def col_kernel(column, hidden, w, wx, wo, wox, out, mixed, *, heads, block):
    r = lax.axis_index("rep")
    embed = w.shape[1]
    width = embed // 2
    at = pl.ds(pl.multiple_of(r * width, width), width)
    away = NEG * (hidden[...].astype(jnp.float32).reshape(1, mixed.shape[0]) - 1.0)
    for t in range(out.shape[0]):
        here = column[:, :, t * embed : (t + 1) * embed].astype(jnp.float32).reshape(mixed.shape)
        x = standardize_features(here).astype(jnp.bfloat16)
        q, k, v, g = [project(x, w[n], wx[n]) for n in range(4)]
        attend_rows(q, k, v, g, lambda n: away, mixed, block, heads)
        half = wo.shape[0]
        delta = dot(mixed[:, :half], wo[:, at]) + dot(mixed[:, half:], wox[:, at])
        keep = jnp.where(r == 0, here[:, :width], here[:, width:])
        out[t] = (keep + delta).astype(jnp.bfloat16)


def local_call(kernel, out, scratch, flops, *operands):
    return pl.pallas_call(
        kernel,
        out_shape=jax.ShapeDtypeStruct(out, jnp.bfloat16),
        in_specs=[VMEM] * len(operands),
        out_specs=VMEM,
        scratch_shapes=[pltpu.VMEM(*s) for s in scratch],
        compiler_params=pltpu.CompilerParams(vmem_limit_bytes=40 << 20),
        cost_estimate=pl.CostEstimate(flops=flops, bytes_accessed=4 << 20, transcendentals=0),
    )(*operands)


def per_device(
    msa,
    pair,
    homolog_present,
    amino_present,
    row_w,
    row_out,
    offset_w,
    col_w,
    col_out,
    side_w,
    final_w,
    sigmoid_w,
):
    rows_here, sites, channels = pair.shape
    seqs_here, embed = msa.shape[0], msa.shape[2]
    chips = lax.axis_size(CHIPS)
    devices = lax.axis_size(DAP)
    heads_here = offset_w.shape[1]
    heads = 2 * heads_here
    flat = rows_here * sites
    flat_w = (row_w.shape[0] * row_w.shape[1], row_w.shape[2])
    queries = chips * rows_here
    operands = (
        pair,
        side_w.swapaxes(1, 2),
        msa,
        row_w.reshape(flat_w),
        row_out,
        col_w.reshape(flat_w),
        col_out,
        amino_present,
        offset_w.T,
        final_w,
        sigmoid_w.T,
    )
    side_channels = side_w.shape[2]
    half = channels // 2
    bf = jnp.bfloat16
    outs = [
        (rows_here, half, sites),
        (devices, seqs_here, rows_here * embed),
        flat_w,
        col_out.shape,
    ]
    scratch = [
        (pair.shape, bf),
        ((side_w.shape[0], side_channels, channels), bf),
        (msa.shape, bf),
        (flat_w, bf),
        (row_out.shape, bf),
        (pair.shape, bf),
        ((devices, rows_here, sites), bf),
        (final_w.shape, bf),
        ((heads_here, flat), bf),
        ((side_channels, 2, flat), bf),
        ((2, 16, chips // 16, heads_here, flat), bf),
        ((2, chips, 2, flat), bf),
        (flat_w, bf),
        (row_out.shape, bf),
        ((chips, rows_here, sites), bf),
        ((queries, heads, sites), jnp.float32),
        ((queries, embed), bf),
        ((seqs_here, queries, embed), jnp.float32),
        ((chips, seqs_here, rows_here * embed), bf),
    ]
    semaphores = [0, 4, 6, 6, 0, 16, 0, 16, 0, 16, 6, 6, 0, 0, 0, 0, 5]
    pair_output, column, col_wx, col_ox = pl.pallas_call(
        functools.partial(main_kernel, heads=heads, block=24),
        out_shape=[jax.ShapeDtypeStruct(shape, bf) for shape in outs],
        in_specs=[pl.BlockSpec(memory_space=pl.ANY)] * 7 + [VMEM] * (len(operands) - 7),
        out_specs=[VMEM] * len(outs),
        scratch_shapes=[pltpu.VMEM(*one) for one in scratch]
        + [pltpu.SemaphoreType.DMA if n == 0 else pltpu.SemaphoreType.DMA((n,)) for n in semaphores]
        + [pltpu.VMEM((queries, sites), bf)],
        compiler_params=pltpu.CompilerParams(
            collective_id=0, has_side_effects=True, vmem_limit_bytes=60 << 20
        ),
    )(*operands)
    width = embed // 2
    alignment_output = local_call(
        functools.partial(col_kernel, heads=heads, block=32),
        (rows_here, devices * seqs_here, width),
        [((devices * seqs_here, embed), jnp.bfloat16)],
        3 << 30,
        column,
        homolog_present,
        col_w,
        col_wx.reshape(col_w.shape),
        col_out,
        col_ox,
    ).swapaxes(0, 1)

    return (alignment_output, pair_output.swapaxes(1, 2))


def solution(mesh):
    finer = Mesh(
        mesh.devices.reshape(4, 4, 4, 2, mesh.shape["rep"]),
        (*DAP, "rep"),
    )
    return jax.shard_map(
        per_device,
        mesh=finer,
        in_specs=(
            P(DAP, None, None),
            P(DAP, None, None),
            P(),
            P(),
            P(None, None, "rep"),
            P("rep", None),
            P(None, "rep"),
            P(None, None, "rep"),
            P("rep", None),
            P(None, None, "rep"),
            P("rep", None),
            P(None, "rep"),
        ),
        out_specs=(P(None, DAP, "rep"), P(DAP, None, "rep")),
        check_vma=False,
    )
```
